256 devices in a mesh: groups: 2 (over z), tensor: 64 (over x, y), seq: 2 (over core).
Axes of the slice: x: 8, y: 8, z: 2, core: 2. Of those that a mesh axis runs over, the one named last changes fastest.
The devices are a block of a 8x8x16 slice.
Arguments:
- heads_out: bfloat16 [1024, 4096], P(('groups', 'seq'), 'tensor'), parts along dimension 0, may hold values from -6 to 6
- stream_in: bfloat16 [1024, 8192], P(('groups', 'seq', 'tensor')), parts along dimension 0, may hold values from -40 to 40, as said below
- proj_levels: bfloat16 [4096, 8192], P('tensor'), may hold values from -8 to 7, as said below
- proj_scale: float32 [8192], replicated, may hold values from 0.001703125 to 0.006796875
- norm_gain: float32 [8192], replicated, may hold values from 0.25 to 1.75
- gate_levels: bfloat16 [8192, 14336], P(None, 'tensor'), may hold values from -8 to 7, as said below
- gate_scale: float32 [14336], P('tensor'), may hold values from 0.0012153398 to 0.004861359
- gate_index: int32 [64, 8], P('tensor'), may hold values from 0 to 223, as said below
- gate_extra: bfloat16 [8192, 512], P(None, 'tensor'), may hold values from -0.29882812 to 0.29882812
- up_levels: bfloat16 [8192, 14336], P(None, 'tensor'), may hold values from -8 to 7, as said below
- up_scale: float32 [14336], P('tensor'), may hold values from 0.0012153398 to 0.004861359
- up_index: int32 [64, 8], P('tensor'), may hold values from 0 to 223, as said below
- up_extra: bfloat16 [8192, 512], P(None, 'tensor'), may hold values from -0.29882812 to 0.29882812
- down_levels: bfloat16 [14336, 8192], P('tensor'), may hold values from -8 to 7, as said below
- down_scale: float32 [8192], replicated, may hold values from 0.0009020067 to 0.003591323
- down_index: int32 [64, 8], P('tensor'), may hold values from 0 to 8191, as said below
- down_extra: bfloat16 [14336, 8], P('tensor'), may hold values from -0.29882812 to 0.29882812
Outputs:
- stream_out: bfloat16 [1024, 8192], P(('groups', 'seq', 'tensor')), parts along dimension 0
The draws below stay inside these ranges and needn't reach their ends.
There are 2 independent parts, one for each index of `groups`. The reference program is written for one: setup_inputs(seed, part) draws one part's arguments, and reference() takes and returns one part's arrays. A program takes and returns all parts, laid end to end along the dimension named above; an argument that names none is the same for every part. Nothing has to cross between parts.
Inputs may be any that keep to these rules, and one draw needn't show every extreme that they name: stream_in has rows and columns of differing scales. `proj_levels`: integer values. `gate_levels`: integer values. `up_levels`: integer values. `down_levels`: integer values. `gate_index`: each row holds 8 different numbers. `up_index`: each row holds 8 different numbers. `down_index`: each row holds 8 different numbers.
All inputs are finite; a program needn't handle non-finite values.
Results may differ from the reference program's by a relative error of at most 0.0055.
Values may be sent and summed in bfloat16 or wider, within the bound.
A program may use at most 128 MiB of HBM per device.

```python
import math
import jax
import jax.numpy as jnp
from jax import lax

D = 8192
HD = 4096
FF = 14336
K_OUT = 8
TOKENS = 512
N_TENSOR = 64


def level_draw(key, rows, columns):
    return jax.random.randint(key, (rows, columns), -8, 8).astype(jnp.float32)


def index_draw(key, width):
    row_key, edge_key, inner_key = jax.random.split(key, 3)
    keys = jax.random.split(row_key, N_TENSOR)
    orders = jax.vmap(lambda single: jax.random.permutation(single, width))(keys)[:, :K_OUT].astype(jnp.int32)
    inner = (jax.random.permutation(inner_key, width - 2) + 1).astype(jnp.int32)
    edge_row = jnp.concatenate([jnp.array([0, width - 1], dtype=jnp.int32), inner[:K_OUT - 2]])
    chosen = jax.random.randint(edge_key, (), 0, N_TENSOR)
    rows = jnp.arange(N_TENSOR, dtype=jnp.int32)[:, None]
    return jnp.where(rows == chosen, edge_row[None, :], orders).astype(jnp.int32)


def draw_proj_levels(key, part):
    return level_draw(jax.random.fold_in(key, 11), HD, D).astype(jnp.bfloat16)


def draw_gate_levels(key, part):
    return level_draw(jax.random.fold_in(key, 12), D, FF).astype(jnp.bfloat16)


def draw_up_levels(key, part):
    return level_draw(jax.random.fold_in(key, 13), D, FF).astype(jnp.bfloat16)


def draw_down_levels(key, part):
    return level_draw(jax.random.fold_in(key, 14), FF, D).astype(jnp.bfloat16)


def draw_gate_index(key, part):
    return index_draw(jax.random.fold_in(key, 21), FF // N_TENSOR)


def draw_up_index(key, part):
    return index_draw(jax.random.fold_in(key, 22), FF // N_TENSOR)


def draw_down_index(key, part):
    return index_draw(jax.random.fold_in(key, 23), D)


def draw_stream_in(key, part):
    row_key, col_key, base_key = jax.random.split(jax.random.fold_in(key, 31), 3)
    row_scale = jnp.exp(jax.random.uniform(row_key, (TOKENS, 1), jnp.float32, jnp.log(0.3), jnp.log(3.0)))
    col_scale = jnp.exp(jax.random.uniform(col_key, (1, D), jnp.float32, jnp.log(0.3), jnp.log(3.0)))
    base = jnp.clip(jax.random.normal(base_key, (TOKENS, D), jnp.float32), -4.0, 4.0)
    return (base * row_scale * col_scale).astype(jnp.bfloat16)


def level_of(own_key, shape, pieces, low, high):
    loudness = 1.0
    for dim, blocks in pieces:
        draws = jax.random.uniform(jax.random.fold_in(jax.random.fold_in(own_key, 6), dim), (blocks,), jnp.float32, low / len(pieces), high / len(pieces))
        loudness = loudness * jnp.repeat(jnp.exp(draws), shape[dim] // blocks).reshape((-1,) + (1,) * (len(shape) - 1 - dim))
    return loudness


def noise(own_key, dims, spread, most, cuts=(), kind=jnp.bfloat16):
    values = spread * jax.random.normal(own_key, dims, jnp.float32)
    if cuts:
        values = values * level_of(own_key, dims, cuts, -0.22, 0.18)
    return jnp.clip(values, -most, most).astype(kind)


def setup_inputs(seed: int = 0, part: int = 0) -> dict:
    key_list = jax.random.split(jax.random.key(seed), 18)
    part_splits = jax.random.split(jax.random.fold_in(key_list[17], part), 18)
    return {
        "heads_out": noise(part_splits[0], (TOKENS, HD), 1.0, 6.0, ((0, 2), (1, 64))),
        "stream_in": draw_stream_in(jax.random.fold_in(jax.random.fold_in(key_list[17], part), 71), part),
        "proj_levels": draw_proj_levels(jax.random.fold_in(key_list[17], 71), part),
        "proj_scale": jnp.clip(jnp.exp(jax.random.uniform(key_list[3], (D,), jnp.float32, math.log(0.001703125), math.log(0.006796875))), 0.001703125, 0.006796875),
        "norm_gain": jnp.clip(1.0 + 0.15 * jax.random.normal(key_list[4], (D,), jnp.float32), 0.25, 1.75),
        "gate_levels": draw_gate_levels(jax.random.fold_in(key_list[17], 71), part),
        "gate_scale": jnp.clip(jnp.exp(math.log(0.004861359) - 1.3862944 * jax.random.uniform(key_list[6], (FF,), jnp.float32) ** level_of(key_list[6], (FF,), ((0, 64),), -0.2, 0.2)), 0.0012153398, 0.004861359),
        "gate_index": draw_gate_index(jax.random.fold_in(key_list[17], 71), part),
        "gate_extra": noise(key_list[8], (D, N_TENSOR * K_OUT), 0.05, 0.29882812, ((1, 64),)),
        "up_levels": draw_up_levels(jax.random.fold_in(key_list[17], 71), part),
        "up_scale": jnp.clip(jnp.exp(math.log(0.004861359) - 1.3862944 * jax.random.uniform(key_list[10], (FF,), jnp.float32) ** level_of(key_list[10], (FF,), ((0, 64),), -0.2, 0.2)), 0.0012153398, 0.004861359),
        "up_index": draw_up_index(jax.random.fold_in(key_list[17], 71), part),
        "up_extra": noise(key_list[12], (D, N_TENSOR * K_OUT), 0.05, 0.29882812, ((1, 64),)),
        "down_levels": draw_down_levels(jax.random.fold_in(key_list[17], 71), part),
        "down_scale": jnp.clip(jnp.exp(jax.random.uniform(key_list[14], (D,), jnp.float32, math.log(0.0009020067), math.log(0.003591323))), 0.0009020067, 0.003591323),
        "down_index": draw_down_index(jax.random.fold_in(key_list[17], 71), part),
        "down_extra": noise(key_list[16], (FF, K_OUT), 0.05, 0.29882812, ((0, 64),)),
    }


def wide_dot(left, right):
    return jnp.dot(left.astype(jnp.float32), right.astype(jnp.float32), precision=lax.Precision.HIGHEST, preferred_element_type=jnp.float32)

def rms_norm(mixed, norm_gain):
    mean_sq = lax.optimization_barrier(jnp.mean(mixed * mixed, axis=-1, keepdims=True))
    return (mixed * lax.rsqrt(mean_sq + 1e-05) * norm_gain).astype(jnp.bfloat16)

def column_parallel(normed, levels, scale, index, extra):
    shard_width = FF // N_TENSOR
    base = wide_dot(normed, levels) * scale
    added = wide_dot(normed, extra)
    columns = (jnp.arange(N_TENSOR, dtype=jnp.int32)[:, None] * shard_width + index.astype(jnp.int32)).reshape(-1).astype(jnp.int32)
    return base.at[:, columns].add(added)

def reference(heads_out, stream_in, proj_levels, proj_scale, norm_gain, gate_levels, gate_scale, gate_index, gate_extra, up_levels, up_scale, up_index, up_extra, down_levels, down_scale, down_index, down_extra):
    shard_width = FF // N_TENSOR
    proj = wide_dot(heads_out, proj_levels) * proj_scale
    mixed = stream_in.astype(jnp.float32) + proj
    normed = rms_norm(mixed, norm_gain)
    gate = column_parallel(normed, gate_levels, gate_scale, gate_index, gate_extra)
    up = column_parallel(normed, up_levels, up_scale, up_index, up_extra)
    hidden = (jax.nn.silu(gate) * up).astype(jnp.bfloat16)
    down = wide_dot(hidden, down_levels) * down_scale
    parts = hidden.astype(jnp.float32).reshape(hidden.shape[0], N_TENSOR, shard_width)
    extra = down_extra.astype(jnp.float32).reshape(N_TENSOR, shard_width, K_OUT)
    added = jnp.einsum('tns,nsk->tnk', parts, extra, precision=lax.Precision.HIGHEST).reshape(hidden.shape[0], N_TENSOR * K_OUT)
    down = down.at[:, down_index.reshape(-1).astype(jnp.int32)].add(added)
    return (mixed + down).astype(jnp.bfloat16)
```

```python
import functools
import math

import jax
import jax.numpy as jnp
from jax import lax
from jax.experimental import pallas as pl
from jax.experimental.pallas import tpu as pltpu
from jax.sharding import Mesh
from jax.sharding import PartitionSpec as P

TENSOR = ("tensor_0", "tensor_1")
GROUPS_SEQ_TENSOR = ("groups", "seq", "tensor_0", "tensor_1")
MESH = pl.DeviceIdType.MESH
F32 = jnp.float32
BF16 = jnp.bfloat16
NT = (((1,), (1,)), ((), ()))


def dot(a, b):
    return jnp.dot(a, b, preferred_element_type=F32)


def dot_nt(a, b):
    return lax.dot_general(a, b, NT, preferred_element_type=F32)


def kernel(
    n,
    heads_ref,
    stream_ref,
    projw_ref,
    pscale_ref,
    gain_ref,
    gatew_ref,
    gscale_ref,
    gidx_ref,
    gext_ref,
    upw_ref,
    uscale_ref,
    uidx_ref,
    uext_ref,
    downw_ref,
    dscale_ref,
    didx_ref,
    dext_ref,
    out_ref,
    wcat,
    wd,
    onehot,
    perm,
    gpick,
    upick,
    dextp,
    invg,
    heads_all,
    w_all,
    strm,
    t_sum,
    t_half,
    r_one,
    mixed,
    y_all,
    acc,
    sumsq,
    hid,
    extra_parts,
    ring_s,
    ring_r,
    r_two,
    out_s,
    load_sem,
    heads_ss,
    heads_rs,
    w_ss,
    w_rs,
    strm_ss,
    strm_rs,
    one_ss,
    one_rs,
    aga_ss,
    aga_rs,
    agb_ss,
    agb_rs,
    ring_ss,
    ring_rs,
    two_ss,
    two_rs,
    out_ss,
    out_rs,
):
    feats, tokens = heads_ref.shape
    width = projw_ref.shape[1]
    hidden = gatew_ref.shape[0]
    rows = stream_ref.shape[0]
    slots = gpick.shape[0]
    k_out = gext_ref.shape[0]
    half = width // 2
    strip = half // n
    block = tokens // n
    sub = tokens // 2
    reach = n // 2
    axes = (("tensor_0", "tensor_1"), ("tensor_1", "tensor_0"))
    pos = {name: lax.axis_index(name) for name in TENSOR}
    offsets = sorted(range(1, n), key=lambda r: -min(r, n - r))

    def at(name, shift):
        return lax.rem(pos[name] + (shift + n) % n, n)

    def cols(h, j):
        return pl.ds(pl.multiple_of(h * half + j * strip, strip), strip)

    def send(src, dst, ssem, rsem, name, target):
        return pltpu.make_async_remote_copy(
            src_ref=src,
            dst_ref=dst,
            send_sem=ssem,
            recv_sem=rsem,
            device_id={name: target},
            device_id_type=MESH,
        )

    barrier = pltpu.get_barrier_semaphore()
    for name in TENSOR:
        for r in range(1, n):
            pl.semaphore_signal(
                barrier, inc=1, device_id={name: at(name, r)}, device_id_type=MESH
            )
    loads = [
        pltpu.make_async_copy(gatew_ref, wcat.at[pl.ds(0, hidden), :], load_sem.at[0]),
        pltpu.make_async_copy(upw_ref, wcat.at[pl.ds(slots, hidden), :], load_sem.at[1]),
        pltpu.make_async_copy(downw_ref, wd.at[pl.ds(0, hidden), :], load_sem.at[2]),
    ]
    own_w = []
    for h in (0, 1):
        me = pos[axes[h][0]]
        own_w.append(
            pltpu.make_async_copy(
                projw_ref.at[:, cols(h, me)],
                w_all.at[h, pl.ds(pl.multiple_of(me * feats, feats), feats), :],
                load_sem.at[3 + h],
            )
        )
        own_w[h].start()
    pl.semaphore_wait(barrier, 2 * (n - 1))

    def heads_copy(h, r, sender):
        a = axes[h][0]
        place = pl.ds(pl.multiple_of(sender * feats, feats), feats)
        return send(
            heads_ref,
            heads_all.at[h, place, :],
            heads_ss.at[h, r],
            heads_rs.at[h, r],
            a,
            at(a, r),
        )

    def w_copy(h, r, sender):
        a = axes[h][0]
        place = pl.ds(pl.multiple_of(sender * feats, feats), feats)
        return send(
            projw_ref.at[:, cols(h, at(a, r))],
            w_all.at[h, place, :],
            w_ss.at[h, r],
            w_rs.at[h, r],
            a,
            at(a, r),
        )

    def strm_copy(h, r, sender):
        a = axes[h][0]
        return send(
            stream_ref.at[:, cols(h, at(a, r))],
            strm.at[h, sender],
            strm_ss.at[h, r],
            strm_rs.at[h, r],
            a,
            at(a, r),
        )

    for r in offsets:
        for h in (0, 1):
            heads_copy(h, r, pos[axes[h][0]]).start()
            w_copy(h, r, pos[axes[h][0]]).start()
    for r in offsets:
        for h in (0, 1):
            strm_copy(h, r, pos[axes[h][0]]).start()
    for load in loads:
        load.start()

    for h in (0, 1):
        me = pos[axes[h][0]]
        heads_all[h, pl.ds(pl.multiple_of(me * feats, feats), feats), :] = heads_ref[...]
        strm[h, me] = stream_ref[:, cols(h, me)]
    r_i = lax.broadcasted_iota(jnp.int32, (tokens, tokens), 0)
    c_i = lax.broadcasted_iota(jnp.int32, (tokens, tokens), 1)
    swapped = (
        lax.rem(lax.div(r_i, rows), n) * block + lax.div(r_i, block) * rows + lax.rem(r_i, rows)
    )
    perm[...] = jnp.where(c_i == swapped, 1.0, 0.0).astype(BF16)

    def index_column(idx_ref, count):
        row = lax.rem(lax.broadcasted_iota(jnp.int32, (count, 1), 0), k_out)
        column = jnp.zeros((count, 1), jnp.int32)
        for k in range(k_out):
            column = jnp.where(row == k, idx_ref[0, k], column)
        return column

    for pick, idx_ref in ((gpick, gidx_ref), (upick, uidx_ref)):
        pick[...] = jnp.zeros_like(pick)
        chosen = lax.broadcasted_iota(jnp.int32, (k_out, slots), 1) == index_column(idx_ref, k_out)
        pick[pl.ds(hidden, k_out), :] = jnp.where(chosen, 1.0, 0.0)

    one_rows = onehot.shape[0]
    didx = index_column(didx_ref, one_rows)
    live = lax.broadcasted_iota(jnp.int32, (one_rows, strip), 0) < 2 * k_out

    def prepare(j, carry):
        here = pl.ds(pl.multiple_of(j * strip, strip), strip)
        column = lax.broadcasted_iota(jnp.int32, (one_rows, strip), 1) + j * strip
        onehot[:, here] = jnp.where((column == didx) & live, 1.0, 0.0).astype(BF16)
        blank = jnp.zeros((slots - hidden - k_out, strip), F32)
        for base, ext in ((0, gext_ref), (slots, uext_ref)):
            filled = jnp.concatenate([ext[:, here].astype(F32), blank], axis=0)
            wcat[pl.ds(base + hidden, slots - hidden), here] = filled.astype(BF16)
        wd[pl.ds(hidden, slots - hidden), here] = jnp.zeros((slots - hidden, strip), BF16)
        invg[:, here] = 1.0 / gain_ref[:, here]
        return carry

    lax.fori_loop(0, width // strip, prepare, 0)
    dext = jnp.concatenate([dext_ref[...].astype(F32)] * 2, axis=0)
    dext = jnp.concatenate([dext, jnp.zeros((dextp.shape[0] - 2 * k_out, hidden), F32)], axis=0)
    dextp[...] = jnp.zeros_like(dextp)
    dextp[:, pl.ds(0, hidden)] = dext.astype(BF16)
    acc[...] = jnp.zeros_like(acc)
    sumsq[...] = jnp.zeros_like(sumsq)
    for h in (0, 1):
        for d in (0, 1):
            for m in (0, 1):
                ring_r[h, d, m] = jnp.zeros((sub, strip), BF16)

    def one_copy(h, r):
        b = axes[h][1]
        away = pl.ds(pl.multiple_of(at(b, r) * block, block), block)
        return send(
            t_half.at[h, away, :], r_one.at[h, r], one_ss.at[h, r], one_rs.at[h, r], b, at(b, r)
        )

    for h in (0, 1):
        a = axes[h][0]
        own_w[h].wait()
        for r in offsets:
            heads_copy(h, r, at(a, -r)).wait_recv()
            w_copy(h, r, at(a, -r)).wait_recv()
        if h == 0:
            turn = perm[...]
        else:
            turn = jnp.where(r_i == c_i, 1.0, 0.0).astype(BF16)
        ordered = dot_nt(turn, heads_all[h]).astype(BF16)
        t_sum[h] = dot(ordered, w_all[h])
        t_half[h] = t_sum[h].astype(BF16)
        for r in offsets:
            one_copy(h, r).start()

    def aga_copy(h, r, owner):
        a, b = axes[h]
        place = pl.ds(pl.multiple_of(owner * block, block), block)
        there = y_all.at[h, pos[a], place, :]
        return send(there, there, aga_ss.at[h, r], aga_rs.at[h, r], b, at(b, r))

    for h in (0, 1):
        a, b = axes[h]
        here = cols(h, pos[a])
        own = pl.ds(pl.multiple_of(pos[b] * block, block), block)
        total = t_sum[h, own, :]
        for r in range(1, n):
            one_copy(h, r).wait_recv()
            total += r_one[h, r].astype(F32)
        mixed[h] = total * pscale_ref[:, here]
        for r in range(1, n):
            strm_copy(h, r, at(a, -r)).wait_recv()
        for j in range(n):
            part = pl.ds(j * rows, rows)
            mixed[h, part, :] = mixed[h, part, :] + strm[h, j].astype(F32)
        y_all[h, pos[a], own, :] = (mixed[h] * gain_ref[:, here]).astype(BF16)
        for r in offsets:
            aga_copy(h, r, pos[b]).start()

    def agb_copy(h, d, k, s, strip_id):
        a = axes[h][0]
        there = y_all.at[h, strip_id, pl.ds(s * sub, sub), :]
        return send(
            there, there, agb_ss.at[h, d, k, s], agb_rs.at[h, d, k, s], a, at(a, 1 - 2 * d)
        )

    def behind(h, d, k):
        shift = k if d else n - k
        return lax.rem(pos[axes[h][0]] + shift, n)

    def use(h, j):
        y = y_all[h, j]
        if h == 0:
            y = dot(perm[...], y).astype(BF16)
        here = cols(h, j)
        scaled = y.astype(F32) * invg[:, here]
        scaled = scaled * scaled
        lanes = sumsq.shape[1]
        part = scaled[:, :lanes]
        for q in range(1, strip // lanes):
            part += scaled[:, q * lanes : (q + 1) * lanes]
        sumsq[...] += part
        acc[...] += dot_nt(y, wcat[:, here])

    for h in (0, 1):
        a, b = axes[h]
        for r in range(1, n):
            aga_copy(h, r, at(b, -r)).wait_recv()
        for step in (0, 1):
            for d in (0, 1):
                s = step if d == 0 else 1 - step
                agb_copy(h, d, 0, s, pos[a]).start()
    loads[0].wait()
    loads[1].wait()
    for h in (0, 1):
        use(h, pos[axes[h][0]])

    def gather_step(k, carry):
        for step in (0, 1):
            for h in (0, 1):
                for d in (0, 1):
                    s = step if d == 0 else 1 - step
                    j = behind(h, d, k)
                    agb_copy(h, d, k - 1, s, j).wait_recv()
                    if step == 0:
                        agb_copy(h, d, k, s, j).start()
                    else:

                        @pl.when(k < reach - 1)
                        def _():
                            agb_copy(h, d, k, s, j).start()

        for h in (0, 1):
            for d in (0, 1):
                use(h, behind(h, d, k))
        return carry

    lax.fori_loop(1, reach, gather_step, 0)
    for h in (0, 1):
        j = behind(h, 0, reach)
        agb_copy(h, 0, reach - 1, 0, j).wait_recv()
        agb_copy(h, 1, reach - 1, 1, j).wait_recv()
        use(h, j)

    mean_sq = jnp.sum(sumsq[...], axis=1, keepdims=True) * (1.0 / width)
    factor = lax.rsqrt(mean_sq + 1e-05)

    def branch(base, scale_ref, pick):
        part = acc[:, pl.ds(base, slots)]
        scale = jnp.concatenate([scale_ref[...], jnp.zeros((1, slots - hidden), F32)], axis=1)
        added = jnp.dot(
            part, pick[...], precision=lax.Precision.HIGHEST, preferred_element_type=F32
        )
        return (part * scale + added) * factor

    gate = branch(0, gscale_ref, gpick)
    up = branch(slots, uscale_ref, upick)
    hid[1] = (gate / (1.0 + jnp.exp(-gate)) * up).astype(BF16)
    hid[0] = dot(perm[...], hid[1]).astype(BF16)
    for h in (0, 1):
        added = dot_nt(hid[h], dextp[...])
        high = added.astype(BF16)
        low = (added - high.astype(F32)).astype(BF16)
        lane = lax.broadcasted_iota(jnp.int32, added.shape, 1)
        extra_parts[h] = jnp.where(lane < k_out, high.astype(F32), low.astype(F32)).astype(BF16)
    loads[2].wait()

    def down(h, j, s):
        here = cols(h, j)
        some = pl.ds(pl.multiple_of(s * sub, sub), sub)
        base = dot(hid[h, some, :], wd[:, here]) * dscale_ref[:, here]
        return base + dot(extra_parts[h, some, :], onehot[:, here])

    def ring_copy(h, d, m):
        a = axes[h][0]
        return send(
            ring_s.at[h, d, m],
            ring_r.at[h, d, m + 2],
            ring_ss.at[h, d, m],
            ring_rs.at[h, d, m],
            a,
            at(a, 1 - 2 * d),
        )

    def ring_step(m, carry):
        away = lax.div(n - m, 2)
        for h in (0, 1):
            for d in (0, 1):
                odd = lax.rem(m, 2)
                s = odd if d == 0 else 1 - odd
                shift = n - away if d else away
                j = lax.rem(pos[axes[h][0]] + shift, n)
                value = down(h, j, s)

                @pl.when(m >= 2)
                def _():
                    ring_copy(h, d, m - 2).wait_recv()

                ring_s[h, d, m] = (value + ring_r[h, d, m].astype(F32)).astype(BF16)
                ring_copy(h, d, m).start()
        return carry

    lax.fori_loop(0, n - 1, ring_step, 0)

    def two_copy(h, r):
        b = axes[h][1]
        away = pl.ds(pl.multiple_of(at(b, r) * block, block), block)
        return send(
            t_half.at[h, away, :], r_two.at[h, r], two_ss.at[h, r], two_rs.at[h, r], b, at(b, r)
        )

    for h in (0, 1):
        for r in range(1, n):
            one_copy(h, r).wait_send()
        for s in (0, 1):
            t_sum[h, pl.ds(s * sub, sub), :] = down(h, pos[axes[h][0]], s)
    for h in (0, 1):
        for d in (0, 1):
            for m in (n - 3, n - 2):
                ring_copy(h, d, m).wait_recv()
        for s in (0, 1):
            some = pl.ds(s * sub, sub)
            plus = ring_r[h, 0, n - s].astype(F32)
            minus = ring_r[h, 1, n - 1 + s].astype(F32)
            total = t_sum[h, some, :] + plus + minus
            t_sum[h, some, :] = total
            t_half[h, some, :] = total.astype(BF16)
        for r in offsets:
            two_copy(h, r).start()

    def out_copy(h, r, sender):
        a = axes[h][0]
        return send(
            out_s.at[h, at(a, r)],
            out_ref.at[:, cols(h, sender)],
            out_ss.at[h, r],
            out_rs.at[h, r],
            a,
            at(a, r),
        )

    for h in (0, 1):
        a, b = axes[h]
        own = pl.ds(pl.multiple_of(pos[b] * block, block), block)
        total = t_sum[h, own, :] + mixed[h]
        for r in range(1, n):
            two_copy(h, r).wait_recv()
            total += r_two[h, r].astype(F32)
        mixed[h] = total
        for j in range(n):
            out_s[h, j] = mixed[h, pl.ds(j * rows, rows), :].astype(BF16)
        for r in offsets:
            out_copy(h, r, pos[a]).start()
        out_ref[:, cols(h, pos[a])] = out_s[h, pos[a]]

    for h in (0, 1):
        a, b = axes[h]
        for r in range(1, n):
            heads_copy(h, r, pos[a]).wait_send()
            w_copy(h, r, pos[a]).wait_send()
            strm_copy(h, r, pos[a]).wait_send()
            aga_copy(h, r, pos[b]).wait_send()
            two_copy(h, r).wait_send()
        for d in (0, 1):
            for k in range(reach):
                for s in (0, 1):
                    if k < reach - 1 or s == d:
                        agb_copy(h, d, k, s, behind(h, d, k)).wait_send()
            for m in range(n - 1):
                ring_copy(h, d, m).wait_send()
    for h in (0, 1):
        a = axes[h][0]
        for r in range(1, n):
            out_copy(h, r, pos[a]).wait_send()
            out_copy(h, r, at(a, -r)).wait_recv()


def local(n, *args):
    (
        heads_out,
        stream_in,
        proj_levels,
        proj_scale,
        norm_gain,
        gate_levels,
        gate_scale,
        gate_index,
        gate_extra,
        up_levels,
        up_scale,
        up_index,
        up_extra,
        down_levels,
        down_scale,
        down_index,
        down_extra,
    ) = args
    tokens, feats = heads_out.shape
    rows, width = stream_in.shape
    hidden = gate_levels.shape[1]
    k_out = gate_extra.shape[1]
    slots = -(-(hidden + k_out) // 128) * 128
    strip = width // 2 // n
    block = tokens // n
    sub = tokens // 2
    reach = n // 2
    vmem = pl.BlockSpec(memory_space=pltpu.VMEM)
    smem = pl.BlockSpec(memory_space=pltpu.SMEM)
    hbm = pl.BlockSpec(memory_space=pl.ANY)
    dma = pltpu.SemaphoreType.DMA
    scratch = [
        pltpu.VMEM((2 * slots, width), BF16),
        pltpu.VMEM((slots, width), BF16),
        pltpu.VMEM((128, width), BF16),
        pltpu.VMEM((tokens, tokens), BF16),
        pltpu.VMEM((slots, slots), F32),
        pltpu.VMEM((slots, slots), F32),
        pltpu.VMEM((128, slots), BF16),
        pltpu.VMEM((1, width), F32),
        pltpu.VMEM((2, n * feats, tokens), BF16),
        pltpu.VMEM((2, n * feats, strip), BF16),
        pltpu.VMEM((2, n, rows, strip), BF16),
        pltpu.VMEM((2, tokens, strip), F32),
        pltpu.VMEM((2, tokens, strip), BF16),
        pltpu.VMEM((2, n, block, strip), BF16),
        pltpu.VMEM((2, block, strip), F32),
        pltpu.VMEM((2, n, tokens, strip), BF16),
        pltpu.VMEM((tokens, 2 * slots), F32),
        pltpu.VMEM((tokens, 128), F32),
        pltpu.VMEM((2, tokens, slots), BF16),
        pltpu.VMEM((2, tokens, 128), BF16),
        pltpu.VMEM((2, 2, n - 1, sub, strip), BF16),
        pltpu.VMEM((2, 2, n + 1, sub, strip), BF16),
        pltpu.VMEM((2, n, block, strip), BF16),
        pltpu.VMEM((2, n, rows, strip), BF16),
        dma((5,)),
    ]
    for _ in range(5):
        scratch += [dma((2, n)), dma((2, n))]
    scratch += [dma((2, 2, reach, 2)), dma((2, 2, reach, 2))]
    scratch += [dma((2, 2, n - 1)), dma((2, 2, n - 1))]
    scratch += [dma((2, n)), dma((2, n)), dma((2, n)), dma((2, n))]
    return pl.pallas_call(
        functools.partial(kernel, n),
        out_shape=jax.ShapeDtypeStruct((rows, width), BF16),
        in_specs=[
            vmem, vmem, hbm, vmem, vmem, hbm, vmem, smem, vmem, hbm, vmem, smem, vmem, hbm, vmem, smem, vmem,
        ],
        out_specs=vmem,
        scratch_shapes=scratch,
        compiler_params=pltpu.CompilerParams(
            collective_id=0, has_side_effects=True, vmem_limit_bytes=60 * 1024 * 1024
        ),
    )(
        heads_out.T,
        stream_in,
        proj_levels,
        proj_scale[None, :],
        norm_gain[None, :],
        gate_levels.T,
        gate_scale[None, :],
        gate_index,
        gate_extra.T,
        up_levels.T,
        up_scale[None, :],
        up_index,
        up_extra.T,
        down_levels,
        down_scale[None, :],
        down_index,
        down_extra.T,
    )


def solution(mesh):
    n = math.isqrt(mesh.shape["tensor"])
    torus = Mesh(
        mesh.devices.reshape(mesh.shape["groups"], n, n, mesh.shape["seq"]),
        ("groups", "tensor_0", "tensor_1", "seq"),
    )
    return jax.shard_map(
        functools.partial(local, n),
        mesh=torus,
        in_specs=(
            P(("groups", "seq"), TENSOR),
            P(GROUPS_SEQ_TENSOR, None),
            P(TENSOR, None),
            P(),
            P(),
            P(None, TENSOR),
            P(TENSOR),
            P(TENSOR, None),
            P(None, TENSOR),
            P(None, TENSOR),
            P(TENSOR),
            P(TENSOR, None),
            P(None, TENSOR),
            P(TENSOR, None),
            P(),
            P(TENSOR, None),
            P(TENSOR, None),
        ),
        out_specs=P(GROUPS_SEQ_TENSOR, None),
        check_vma=False,
    )
```

```python
import functools
import math

import jax
import jax.numpy as jnp
from jax import lax
from jax.experimental import pallas as pl
from jax.experimental.pallas import tpu as pltpu
from jax.sharding import Mesh
from jax.sharding import PartitionSpec as P

TENSOR = ("tensor_0", "tensor_1")
GROUPS_SEQ_TENSOR = ("groups", "seq", "tensor_0", "tensor_1")
MESH = pl.DeviceIdType.MESH
F32 = jnp.float32
BF16 = jnp.bfloat16
NT = (((1,), (1,)), ((), ()))


def dot(a, b):
    return jnp.dot(a, b, preferred_element_type=F32)


def dot_nt(a, b):
    return lax.dot_general(a, b, NT, preferred_element_type=F32)


def kernel(
    n,
    cores,
    heads_ref,
    stream_ref,
    projw_ref,
    pscale_in,
    gain_in,
    gatew_ref,
    gscale_in,
    gidx_in,
    gext_in,
    upw_ref,
    uscale_in,
    uidx_in,
    uext_in,
    downw_ref,
    dscale_in,
    didx_in,
    dext_in,
    out_ref,
    pscale_ref,
    gain_ref,
    gscale_ref,
    gidx_ref,
    gext_ref,
    uscale_ref,
    uidx_ref,
    uext_ref,
    dscale_ref,
    didx_ref,
    dext_ref,
    wcat,
    wd,
    onehot,
    perm,
    gpick,
    upick,
    dextp,
    invg,
    heads_all,
    w_all,
    strm,
    t_sum,
    t_half,
    r_one,
    mixed,
    y_all,
    acc,
    sumsq,
    hid,
    extra_parts,
    ring_s,
    ring_r,
    r_two,
    out_s,
    load_sem,
    heads_ss,
    heads_rs,
    w_ss,
    w_rs,
    share_ss,
    share_rs,
    strm_ss,
    strm_rs,
    one_ss,
    one_rs,
    aga_ss,
    aga_rs,
    agb_ss,
    agb_rs,
    ring_ss,
    ring_rs,
    two_ss,
    two_rs,
    out_ss,
    out_rs,
):
    feats, tokens = heads_ref.shape
    width = projw_ref.shape[1]
    hidden = gatew_ref.shape[0]
    part = w_all.shape[2] // cores
    rows = stream_ref.shape[0]
    slots = gpick.shape[0]
    k_out = gext_ref.shape[0]
    half = width // 2
    strip = half // n
    block = tokens // n
    sub = tokens // 2
    reach = n // 2
    axes = (("tensor_0", "tensor_1"), ("tensor_1", "tensor_0"))
    pos = {name: lax.axis_index(name) for name in TENSOR}
    offsets = sorted(range(1, n), key=lambda r: -min(r, n - r))

    def at(name, shift):
        return lax.rem(pos[name] + (shift + n) % n, n)

    def cols(h, j):
        return pl.ds(pl.multiple_of(h * half + j * strip, strip), strip)

    def send(src, dst, ssem, rsem, name, target):
        return pltpu.make_async_remote_copy(
            src_ref=src,
            dst_ref=dst,
            send_sem=ssem,
            recv_sem=rsem,
            device_id={name: target},
            device_id_type=MESH,
        )

    def all_but_one(ref, ssem, rsem, name):
        return send(ref, ref, ssem, rsem, name, at(name, 1))

    core = lax.axis_index("seq")
    barrier = pltpu.get_barrier_semaphore()
    for name in TENSOR:
        for r in range(1, n):
            pl.semaphore_signal(
                barrier, inc=1, device_id={name: at(name, r)}, device_id_type=MESH
            )
    for q in range(1, cores):
        pl.semaphore_signal(
            barrier, inc=1, device_id={"seq": lax.rem(core + q, cores)}, device_id_type=MESH
        )

    def place(sender):
        return pl.ds(pl.multiple_of(sender * feats, feats), feats)

    mine = pl.ds(pl.multiple_of(core * part, part), part)

    def own_part(h, j):
        return pl.ds(pl.multiple_of(h * half + j * strip + core * part, part), part)

    first = []
    for h in (0, 1):
        me = pos[axes[h][0]]
        for src, dst in (
            (heads_ref, heads_all.at[h, place(me), :]),
            (projw_ref.at[:, own_part(h, me)], w_all.at[h, place(me), mine]),
            (stream_ref.at[:, cols(h, me)], strm.at[h, me]),
        ):
            first.append(pltpu.make_async_copy(src, dst, load_sem.at[len(first)]))
            first[-1].start()
    pl.semaphore_wait(barrier, 2 * (n - 1) + cores - 1)

    def heads_copy(h, r):
        a = axes[h][0]
        there = heads_all.at[h, place(pos[a]), :]
        return send(there, there, heads_ss.at[h], heads_rs.at[h], a, at(a, r))

    def w_copy(h, r):
        a = axes[h][0]
        return send(
            projw_ref.at[:, own_part(h, at(a, r))],
            w_all.at[h, place(pos[a]), mine],
            w_ss.at[h],
            w_rs.at[h],
            a,
            at(a, r),
        )

    def share_copy(h, q):
        there = w_all.at[h, :, mine]
        return send(
            there, there, share_ss.at[h, q], share_rs.at[h, q], "seq", lax.rem(core + q, cores)
        )

    def strm_copy(h, r):
        a = axes[h][0]
        return send(
            stream_ref.at[:, cols(h, at(a, r))],
            strm.at[h, pos[a]],
            strm_ss.at[h],
            strm_rs.at[h],
            a,
            at(a, r),
        )

    for r in offsets:
        for h in (0, 1):
            w_copy(h, r).start()
    for h in (0, 1):
        first[3 * h].wait()
    for r in offsets:
        for h in (0, 1):
            heads_copy(h, r).start()
    for r in offsets:
        for h in (0, 1):
            strm_copy(h, r).start()
    small = []
    for src, dst in (
        (pscale_in, pscale_ref),
        (gain_in, gain_ref),
        (gscale_in, gscale_ref),
        (gidx_in, gidx_ref),
        (gext_in, gext_ref),
        (uscale_in, uscale_ref),
        (uidx_in, uidx_ref),
        (uext_in, uext_ref),
        (dscale_in, dscale_ref),
        (didx_in, didx_ref),
        (dext_in, dext_ref),
    ):
        small.append(pltpu.make_async_copy(src, dst, load_sem.at[6 + len(small)]))
        small[-1].start()
    base = 6 + len(small)
    loads = [
        pltpu.make_async_copy(gatew_ref, wcat.at[pl.ds(0, hidden), :], load_sem.at[base]),
        pltpu.make_async_copy(upw_ref, wcat.at[pl.ds(slots, hidden), :], load_sem.at[base + 1]),
        pltpu.make_async_copy(downw_ref, wd.at[pl.ds(0, hidden), :], load_sem.at[base + 2]),
    ]
    for load in loads:
        load.start()

    for copy in small:
        copy.wait()
    r_i = lax.broadcasted_iota(jnp.int32, (tokens, tokens), 0)
    c_i = lax.broadcasted_iota(jnp.int32, (tokens, tokens), 1)
    swapped = (
        lax.rem(lax.div(r_i, rows), n) * block + lax.div(r_i, block) * rows + lax.rem(r_i, rows)
    )
    perm[...] = jnp.where(c_i == swapped, 1.0, 0.0).astype(BF16)

    def index_column(idx_ref, count):
        row = lax.rem(lax.broadcasted_iota(jnp.int32, (count, 1), 0), k_out)
        column = jnp.zeros((count, 1), jnp.int32)
        for k in range(k_out):
            column = jnp.where(row == k, idx_ref[0, k], column)
        return column

    for pick, idx_ref in ((gpick, gidx_ref), (upick, uidx_ref)):
        pick[...] = jnp.zeros_like(pick)
        chosen = lax.broadcasted_iota(jnp.int32, (k_out, slots), 1) == index_column(idx_ref, k_out)
        pick[pl.ds(hidden, k_out), :] = jnp.where(chosen, 1.0, 0.0)

    one_rows = onehot.shape[0]
    didx = index_column(didx_ref, one_rows)
    live = lax.broadcasted_iota(jnp.int32, (one_rows, strip), 0) < 2 * k_out

    def prepare(j, carry):
        here = pl.ds(pl.multiple_of(j * strip, strip), strip)
        column = lax.broadcasted_iota(jnp.int32, (one_rows, strip), 1) + j * strip
        onehot[:, here] = jnp.where((column == didx) & live, 1.0, 0.0).astype(BF16)
        blank = jnp.zeros((slots - hidden - k_out, strip), F32)
        for base, ext in ((0, gext_ref), (slots, uext_ref)):
            filled = jnp.concatenate([ext[:, here].astype(F32), blank], axis=0)
            wcat[pl.ds(base + hidden, slots - hidden), here] = filled.astype(BF16)
        wd[pl.ds(hidden, slots - hidden), here] = jnp.zeros((slots - hidden, strip), BF16)
        invg[:, here] = 1.0 / gain_ref[:, here]
        return carry

    lax.fori_loop(0, width // strip, prepare, 0)
    dext = jnp.concatenate([dext_ref[...].astype(F32)] * 2, axis=0)
    dext = jnp.concatenate([dext, jnp.zeros((dextp.shape[0] - 2 * k_out, hidden), F32)], axis=0)
    dextp[...] = jnp.zeros_like(dextp)
    dextp[:, pl.ds(0, hidden)] = dext.astype(BF16)
    acc[...] = jnp.zeros_like(acc)
    sumsq[...] = jnp.zeros_like(sumsq)
    for h in (0, 1):
        for d in (0, 1):
            for m in (0, 1):
                ring_r[h, d, m] = jnp.zeros((sub, strip), BF16)

    def one_copy(h, r):
        b = axes[h][1]
        away = pl.ds(pl.multiple_of(at(b, r) * block, block), block)
        return send(
            t_half.at[h, away, :], r_one.at[h, r - 1], one_ss.at[h], one_rs.at[h], b, at(b, r)
        )

    seen_w = pl.ds(0, (n - 1) * feats)
    seen_b = pl.ds(0, (n - 1) * block)
    for h in (0, 1):
        first[3 * h + 1].wait()
        all_but_one(w_all.at[h, seen_w, mine], w_ss.at[h], w_rs.at[h], axes[h][0]).wait_recv()
        for q in range(1, cores):
            share_copy(h, q).start()
    for h in (0, 1):
        a = axes[h][0]
        all_but_one(heads_all.at[h, seen_w, :], heads_ss.at[h], heads_rs.at[h], a).wait_recv()
        for q in range(1, cores):
            share_copy(h, q).wait_recv()
        if h == 0:
            turn = perm[...]
        else:
            turn = jnp.where(r_i == c_i, 1.0, 0.0).astype(BF16)
        ordered = dot_nt(turn, heads_all[h]).astype(BF16)
        t_sum[h] = dot(ordered, w_all[h])
        t_half[h] = t_sum[h].astype(BF16)
        for r in offsets:
            one_copy(h, r).start()

    def aga_copy(h, r, owner):
        a, b = axes[h]
        there = y_all.at[h, pos[a], pl.ds(pl.multiple_of(owner * block, block), block), :]
        return send(there, there, aga_ss.at[h], aga_rs.at[h], b, at(b, r))

    for h in (0, 1):
        a, b = axes[h]
        here = cols(h, pos[a])
        own = pl.ds(pl.multiple_of(pos[b] * block, block), block)
        total = t_sum[h, own, :]
        all_but_one(r_one.at[h], one_ss.at[h], one_rs.at[h], b).wait_recv()
        for r in range(1, n):
            total += r_one[h, r - 1].astype(F32)
        mixed[h] = total * pscale_ref[:, here]
        first[3 * h + 2].wait()
        all_but_one(strm.at[h, pl.ds(0, n - 1)], strm_ss.at[h], strm_rs.at[h], a).wait_recv()
        for j in range(n):
            few = pl.ds(j * rows, rows)
            mixed[h, few, :] = mixed[h, few, :] + strm[h, j].astype(F32)
        y_all[h, pos[a], own, :] = (mixed[h] * gain_ref[:, here]).astype(BF16)
        for r in offsets:
            aga_copy(h, r, pos[b]).start()

    def agb_copy(h, d, k, s, strip_id):
        a = axes[h][0]
        there = y_all.at[h, strip_id, pl.ds(s * sub, sub), :]
        return send(
            there, there, agb_ss.at[h, d, k, s], agb_rs.at[h, d, k, s], a, at(a, 1 - 2 * d)
        )

    def behind(h, d, k):
        shift = k if d else n - k
        return lax.rem(pos[axes[h][0]] + shift, n)

    def use(h, j):
        y = y_all[h, j]
        if h == 0:
            y = dot(perm[...], y).astype(BF16)
        here = cols(h, j)
        scaled = y.astype(F32) * invg[:, here]
        scaled = scaled * scaled
        lanes = sumsq.shape[1]
        part = scaled[:, :lanes]
        for q in range(1, strip // lanes):
            part += scaled[:, q * lanes : (q + 1) * lanes]
        sumsq[...] += part
        acc[...] += dot_nt(y, wcat[:, here])

    for h in (0, 1):
        a, b = axes[h]
        all_but_one(y_all.at[h, 0, seen_b, :], aga_ss.at[h], aga_rs.at[h], b).wait_recv()
        for step in (0, 1):
            for d in (0, 1):
                s = step if d == 0 else 1 - step
                agb_copy(h, d, 0, s, pos[a]).start()
    loads[0].wait()
    loads[1].wait()
    for h in (0, 1):
        use(h, pos[axes[h][0]])

    def gather_step(k, carry):
        for step in (0, 1):
            for h in (0, 1):
                for d in (0, 1):
                    s = step if d == 0 else 1 - step
                    j = behind(h, d, k)
                    agb_copy(h, d, k - 1, s, j).wait_recv()
                    if step == 0:
                        agb_copy(h, d, k, s, j).start()
                    else:

                        @pl.when(k < reach - 1)
                        def _():
                            agb_copy(h, d, k, s, j).start()

        for h in (0, 1):
            for d in (0, 1):
                use(h, behind(h, d, k))
        return carry

    lax.fori_loop(1, reach, gather_step, 0)
    for h in (0, 1):
        j = behind(h, 0, reach)
        agb_copy(h, 0, reach - 1, 0, j).wait_recv()
        agb_copy(h, 1, reach - 1, 1, j).wait_recv()
        use(h, j)

    mean_sq = jnp.sum(sumsq[...], axis=1, keepdims=True) * (1.0 / width)
    factor = lax.rsqrt(mean_sq + 1e-05)

    def branch(base, scale_ref, pick):
        part = acc[:, pl.ds(base, slots)]
        scale = jnp.concatenate([scale_ref[...], jnp.zeros((1, slots - hidden), F32)], axis=1)
        added = jnp.dot(
            part, pick[...], precision=lax.Precision.HIGHEST, preferred_element_type=F32
        )
        return (part * scale + added) * factor

    gate = branch(0, gscale_ref, gpick)
    up = branch(slots, uscale_ref, upick)
    hid[1] = (gate / (1.0 + jnp.exp(-gate)) * up).astype(BF16)
    hid[0] = dot(perm[...], hid[1]).astype(BF16)
    for h in (0, 1):
        added = dot_nt(hid[h], dextp[...])
        high = added.astype(BF16)
        low = (added - high.astype(F32)).astype(BF16)
        lane = lax.broadcasted_iota(jnp.int32, added.shape, 1)
        extra_parts[h] = jnp.where(lane < k_out, high.astype(F32), low.astype(F32)).astype(BF16)
    loads[2].wait()

    def down(h, j, s):
        here = cols(h, j)
        some = pl.ds(pl.multiple_of(s * sub, sub), sub)
        base = dot(hid[h, some, :], wd[:, here]) * dscale_ref[:, here]
        return base + dot(extra_parts[h, some, :], onehot[:, here])

    def ring_copy(h, d, m):
        a = axes[h][0]
        return send(
            ring_s.at[h, d, m],
            ring_r.at[h, d, m + 2],
            ring_ss.at[h, d, m],
            ring_rs.at[h, d, m],
            a,
            at(a, 1 - 2 * d),
        )

    def ring_step(m, carry):
        away = lax.div(n - m, 2)
        for h in (0, 1):
            for d in (0, 1):
                odd = lax.rem(m, 2)
                s = odd if d == 0 else 1 - odd
                shift = n - away if d else away
                j = lax.rem(pos[axes[h][0]] + shift, n)
                value = down(h, j, s)

                @pl.when(m >= 2)
                def _():
                    ring_copy(h, d, m - 2).wait_recv()

                ring_s[h, d, m] = (value + ring_r[h, d, m].astype(F32)).astype(BF16)
                ring_copy(h, d, m).start()
        return carry

    lax.fori_loop(0, n - 1, ring_step, 0)

    def two_copy(h, r):
        b = axes[h][1]
        away = pl.ds(pl.multiple_of(at(b, r) * block, block), block)
        return send(
            t_half.at[h, away, :], r_two.at[h, r - 1], two_ss.at[h], two_rs.at[h], b, at(b, r)
        )

    for h in (0, 1):
        all_but_one(r_one.at[h], one_ss.at[h], one_rs.at[h], axes[h][1]).wait_send()
        for s in (0, 1):
            t_sum[h, pl.ds(s * sub, sub), :] = down(h, pos[axes[h][0]], s)
    for h in (0, 1):
        for d in (0, 1):
            for m in (n - 3, n - 2):
                ring_copy(h, d, m).wait_recv()
        for s in (0, 1):
            some = pl.ds(s * sub, sub)
            plus = ring_r[h, 0, n - s].astype(F32)
            minus = ring_r[h, 1, n - 1 + s].astype(F32)
            total = t_sum[h, some, :] + plus + minus
            t_sum[h, some, :] = total
            t_half[h, some, :] = total.astype(BF16)
        for r in offsets:
            two_copy(h, r).start()

    def out_copy(h, r):
        a = axes[h][0]
        return send(
            out_s.at[h, at(a, r)],
            out_ref.at[:, cols(h, pos[a])],
            out_ss.at[h],
            out_rs.at[h],
            a,
            at(a, r),
        )

    last = []
    for h in (0, 1):
        a, b = axes[h]
        own = pl.ds(pl.multiple_of(pos[b] * block, block), block)
        total = t_sum[h, own, :] + mixed[h]
        all_but_one(r_two.at[h], two_ss.at[h], two_rs.at[h], b).wait_recv()
        for r in range(1, n):
            total += r_two[h, r - 1].astype(F32)
        mixed[h] = total
        for j in range(n):
            out_s[h, j] = mixed[h, pl.ds(j * rows, rows), :].astype(BF16)
        for r in offsets:
            out_copy(h, r).start()
        last.append(
            pltpu.make_async_copy(
                out_s.at[h, pos[a]], out_ref.at[:, cols(h, pos[a])], load_sem.at[3 * h]
            )
        )
        last[h].start()

    for h in (0, 1):
        a, b = axes[h]
        all_but_one(heads_all.at[h, seen_w, :], heads_ss.at[h], heads_rs.at[h], a).wait_send()
        all_but_one(w_all.at[h, seen_w, mine], w_ss.at[h], w_rs.at[h], a).wait_send()
        for q in range(1, cores):
            share_copy(h, q).wait_send()
        all_but_one(strm.at[h, pl.ds(0, n - 1)], strm_ss.at[h], strm_rs.at[h], a).wait_send()
        all_but_one(y_all.at[h, 0, seen_b, :], aga_ss.at[h], aga_rs.at[h], b).wait_send()
        all_but_one(r_two.at[h], two_ss.at[h], two_rs.at[h], b).wait_send()
        for d in (0, 1):
            for k in range(reach):
                for s in (0, 1):
                    if k < reach - 1 or s == d:
                        agb_copy(h, d, k, s, behind(h, d, k)).wait_send()
            for m in range(n - 1):
                ring_copy(h, d, m).wait_send()
    for h in (0, 1):
        a = axes[h][0]
        pieces = all_but_one(out_s.at[h, pl.ds(0, n - 1)], out_ss.at[h], out_rs.at[h], a)
        pieces.wait_send()
        pieces.wait_recv()
        last[h].wait()


def local(n, cores, *args):
    (
        heads_out,
        stream_in,
        proj_levels,
        proj_scale,
        norm_gain,
        gate_levels,
        gate_scale,
        gate_index,
        gate_extra,
        up_levels,
        up_scale,
        up_index,
        up_extra,
        down_levels,
        down_scale,
        down_index,
        down_extra,
    ) = args
    tokens, feats = heads_out.shape
    rows, width = stream_in.shape
    hidden = gate_levels.shape[1]
    k_out = gate_extra.shape[1]
    slots = -(-(hidden + k_out) // 128) * 128
    strip = width // 2 // n
    block = tokens // n
    sub = tokens // 2
    reach = n // 2
    index = pltpu.SMEM(gate_index.shape, jnp.int32)
    hbm = pl.BlockSpec(memory_space=pl.ANY)
    dma = pltpu.SemaphoreType.DMA
    scratch = [
        pltpu.VMEM((1, width), F32),
        pltpu.VMEM((1, width), F32),
        pltpu.VMEM((1, hidden), F32),
        index,
        pltpu.VMEM((k_out, width), BF16),
        pltpu.VMEM((1, hidden), F32),
        index,
        pltpu.VMEM((k_out, width), BF16),
        pltpu.VMEM((1, width), F32),
        index,
        pltpu.VMEM((k_out, hidden), BF16),
        pltpu.VMEM((2 * slots, width), BF16),
        pltpu.VMEM((slots, width), BF16),
        pltpu.VMEM((128, width), BF16),
        pltpu.VMEM((tokens, tokens), BF16),
        pltpu.VMEM((slots, slots), F32),
        pltpu.VMEM((slots, slots), F32),
        pltpu.VMEM((128, slots), BF16),
        pltpu.VMEM((1, width), F32),
        pltpu.VMEM((2, n * feats, tokens), BF16),
        pltpu.VMEM((2, n * feats, strip), BF16),
        pltpu.VMEM((2, n, rows, strip), BF16),
        pltpu.VMEM((2, tokens, strip), F32),
        pltpu.VMEM((2, tokens, strip), BF16),
        pltpu.VMEM((2, n - 1, block, strip), BF16),
        pltpu.VMEM((2, block, strip), F32),
        pltpu.VMEM((2, n, tokens, strip), BF16),
        pltpu.VMEM((tokens, 2 * slots), F32),
        pltpu.VMEM((tokens, 128), F32),
        pltpu.VMEM((2, tokens, slots), BF16),
        pltpu.VMEM((2, tokens, 128), BF16),
        pltpu.VMEM((2, 2, n - 1, sub, strip), BF16),
        pltpu.VMEM((2, 2, n + 1, sub, strip), BF16),
        pltpu.VMEM((2, n - 1, block, strip), BF16),
        pltpu.VMEM((2, n, rows, strip), BF16),
        dma((20,)),
    ]
    scratch += [dma((2,)), dma((2,)), dma((2,)), dma((2,)), dma((2, cores)), dma((2, cores))]
    scratch += [dma((2,)) for _ in range(6)]
    scratch += [dma((2, 2, reach, 2)), dma((2, 2, reach, 2))]
    scratch += [dma((2, 2, n - 1)), dma((2, 2, n - 1))]
    scratch += [dma((2,)) for _ in range(4)]
    return pl.pallas_call(
        functools.partial(kernel, n, cores),
        out_shape=jax.ShapeDtypeStruct((rows, width), BF16),
        in_specs=[hbm] * len(args),
        out_specs=hbm,
        scratch_shapes=scratch,
        compiler_params=pltpu.CompilerParams(
            collective_id=0, has_side_effects=True, vmem_limit_bytes=60 * 1024 * 1024
        ),
    )(
        heads_out.T,
        stream_in,
        proj_levels,
        proj_scale[None, :],
        norm_gain[None, :],
        gate_levels.T,
        gate_scale[None, :],
        gate_index,
        gate_extra.T,
        up_levels.T,
        up_scale[None, :],
        up_index,
        up_extra.T,
        down_levels,
        down_scale[None, :],
        down_index,
        down_extra.T,
    )


def solution(mesh):
    n = math.isqrt(mesh.shape["tensor"])
    torus = Mesh(
        mesh.devices.reshape(mesh.shape["groups"], n, n, mesh.shape["seq"]),
        ("groups", "tensor_0", "tensor_1", "seq"),
    )
    return jax.shard_map(
        functools.partial(local, n, mesh.shape["seq"]),
        mesh=torus,
        in_specs=(
            P(("groups", "seq"), TENSOR),
            P(GROUPS_SEQ_TENSOR, None),
            P(TENSOR, None),
            P(),
            P(),
            P(None, TENSOR),
            P(TENSOR),
            P(TENSOR, None),
            P(None, TENSOR),
            P(None, TENSOR),
            P(TENSOR),
            P(TENSOR, None),
            P(None, TENSOR),
            P(TENSOR, None),
            P(),
            P(TENSOR, None),
            P(TENSOR, None),
        ),
        out_specs=P(GROUPS_SEQ_TENSOR, None),
        check_vma=False,
    )
```

```python
import functools
import math

import jax
import jax.numpy as jnp
from jax import lax
from jax.experimental import pallas as pl
from jax.experimental.pallas import tpu as pltpu
from jax.sharding import Mesh
from jax.sharding import PartitionSpec as P

TENSOR = ("tensor_0", "tensor_1")
GROUPS_SEQ_TENSOR = ("groups", "seq", "tensor_0", "tensor_1")
MESH = pl.DeviceIdType.MESH
F32 = jnp.float32
BF16 = jnp.bfloat16
NT = (((1,), (1,)), ((), ()))


def dot(a, b):
    return jnp.dot(a, b, preferred_element_type=F32)


def dot_nt(a, b):
    return lax.dot_general(a, b, NT, preferred_element_type=F32)


def kernel(
    n,
    cores,
    heads_ref,
    stream_ref,
    projw_ref,
    pscale_in,
    gain_in,
    gatew_ref,
    gscale_in,
    gidx_in,
    gext_in,
    upw_ref,
    uscale_in,
    uidx_in,
    uext_in,
    downw_ref,
    dscale_in,
    didx_in,
    dext_in,
    out_ref,
    pscale_ref,
    gain_ref,
    gscale_ref,
    gidx_ref,
    gext_ref,
    uscale_ref,
    uidx_ref,
    uext_ref,
    dscale_ref,
    didx_ref,
    dext_ref,
    wcat,
    wd,
    onehot,
    perm,
    gpick,
    upick,
    dextp,
    invg,
    heads_all,
    w_all,
    strm,
    t_sum,
    t_half,
    r_one,
    mixed,
    y_all,
    acc,
    sumsq,
    hid,
    extra_parts,
    ring_s,
    ring_r,
    two_s,
    r_two,
    mix_s,
    mix_r,
    down_sum,
    out_v,
    load_sem,
    heads_ss,
    heads_rs,
    w_ss,
    w_rs,
    share_ss,
    share_rs,
    strm_ss,
    strm_rs,
    one_ss,
    one_rs,
    aga_ss,
    aga_rs,
    agb_ss,
    agb_rs,
    ring_ss,
    ring_rs,
    two_ss,
    two_rs,
    mix_ss,
    mix_rs,
):
    feats, tokens = heads_ref.shape
    width = projw_ref.shape[1]
    hidden = gatew_ref.shape[0]
    part = w_all.shape[2] // cores
    rows = stream_ref.shape[0]
    slots = gpick.shape[0]
    k_out = gext_ref.shape[0]
    half = width // 2
    strip = half // n
    block = tokens // n
    sub = tokens // 2
    wide = half // 2
    reach = n // 2
    axes = (("tensor_0", "tensor_1"), ("tensor_1", "tensor_0"))
    pos = {name: lax.axis_index(name) for name in TENSOR}
    offsets = sorted(range(1, n), key=lambda r: -min(r, n - r))

    def at(name, shift):
        return lax.rem(pos[name] + (shift + n) % n, n)

    def cols(h, j):
        return pl.ds(pl.multiple_of(h * half + j * strip, strip), strip)

    def send(src, dst, ssem, rsem, name, target):
        return pltpu.make_async_remote_copy(
            src_ref=src,
            dst_ref=dst,
            send_sem=ssem,
            recv_sem=rsem,
            device_id={name: target},
            device_id_type=MESH,
        )

    def all_but_one(ref, ssem, rsem, name):
        return send(ref, ref, ssem, rsem, name, at(name, 1))

    core = lax.axis_index("seq")
    barrier = pltpu.get_barrier_semaphore()
    for name in TENSOR:
        for r in range(1, n):
            pl.semaphore_signal(
                barrier, inc=1, device_id={name: at(name, r)}, device_id_type=MESH
            )
    for q in range(1, cores):
        pl.semaphore_signal(
            barrier, inc=1, device_id={"seq": lax.rem(core + q, cores)}, device_id_type=MESH
        )

    def place(sender):
        return pl.ds(pl.multiple_of(sender * feats, feats), feats)

    mine = pl.ds(pl.multiple_of(core * part, part), part)

    def own_part(h, j):
        return pl.ds(pl.multiple_of(h * half + j * strip + core * part, part), part)

    first = []
    for h in (0, 1):
        me = pos[axes[h][0]]
        for src, dst in (
            (heads_ref, heads_all.at[h, place(me), :]),
            (projw_ref.at[:, own_part(h, me)], w_all.at[h, place(me), mine]),
            (stream_ref.at[:, cols(h, me)], strm.at[h, me]),
        ):
            first.append(pltpu.make_async_copy(src, dst, load_sem.at[len(first)]))
            first[-1].start()
    pl.semaphore_wait(barrier, 2 * (n - 1) + cores - 1)

    def heads_copy(h, r):
        a = axes[h][0]
        there = heads_all.at[h, place(pos[a]), :]
        return send(there, there, heads_ss.at[h], heads_rs.at[h], a, at(a, r))

    def w_copy(h, r):
        a = axes[h][0]
        return send(
            projw_ref.at[:, own_part(h, at(a, r))],
            w_all.at[h, place(pos[a]), mine],
            w_ss.at[h],
            w_rs.at[h],
            a,
            at(a, r),
        )

    def share_copy(h, q):
        there = w_all.at[h, :, mine]
        return send(
            there, there, share_ss.at[h, q], share_rs.at[h, q], "seq", lax.rem(core + q, cores)
        )

    def strm_copy(h, r):
        a = axes[h][0]
        return send(
            stream_ref.at[:, cols(h, at(a, r))],
            strm.at[h, pos[a]],
            strm_ss.at[h],
            strm_rs.at[h],
            a,
            at(a, r),
        )

    for r in offsets:
        for h in (0, 1):
            w_copy(h, r).start()
    for h in (0, 1):
        first[3 * h].wait()
    for r in offsets:
        for h in (0, 1):
            heads_copy(h, r).start()
    for r in offsets:
        for h in (0, 1):
            strm_copy(h, r).start()
    small = []
    for src, dst in (
        (pscale_in, pscale_ref),
        (gain_in, gain_ref),
        (gscale_in, gscale_ref),
        (gidx_in, gidx_ref),
        (gext_in, gext_ref),
        (uscale_in, uscale_ref),
        (uidx_in, uidx_ref),
        (uext_in, uext_ref),
        (dscale_in, dscale_ref),
        (didx_in, didx_ref),
        (dext_in, dext_ref),
    ):
        small.append(pltpu.make_async_copy(src, dst, load_sem.at[6 + len(small)]))
        small[-1].start()
    base = 6 + len(small)
    loads = [
        pltpu.make_async_copy(gatew_ref, wcat.at[pl.ds(0, hidden), :], load_sem.at[base]),
        pltpu.make_async_copy(upw_ref, wcat.at[pl.ds(slots, hidden), :], load_sem.at[base + 1]),
        pltpu.make_async_copy(downw_ref, wd.at[pl.ds(0, hidden), :], load_sem.at[base + 2]),
    ]
    for load in loads:
        load.start()

    for copy in small:
        copy.wait()
    r_i = lax.broadcasted_iota(jnp.int32, (tokens, tokens), 0)
    c_i = lax.broadcasted_iota(jnp.int32, (tokens, tokens), 1)
    swapped = (
        lax.rem(lax.div(r_i, rows), n) * block + lax.div(r_i, block) * rows + lax.rem(r_i, rows)
    )
    perm[...] = jnp.where(c_i == swapped, 1.0, 0.0).astype(BF16)

    def index_column(idx_ref, count):
        row = lax.rem(lax.broadcasted_iota(jnp.int32, (count, 1), 0), k_out)
        column = jnp.zeros((count, 1), jnp.int32)
        for k in range(k_out):
            column = jnp.where(row == k, idx_ref[0, k], column)
        return column

    for pick, idx_ref in ((gpick, gidx_ref), (upick, uidx_ref)):
        pick[...] = jnp.zeros_like(pick)
        chosen = lax.broadcasted_iota(jnp.int32, (k_out, slots), 1) == index_column(idx_ref, k_out)
        pick[pl.ds(hidden, k_out), :] = jnp.where(chosen, 1.0, 0.0)

    one_rows = onehot.shape[0]
    didx = index_column(didx_ref, one_rows)
    live = lax.broadcasted_iota(jnp.int32, (one_rows, strip), 0) < 2 * k_out

    def prepare(j, carry):
        here = pl.ds(pl.multiple_of(j * strip, strip), strip)
        column = lax.broadcasted_iota(jnp.int32, (one_rows, strip), 1) + j * strip
        onehot[:, here] = jnp.where((column == didx) & live, 1.0, 0.0).astype(BF16)
        blank = jnp.zeros((slots - hidden - k_out, strip), F32)
        for base, ext in ((0, gext_ref), (slots, uext_ref)):
            filled = jnp.concatenate([ext[:, here].astype(F32), blank], axis=0)
            wcat[pl.ds(base + hidden, slots - hidden), here] = filled.astype(BF16)
        wd[pl.ds(hidden, slots - hidden), here] = jnp.zeros((slots - hidden, strip), BF16)
        invg[:, here] = 1.0 / gain_ref[:, here]
        return carry

    lax.fori_loop(0, width // strip, prepare, 0)
    dext = jnp.concatenate([dext_ref[...].astype(F32)] * 2, axis=0)
    dext = jnp.concatenate([dext, jnp.zeros((dextp.shape[0] - 2 * k_out, hidden), F32)], axis=0)
    dextp[...] = jnp.zeros_like(dextp)
    dextp[:, pl.ds(0, hidden)] = dext.astype(BF16)
    acc[...] = jnp.zeros_like(acc)
    sumsq[...] = jnp.zeros_like(sumsq)
    for h in (0, 1):
        for d in (0, 1):
            for m in (0, 1):
                ring_r[h, d, m] = jnp.zeros((block, wide), BF16)

    def one_copy(h, r):
        b = axes[h][1]
        away = pl.ds(pl.multiple_of(at(b, r) * block, block), block)
        return send(
            t_half.at[h, away, :], r_one.at[h, r - 1], one_ss.at[h], one_rs.at[h], b, at(b, r)
        )

    seen_w = pl.ds(0, (n - 1) * feats)
    seen_b = pl.ds(0, (n - 1) * block)
    for h in (0, 1):
        first[3 * h + 1].wait()
        all_but_one(w_all.at[h, seen_w, mine], w_ss.at[h], w_rs.at[h], axes[h][0]).wait_recv()
        for q in range(1, cores):
            share_copy(h, q).start()
    for h in (0, 1):
        a = axes[h][0]
        all_but_one(heads_all.at[h, seen_w, :], heads_ss.at[h], heads_rs.at[h], a).wait_recv()
        for q in range(1, cores):
            share_copy(h, q).wait_recv()
        if h == 0:
            turn = perm[...]
        else:
            turn = jnp.where(r_i == c_i, 1.0, 0.0).astype(BF16)
        ordered = dot_nt(turn, heads_all[h]).astype(BF16)
        t_sum[h] = dot(ordered, w_all[h])
        t_half[h] = t_sum[h].astype(BF16)
        for r in offsets:
            one_copy(h, r).start()

    def aga_copy(h, r, owner):
        a, b = axes[h]
        there = y_all.at[h, pos[a], pl.ds(pl.multiple_of(owner * block, block), block), :]
        return send(there, there, aga_ss.at[h], aga_rs.at[h], b, at(b, r))

    def mix_copy(h, r):
        a = axes[h][0]
        there = mix_r.at[h, :, pl.ds(pl.multiple_of(pos[a] * strip, strip), strip)]
        return send(mix_s.at[h, at(a, r)], there, mix_ss.at[h], mix_rs.at[h], a, at(a, r))

    for h in (0, 1):
        a, b = axes[h]
        here = cols(h, pos[a])
        own = pl.ds(pl.multiple_of(pos[b] * block, block), block)
        total = t_sum[h, own, :]
        all_but_one(r_one.at[h], one_ss.at[h], one_rs.at[h], b).wait_recv()
        for r in range(1, n):
            total += r_one[h, r - 1].astype(F32)
        mixed[h] = total * pscale_ref[:, here]
        first[3 * h + 2].wait()
        all_but_one(strm.at[h, pl.ds(0, n - 1)], strm_ss.at[h], strm_rs.at[h], a).wait_recv()
        for j in range(n):
            few = pl.ds(j * rows, rows)
            mixed[h, few, :] = mixed[h, few, :] + strm[h, j].astype(F32)
        y_all[h, pos[a], own, :] = (mixed[h] * gain_ref[:, here]).astype(BF16)
        for r in offsets:
            aga_copy(h, r, pos[b]).start()
        for j in range(n):
            mix_s[h, j] = mixed[h, pl.ds(j * rows, rows), :]
    for h in (0, 1):
        me = pos[axes[h][0]]
        for r in offsets:
            mix_copy(h, r).start()
        mix_r[h, :, pl.ds(pl.multiple_of(me * strip, strip), strip)] = mix_s[h, me]

    def agb_copy(h, d, k, s, strip_id):
        a = axes[h][0]
        there = y_all.at[h, strip_id, pl.ds(s * sub, sub), :]
        return send(
            there, there, agb_ss.at[h, d, k, s], agb_rs.at[h, d, k, s], a, at(a, 1 - 2 * d)
        )

    def behind(h, d, k):
        shift = k if d else n - k
        return lax.rem(pos[axes[h][0]] + shift, n)

    def use(h, j):
        y = y_all[h, j]
        if h == 0:
            y = dot(perm[...], y).astype(BF16)
        here = cols(h, j)
        scaled = y.astype(F32) * invg[:, here]
        scaled = scaled * scaled
        lanes = sumsq.shape[1]
        part = scaled[:, :lanes]
        for q in range(1, strip // lanes):
            part += scaled[:, q * lanes : (q + 1) * lanes]
        sumsq[...] += part
        acc[...] += dot_nt(y, wcat[:, here])

    for h in (0, 1):
        a, b = axes[h]
        all_but_one(y_all.at[h, 0, seen_b, :], aga_ss.at[h], aga_rs.at[h], b).wait_recv()
        for step in (0, 1):
            for d in (0, 1):
                s = step if d == 0 else 1 - step
                agb_copy(h, d, 0, s, pos[a]).start()
    loads[0].wait()
    loads[1].wait()
    for h in (0, 1):
        use(h, pos[axes[h][0]])

    def gather_step(k, carry):
        for step in (0, 1):
            for h in (0, 1):
                for d in (0, 1):
                    s = step if d == 0 else 1 - step
                    j = behind(h, d, k)
                    agb_copy(h, d, k - 1, s, j).wait_recv()
                    if step == 0:
                        agb_copy(h, d, k, s, j).start()
                    else:

                        @pl.when(k < reach - 1)
                        def _():
                            agb_copy(h, d, k, s, j).start()

        for h in (0, 1):
            for d in (0, 1):
                use(h, behind(h, d, k))
        return carry

    lax.fori_loop(1, reach, gather_step, 0)
    for h in (0, 1):
        j = behind(h, 0, reach)
        agb_copy(h, 0, reach - 1, 0, j).wait_recv()
        agb_copy(h, 1, reach - 1, 1, j).wait_recv()
        use(h, j)

    mean_sq = jnp.sum(sumsq[...], axis=1, keepdims=True) * (1.0 / width)
    factor = lax.rsqrt(mean_sq + 1e-05)

    def branch(base, scale_ref, pick):
        part = acc[:, pl.ds(base, slots)]
        scale = jnp.concatenate([scale_ref[...], jnp.zeros((1, slots - hidden), F32)], axis=1)
        added = jnp.dot(
            part, pick[...], precision=lax.Precision.HIGHEST, preferred_element_type=F32
        )
        return (part * scale + added) * factor

    gate = branch(0, gscale_ref, gpick)
    up = branch(slots, uscale_ref, upick)
    hid[0] = (gate / (1.0 + jnp.exp(-gate)) * up).astype(BF16)
    hid[1] = dot(perm[...], hid[0]).astype(BF16)
    for h in (0, 1):
        added = dot_nt(hid[h], dextp[...])
        high = added.astype(BF16)
        low = (added - high.astype(F32)).astype(BF16)
        lane = lax.broadcasted_iota(jnp.int32, added.shape, 1)
        extra_parts[h] = jnp.where(lane < k_out, high.astype(F32), low.astype(F32)).astype(BF16)
    loads[2].wait()

    def down(h, j, s):
        here = pl.ds(pl.multiple_of(h * half + s * wide, wide), wide)
        some = pl.ds(pl.multiple_of(j * block, block), block)
        base = dot(hid[h, some, :], wd[:, here]) * dscale_ref[:, here]
        return base + dot(extra_parts[h, some, :], onehot[:, here])

    def ring_copy(h, d, m):
        a = axes[h][0]
        return send(
            ring_s.at[h, d, m],
            ring_r.at[h, d, m + 2],
            ring_ss.at[h, d, m],
            ring_rs.at[h, d, m],
            a,
            at(a, 1 - 2 * d),
        )

    def ring_step(m, carry):
        away = lax.div(n - m, 2)
        for h in (0, 1):
            for d in (0, 1):
                odd = lax.rem(m, 2)
                s = odd if d == 0 else 1 - odd
                shift = n - away if d else away
                j = lax.rem(pos[axes[h][0]] + shift, n)
                value = down(h, j, s)

                @pl.when(m >= 2)
                def _():
                    ring_copy(h, d, m - 2).wait_recv()

                ring_s[h, d, m] = (value + ring_r[h, d, m].astype(F32)).astype(BF16)
                ring_copy(h, d, m).start()
        return carry

    lax.fori_loop(0, n - 1, ring_step, 0)

    def two_copy(h, r):
        b = axes[h][1]
        return send(
            two_s.at[h, at(b, r)], r_two.at[h, r - 1], two_ss.at[h], two_rs.at[h], b, at(b, r)
        )

    for h in (0, 1):
        for s in (0, 1):
            down_sum[h, :, pl.ds(s * wide, wide)] = down(h, pos[axes[h][0]], s)
    for h in (0, 1):
        for d in (0, 1):
            for m in (n - 3, n - 2):
                ring_copy(h, d, m).wait_recv()
        for s in (0, 1):
            some = pl.ds(s * wide, wide)
            plus = ring_r[h, 0, n - s].astype(F32)
            minus = ring_r[h, 1, n - 1 + s].astype(F32)
            down_sum[h, :, some] = down_sum[h, :, some] + plus + minus
        for j in range(n):
            two_s[h, j] = down_sum[h, pl.ds(j * rows, rows), :].astype(BF16)
        for r in offsets:
            two_copy(h, r).start()

    last = []
    for h in (0, 1):
        a, b = axes[h]
        all_but_one(mix_s.at[h, pl.ds(0, n - 1)], mix_ss.at[h], mix_rs.at[h], a).wait_recv()
        total = mix_r[h] + two_s[h, pos[b]].astype(F32)
        all_but_one(r_two.at[h], two_ss.at[h], two_rs.at[h], b).wait_recv()
        for r in range(1, n):
            total += r_two[h, r - 1].astype(F32)
        here = pl.ds(h * half, half)
        out_v[:, here] = total.astype(BF16)
        last.append(
            pltpu.make_async_copy(out_v.at[:, here], out_ref.at[:, here], load_sem.at[3 * h])
        )
        last[h].start()

    for h in (0, 1):
        a, b = axes[h]
        all_but_one(heads_all.at[h, seen_w, :], heads_ss.at[h], heads_rs.at[h], a).wait_send()
        all_but_one(w_all.at[h, seen_w, mine], w_ss.at[h], w_rs.at[h], a).wait_send()
        for q in range(1, cores):
            share_copy(h, q).wait_send()
        all_but_one(strm.at[h, pl.ds(0, n - 1)], strm_ss.at[h], strm_rs.at[h], a).wait_send()
        all_but_one(y_all.at[h, 0, seen_b, :], aga_ss.at[h], aga_rs.at[h], b).wait_send()
        all_but_one(r_one.at[h], one_ss.at[h], one_rs.at[h], b).wait_send()
        all_but_one(mix_s.at[h, pl.ds(0, n - 1)], mix_ss.at[h], mix_rs.at[h], a).wait_send()
        all_but_one(r_two.at[h], two_ss.at[h], two_rs.at[h], b).wait_send()
        for d in (0, 1):
            for k in range(reach):
                for s in (0, 1):
                    if k < reach - 1 or s == d:
                        agb_copy(h, d, k, s, behind(h, d, k)).wait_send()
            for m in range(n - 1):
                ring_copy(h, d, m).wait_send()
    for copy in last:
        copy.wait()


def local(n, cores, *args):
    (
        heads_out,
        stream_in,
        proj_levels,
        proj_scale,
        norm_gain,
        gate_levels,
        gate_scale,
        gate_index,
        gate_extra,
        up_levels,
        up_scale,
        up_index,
        up_extra,
        down_levels,
        down_scale,
        down_index,
        down_extra,
    ) = args
    tokens, feats = heads_out.shape
    rows, width = stream_in.shape
    hidden = gate_levels.shape[1]
    k_out = gate_extra.shape[1]
    slots = -(-(hidden + k_out) // 128) * 128
    strip = width // 2 // n
    block = tokens // n
    reach = n // 2
    index = pltpu.SMEM(gate_index.shape, jnp.int32)
    hbm = pl.BlockSpec(memory_space=pl.ANY)
    dma = pltpu.SemaphoreType.DMA
    scratch = [
        pltpu.VMEM((1, width), F32),
        pltpu.VMEM((1, width), F32),
        pltpu.VMEM((1, hidden), F32),
        index,
        pltpu.VMEM((k_out, width), BF16),
        pltpu.VMEM((1, hidden), F32),
        index,
        pltpu.VMEM((k_out, width), BF16),
        pltpu.VMEM((1, width), F32),
        index,
        pltpu.VMEM((k_out, hidden), BF16),
        pltpu.VMEM((2 * slots, width), BF16),
        pltpu.VMEM((slots, width), BF16),
        pltpu.VMEM((128, width), BF16),
        pltpu.VMEM((tokens, tokens), BF16),
        pltpu.VMEM((slots, slots), F32),
        pltpu.VMEM((slots, slots), F32),
        pltpu.VMEM((128, slots), BF16),
        pltpu.VMEM((1, width), F32),
        pltpu.VMEM((2, n * feats, tokens), BF16),
        pltpu.VMEM((2, n * feats, strip), BF16),
        pltpu.VMEM((2, n, rows, strip), BF16),
        pltpu.VMEM((2, tokens, strip), F32),
        pltpu.VMEM((2, tokens, strip), BF16),
        pltpu.VMEM((2, n - 1, block, strip), BF16),
        pltpu.VMEM((2, block, strip), F32),
        pltpu.VMEM((2, n, tokens, strip), BF16),
        pltpu.VMEM((tokens, 2 * slots), F32),
        pltpu.VMEM((tokens, 128), F32),
        pltpu.VMEM((2, tokens, slots), BF16),
        pltpu.VMEM((2, tokens, 128), BF16),
        pltpu.VMEM((2, 2, n - 1, block, width // 4), BF16),
        pltpu.VMEM((2, 2, n + 1, block, width // 4), BF16),
        pltpu.VMEM((2, n, rows, width // 2), BF16),
        pltpu.VMEM((2, n - 1, rows, width // 2), BF16),
        pltpu.VMEM((2, n, rows, strip), F32),
        pltpu.VMEM((2, rows, width // 2), F32),
        pltpu.VMEM((2, block, width // 2), F32),
        pltpu.VMEM((rows, width), BF16),
        dma((20,)),
    ]
    scratch += [dma((2,)), dma((2,)), dma((2,)), dma((2,)), dma((2, cores)), dma((2, cores))]
    scratch += [dma((2,)) for _ in range(6)]
    scratch += [dma((2, 2, reach, 2)), dma((2, 2, reach, 2))]
    scratch += [dma((2, 2, n - 1)), dma((2, 2, n - 1))]
    scratch += [dma((2,)) for _ in range(4)]
    return pl.pallas_call(
        functools.partial(kernel, n, cores),
        out_shape=jax.ShapeDtypeStruct((rows, width), BF16),
        in_specs=[hbm] * len(args),
        out_specs=hbm,
        scratch_shapes=scratch,
        compiler_params=pltpu.CompilerParams(
            collective_id=0, has_side_effects=True, vmem_limit_bytes=60 * 1024 * 1024
        ),
    )(
        heads_out.T,
        stream_in,
        proj_levels,
        proj_scale[None, :],
        norm_gain[None, :],
        gate_levels.T,
        gate_scale[None, :],
        gate_index,
        gate_extra.T,
        up_levels.T,
        up_scale[None, :],
        up_index,
        up_extra.T,
        down_levels,
        down_scale[None, :],
        down_index,
        down_extra.T,
    )


def solution(mesh):
    n = math.isqrt(mesh.shape["tensor"])
    torus = Mesh(
        mesh.devices.reshape(mesh.shape["groups"], n, n, mesh.shape["seq"]),
        ("groups", "tensor_0", "tensor_1", "seq"),
    )
    return jax.shard_map(
        functools.partial(local, n, mesh.shape["seq"]),
        mesh=torus,
        in_specs=(
            P(("groups", "seq"), TENSOR),
            P(GROUPS_SEQ_TENSOR, None),
            P(TENSOR, None),
            P(),
            P(),
            P(None, TENSOR),
            P(TENSOR),
            P(TENSOR, None),
            P(None, TENSOR),
            P(None, TENSOR),
            P(TENSOR),
            P(TENSOR, None),
            P(None, TENSOR),
            P(TENSOR, None),
            P(),
            P(TENSOR, None),
            P(TENSOR, None),
        ),
        out_specs=P(GROUPS_SEQ_TENSOR, None),
        check_vma=False,
    )
```

```python
import functools
import math

import jax
import jax.numpy as jnp
from jax import lax
from jax.experimental import pallas as pl
from jax.experimental.pallas import tpu as pltpu
from jax.sharding import Mesh
from jax.sharding import PartitionSpec as P

TENSOR = ("tensor_0", "tensor_1")
GROUPS_SEQ_TENSOR = ("groups", "seq", "tensor_0", "tensor_1")
MESH = pl.DeviceIdType.MESH
F32 = jnp.float32
BF16 = jnp.bfloat16
NT = (((1,), (1,)), ((), ()))


def dot(a, b):
    return jnp.dot(a, b, preferred_element_type=F32)


def dot_nt(a, b):
    return lax.dot_general(a, b, NT, preferred_element_type=F32)


def kernel(
    n,
    cores,
    heads_ref,
    stream_ref,
    projw_ref,
    pscale_in,
    gain_in,
    gatew_ref,
    gscale_in,
    gidx_in,
    gext_in,
    upw_ref,
    uscale_in,
    uidx_in,
    uext_in,
    downw_ref,
    dscale_in,
    didx_in,
    dext_in,
    out_ref,
    pscale_ref,
    gain_ref,
    gscale_ref,
    gidx_ref,
    gext_ref,
    uscale_ref,
    uidx_ref,
    uext_ref,
    dscale_ref,
    didx_ref,
    dext_ref,
    wcat,
    wd,
    onehot,
    perm,
    gpick,
    upick,
    dextp,
    invg,
    heads_all,
    ordered,
    w_all,
    strm,
    t_sum,
    t_half,
    r_one,
    mixed,
    y_all,
    acc,
    sumsq,
    hid,
    extra_parts,
    ring_s,
    ring_r,
    two_s,
    r_two,
    mix_s,
    mix_r,
    down_sum,
    out_v,
    load_sem,
    heads_ss,
    heads_rs,
    w_ss,
    w_rs,
    share_ss,
    share_rs,
    strm_ss,
    strm_rs,
    one_ss,
    one_rs,
    aga_ss,
    aga_rs,
    agb_ss,
    agb_rs,
    ring_ss,
    ring_rs,
    two_ss,
    two_rs,
    mix_ss,
    mix_rs,
):
    feats, tokens = heads_ref.shape
    width = projw_ref.shape[1]
    hidden = gatew_ref.shape[0]
    chunks = w_all.shape[1]
    chunk = w_all.shape[3]
    part = chunk // cores
    rows = stream_ref.shape[0]
    slots = gpick.shape[0]
    k_out = gext_ref.shape[0]
    half = width // 2
    strip = half // n
    block = tokens // n
    sub = tokens // 2
    wide = half // 2
    reach = n // 2
    axes = (("tensor_0", "tensor_1"), ("tensor_1", "tensor_0"))
    pos = {name: lax.axis_index(name) for name in TENSOR}
    offsets = sorted(range(1, n), key=lambda r: -min(r, n - r))

    def at(name, shift):
        return lax.rem(pos[name] + (shift + n) % n, n)

    def cols(h, j):
        return pl.ds(pl.multiple_of(h * half + j * strip, strip), strip)

    def send(src, dst, ssem, rsem, name, target):
        return pltpu.make_async_remote_copy(
            src_ref=src,
            dst_ref=dst,
            send_sem=ssem,
            recv_sem=rsem,
            device_id={name: target},
            device_id_type=MESH,
        )

    def all_but_one(ref, ssem, rsem, name):
        return send(ref, ref, ssem, rsem, name, at(name, 1))

    core = lax.axis_index("seq")
    barrier = pltpu.get_barrier_semaphore()
    for name in TENSOR:
        for r in range(1, n):
            pl.semaphore_signal(
                barrier, inc=1, device_id={name: at(name, r)}, device_id_type=MESH
            )
    for q in range(1, cores):
        pl.semaphore_signal(
            barrier, inc=1, device_id={"seq": lax.rem(core + q, cores)}, device_id_type=MESH
        )

    def place(sender):
        return pl.ds(pl.multiple_of(sender * feats, feats), feats)

    mine = pl.ds(pl.multiple_of(core * part, part), part)

    def some_cols(h, j, c):
        return pl.ds(pl.multiple_of(h * half + j * strip + c * chunk, chunk), chunk)

    def own_part(h, j, c):
        start = h * half + j * strip + c * chunk + core * part
        return pl.ds(pl.multiple_of(start, part), part)

    first = []
    for h in (0, 1):
        me = pos[axes[h][0]]
        for src, dst in (
            (heads_ref, heads_all.at[h, place(me), :]),
            (stream_ref.at[:, cols(h, me)], strm.at[h, me]),
        ) + tuple(
            (projw_ref.at[:, own_part(h, me, c)], w_all.at[h, c, place(me), mine])
            for c in range(chunks)
        ):
            first.append(pltpu.make_async_copy(src, dst, load_sem.at[len(first)]))
            first[-1].start()
    pl.semaphore_wait(barrier, 2 * (n - 1) + cores - 1)

    def heads_copy(h, r):
        a = axes[h][0]
        there = heads_all.at[h, place(pos[a]), :]
        return send(there, there, heads_ss.at[h], heads_rs.at[h], a, at(a, r))

    def w_copy(h, c, r):
        a = axes[h][0]
        return send(
            projw_ref.at[:, own_part(h, at(a, r), c)],
            w_all.at[h, c, place(pos[a]), mine],
            w_ss.at[h, c],
            w_rs.at[h, c],
            a,
            at(a, r),
        )

    def share_copy(h, c, q):
        there = w_all.at[h, c, :, mine]
        to = lax.rem(core + q, cores)
        return send(there, there, share_ss.at[h, c, q], share_rs.at[h, c, q], "seq", to)

    def strm_copy(h, r):
        a = axes[h][0]
        return send(
            stream_ref.at[:, cols(h, at(a, r))],
            strm.at[h, pos[a]],
            strm_ss.at[h],
            strm_rs.at[h],
            a,
            at(a, r),
        )

    each = 2 + chunks
    for c in range(chunks):
        for r in offsets:
            for h in (0, 1):
                w_copy(h, c, r).start()
        if c == 0:
            for h in (0, 1):
                first[each * h].wait()
            for r in offsets:
                for h in (0, 1):
                    heads_copy(h, r).start()
    for r in offsets:
        for h in (0, 1):
            strm_copy(h, r).start()
    small = []
    for src, dst in (
        (pscale_in, pscale_ref),
        (gain_in, gain_ref),
        (gscale_in, gscale_ref),
        (gidx_in, gidx_ref),
        (gext_in, gext_ref),
        (uscale_in, uscale_ref),
        (uidx_in, uidx_ref),
        (uext_in, uext_ref),
        (dscale_in, dscale_ref),
        (didx_in, didx_ref),
        (dext_in, dext_ref),
    ):
        small.append(pltpu.make_async_copy(src, dst, load_sem.at[len(first) + len(small)]))
        small[-1].start()
    base = len(first) + len(small)
    loads = [
        pltpu.make_async_copy(gatew_ref, wcat.at[pl.ds(0, hidden), :], load_sem.at[base]),
        pltpu.make_async_copy(upw_ref, wcat.at[pl.ds(slots, hidden), :], load_sem.at[base + 1]),
        pltpu.make_async_copy(downw_ref, wd.at[pl.ds(0, hidden), :], load_sem.at[base + 2]),
    ]
    for load in loads:
        load.start()

    for copy in small:
        copy.wait()
    r_i = lax.broadcasted_iota(jnp.int32, (tokens, tokens), 0)
    c_i = lax.broadcasted_iota(jnp.int32, (tokens, tokens), 1)
    swapped = (
        lax.rem(lax.div(r_i, rows), n) * block + lax.div(r_i, block) * rows + lax.rem(r_i, rows)
    )
    perm[...] = jnp.where(c_i == swapped, 1.0, 0.0).astype(BF16)

    def index_column(idx_ref, count):
        row = lax.rem(lax.broadcasted_iota(jnp.int32, (count, 1), 0), k_out)
        column = jnp.zeros((count, 1), jnp.int32)
        for k in range(k_out):
            column = jnp.where(row == k, idx_ref[0, k], column)
        return column

    for pick, idx_ref in ((gpick, gidx_ref), (upick, uidx_ref)):
        pick[...] = jnp.zeros_like(pick)
        chosen = lax.broadcasted_iota(jnp.int32, (k_out, slots), 1) == index_column(idx_ref, k_out)
        pick[pl.ds(hidden, k_out), :] = jnp.where(chosen, 1.0, 0.0)

    one_rows = onehot.shape[0]
    didx = index_column(didx_ref, one_rows)
    live = lax.broadcasted_iota(jnp.int32, (one_rows, strip), 0) < 2 * k_out

    def prepare(j, carry):
        here = pl.ds(pl.multiple_of(j * strip, strip), strip)
        column = lax.broadcasted_iota(jnp.int32, (one_rows, strip), 1) + j * strip
        onehot[:, here] = jnp.where((column == didx) & live, 1.0, 0.0).astype(BF16)
        blank = jnp.zeros((slots - hidden - k_out, strip), F32)
        for base, ext in ((0, gext_ref), (slots, uext_ref)):
            filled = jnp.concatenate([ext[:, here].astype(F32), blank], axis=0)
            wcat[pl.ds(base + hidden, slots - hidden), here] = filled.astype(BF16)
        wd[pl.ds(hidden, slots - hidden), here] = jnp.zeros((slots - hidden, strip), BF16)
        invg[:, here] = 1.0 / gain_ref[:, here]
        return carry

    lax.fori_loop(0, width // strip, prepare, 0)
    dext = jnp.concatenate([dext_ref[...].astype(F32)] * 2, axis=0)
    dext = jnp.concatenate([dext, jnp.zeros((dextp.shape[0] - 2 * k_out, hidden), F32)], axis=0)
    dextp[...] = jnp.zeros_like(dextp)
    dextp[:, pl.ds(0, hidden)] = dext.astype(BF16)
    acc[...] = jnp.zeros_like(acc)
    sumsq[...] = jnp.zeros_like(sumsq)
    for h in (0, 1):
        for d in (0, 1):
            for m in (0, 1):
                ring_r[h, d, m] = jnp.zeros((block, wide), BF16)

    def one_copy(h, c, r):
        b = axes[h][1]
        away = pl.ds(pl.multiple_of(at(b, r) * block, block), block)
        return send(
            t_half.at[h, c, away, :],
            r_one.at[h, c, r - 1],
            one_ss.at[h, c],
            one_rs.at[h, c],
            b,
            at(b, r),
        )

    seen_w = pl.ds(0, (n - 1) * feats)
    seen_b = pl.ds(0, (n - 1) * block)
    for c in range(chunks):
        for h in (0, 1):
            a = axes[h][0]
            first[each * h + 2 + c].wait()
            all_but_one(
                w_all.at[h, c, seen_w, mine], w_ss.at[h, c], w_rs.at[h, c], a
            ).wait_recv()
            for q in range(1, cores):
                share_copy(h, c, q).start()
        for h in (0, 1):
            a = axes[h][0]
            if c == 0:
                all_but_one(
                    heads_all.at[h, seen_w, :], heads_ss.at[h], heads_rs.at[h], a
                ).wait_recv()
                if h == 0:
                    turn = perm[...]
                else:
                    turn = jnp.where(r_i == c_i, 1.0, 0.0).astype(BF16)
                ordered[h] = dot_nt(turn, heads_all[h]).astype(BF16)
            for q in range(1, cores):
                share_copy(h, c, q).wait_recv()
            t_sum[h, c] = dot(ordered[h], w_all[h, c])
            t_half[h, c] = t_sum[h, c].astype(BF16)
            for r in offsets:
                one_copy(h, c, r).start()

    def aga_copy(h, c, r):
        a, b = axes[h]
        own = pl.ds(pl.multiple_of(pos[b] * block, block), block)
        there = y_all.at[h, pos[a], c, own, :]
        return send(there, there, aga_ss.at[h, c], aga_rs.at[h, c], b, at(b, r))

    def mix_copy(h, r):
        a = axes[h][0]
        there = mix_r.at[h, :, pl.ds(pl.multiple_of(pos[a] * strip, strip), strip)]
        return send(mix_s.at[h, at(a, r)], there, mix_ss.at[h], mix_rs.at[h], a, at(a, r))

    for c in range(chunks):
        for h in (0, 1):
            a, b = axes[h]
            here = some_cols(h, pos[a], c)
            within = pl.ds(c * chunk, chunk)
            own = pl.ds(pl.multiple_of(pos[b] * block, block), block)
            total = t_sum[h, c, own, :]
            if c == 0:
                first[each * h + 1].wait()
                all_but_one(
                    strm.at[h, pl.ds(0, n - 1)], strm_ss.at[h], strm_rs.at[h], a
                ).wait_recv()
            all_but_one(r_one.at[h, c], one_ss.at[h, c], one_rs.at[h, c], b).wait_recv()
            for r in range(1, n):
                total += r_one[h, c, r - 1].astype(F32)
            mixed[h, c] = total * pscale_ref[:, here]
            for j in range(n):
                few = pl.ds(j * rows, rows)
                mixed[h, c, few, :] = mixed[h, c, few, :] + strm[h, j, :, within].astype(F32)
            y_all[h, pos[a], c, own, :] = (mixed[h, c] * gain_ref[:, here]).astype(BF16)
            for r in offsets:
                aga_copy(h, c, r).start()
            for j in range(n):
                mix_s[h, j, :, within] = mixed[h, c, pl.ds(j * rows, rows), :]
    for h in (0, 1):
        me = pos[axes[h][0]]
        for r in offsets:
            mix_copy(h, r).start()
        mix_r[h, :, pl.ds(pl.multiple_of(me * strip, strip), strip)] = mix_s[h, me]

    def agb_copy(h, d, k, c, strip_id, whole):
        a = axes[h][0]
        some = pl.ds(0, tokens) if whole else pl.ds(d * sub, sub)
        there = y_all.at[h, strip_id, c, some, :]
        return send(
            there, there, agb_ss.at[h, d, k, c], agb_rs.at[h, d, k, c], a, at(a, 1 - 2 * d)
        )

    def behind(h, d, k):
        shift = k if d else n - k
        return lax.rem(pos[axes[h][0]] + shift, n)

    def use(h, j):
        lanes = sumsq.shape[1]
        squares = sumsq[...]
        total = acc[...]
        for c in range(chunks):
            y = y_all[h, j, c]
            if h == 0:
                y = dot(perm[...], y).astype(BF16)
            here = some_cols(h, j, c)
            scaled = y.astype(F32) * invg[:, here]
            scaled = scaled * scaled
            for q in range(chunk // lanes):
                squares += scaled[:, q * lanes : (q + 1) * lanes]
            total += dot_nt(y, wcat[:, here])
        sumsq[...] = squares
        acc[...] = total

    for c in range(chunks):
        for h in (0, 1):
            a, b = axes[h]
            all_but_one(
                y_all.at[h, 0, c, seen_b, :], aga_ss.at[h, c], aga_rs.at[h, c], b
            ).wait_recv()
            for d in (0, 1):
                agb_copy(h, d, 0, c, pos[a], True).start()
    loads[0].wait()
    loads[1].wait()
    for h in (0, 1):
        use(h, pos[axes[h][0]])

    def gather_step(k, carry):
        for c in range(chunks):
            for h in (0, 1):
                for d in (0, 1):
                    j = behind(h, d, k)
                    agb_copy(h, d, k - 1, c, j, True).wait_recv()

                    @pl.when(k < reach - 1)
                    def _():
                        agb_copy(h, d, k, c, j, True).start()

                    @pl.when(k == reach - 1)
                    def _():
                        agb_copy(h, d, k, c, j, False).start()

        for h in (0, 1):
            for d in (0, 1):
                use(h, behind(h, d, k))
        return carry

    lax.fori_loop(1, reach, gather_step, 0)
    for h in (0, 1):
        j = behind(h, 0, reach)
        for d in (0, 1):
            for c in range(chunks):
                agb_copy(h, d, reach - 1, c, j, False).wait_recv()
        use(h, j)

    mean_sq = jnp.sum(sumsq[...], axis=1, keepdims=True) * (1.0 / width)
    factor = lax.rsqrt(mean_sq + 1e-05)

    def branch(base, scale_ref, pick):
        part = acc[:, pl.ds(base, slots)]
        scale = jnp.concatenate([scale_ref[...], jnp.zeros((1, slots - hidden), F32)], axis=1)
        added = jnp.dot(
            part, pick[...], precision=lax.Precision.HIGHEST, preferred_element_type=F32
        )
        return (part * scale + added) * factor

    gate = branch(0, gscale_ref, gpick)
    up = branch(slots, uscale_ref, upick)
    hid[0] = (gate / (1.0 + jnp.exp(-gate)) * up).astype(BF16)
    hid[1] = dot(perm[...], hid[0]).astype(BF16)
    for h in (0, 1):
        added = dot_nt(hid[h], dextp[...])
        high = added.astype(BF16)
        low = (added - high.astype(F32)).astype(BF16)
        lane = lax.broadcasted_iota(jnp.int32, added.shape, 1)
        extra_parts[h] = jnp.where(lane < k_out, high.astype(F32), low.astype(F32)).astype(BF16)
    loads[2].wait()

    def down(h, j, s):
        here = pl.ds(pl.multiple_of(h * half + s * wide, wide), wide)
        some = pl.ds(pl.multiple_of(j * block, block), block)
        base = dot(hid[h, some, :], wd[:, here]) * dscale_ref[:, here]
        return base + dot(extra_parts[h, some, :], onehot[:, here])

    def ring_copy(h, d, m):
        a = axes[h][0]
        return send(
            ring_s.at[h, d, m],
            ring_r.at[h, d, m + 2],
            ring_ss.at[h, d, m],
            ring_rs.at[h, d, m],
            a,
            at(a, 1 - 2 * d),
        )

    def ring_step(m, carry):
        away = lax.div(n - m, 2)
        for h in (0, 1):
            for d in (0, 1):
                odd = lax.rem(m, 2)
                s = odd if d == 0 else 1 - odd
                shift = n - away if d else away
                j = lax.rem(pos[axes[h][0]] + shift, n)
                value = down(h, j, s)

                @pl.when(m >= 2)
                def _():
                    ring_copy(h, d, m - 2).wait_recv()

                ring_s[h, d, m] = (value + ring_r[h, d, m].astype(F32)).astype(BF16)
                ring_copy(h, d, m).start()
        return carry

    lax.fori_loop(0, n - 1, ring_step, 0)

    def two_copy(h, r):
        b = axes[h][1]
        return send(
            two_s.at[h, at(b, r)], r_two.at[h, r - 1], two_ss.at[h], two_rs.at[h], b, at(b, r)
        )

    for h in (0, 1):
        for s in (0, 1):
            down_sum[h, :, pl.ds(s * wide, wide)] = down(h, pos[axes[h][0]], s)
    for h in (0, 1):
        for d in (0, 1):
            for m in (n - 3, n - 2):
                ring_copy(h, d, m).wait_recv()
        for s in (0, 1):
            some = pl.ds(s * wide, wide)
            plus = ring_r[h, 0, n - s].astype(F32)
            minus = ring_r[h, 1, n - 1 + s].astype(F32)
            down_sum[h, :, some] = down_sum[h, :, some] + plus + minus
        for j in range(n):
            two_s[h, j] = down_sum[h, pl.ds(j * rows, rows), :].astype(BF16)
        for r in offsets:
            two_copy(h, r).start()

    last = []
    for h in (0, 1):
        a, b = axes[h]
        all_but_one(mix_s.at[h, pl.ds(0, n - 1)], mix_ss.at[h], mix_rs.at[h], a).wait_recv()
        total = mix_r[h] + two_s[h, pos[b]].astype(F32)
        all_but_one(r_two.at[h], two_ss.at[h], two_rs.at[h], b).wait_recv()
        for r in range(1, n):
            total += r_two[h, r - 1].astype(F32)
        here = pl.ds(h * half, half)
        out_v[:, here] = total.astype(BF16)
        last.append(
            pltpu.make_async_copy(out_v.at[:, here], out_ref.at[:, here], load_sem.at[3 * h])
        )
        last[h].start()

    for h in (0, 1):
        a, b = axes[h]
        all_but_one(heads_all.at[h, seen_w, :], heads_ss.at[h], heads_rs.at[h], a).wait_send()
        all_but_one(strm.at[h, pl.ds(0, n - 1)], strm_ss.at[h], strm_rs.at[h], a).wait_send()
        for c in range(chunks):
            all_but_one(
                w_all.at[h, c, seen_w, mine], w_ss.at[h, c], w_rs.at[h, c], a
            ).wait_send()
            for q in range(1, cores):
                share_copy(h, c, q).wait_send()
            all_but_one(
                y_all.at[h, 0, c, seen_b, :], aga_ss.at[h, c], aga_rs.at[h, c], b
            ).wait_send()
            all_but_one(r_one.at[h, c], one_ss.at[h, c], one_rs.at[h, c], b).wait_send()
        all_but_one(mix_s.at[h, pl.ds(0, n - 1)], mix_ss.at[h], mix_rs.at[h], a).wait_send()
        all_but_one(r_two.at[h], two_ss.at[h], two_rs.at[h], b).wait_send()
        for d in (0, 1):
            for k in range(reach):
                for c in range(chunks):
                    agb_copy(h, d, k, c, behind(h, d, k), k < reach - 1).wait_send()
            for m in range(n - 1):
                ring_copy(h, d, m).wait_send()
    for copy in last:
        copy.wait()


def local(n, cores, *args):
    (
        heads_out,
        stream_in,
        proj_levels,
        proj_scale,
        norm_gain,
        gate_levels,
        gate_scale,
        gate_index,
        gate_extra,
        up_levels,
        up_scale,
        up_index,
        up_extra,
        down_levels,
        down_scale,
        down_index,
        down_extra,
    ) = args
    tokens, feats = heads_out.shape
    rows, width = stream_in.shape
    hidden = gate_levels.shape[1]
    k_out = gate_extra.shape[1]
    slots = -(-(hidden + k_out) // 128) * 128
    strip = width // 2 // n
    chunks = 2
    chunk = strip // chunks
    block = tokens // n
    reach = n // 2
    index = pltpu.SMEM(gate_index.shape, jnp.int32)
    hbm = pl.BlockSpec(memory_space=pl.ANY)
    dma = pltpu.SemaphoreType.DMA
    scratch = [
        pltpu.VMEM((1, width), F32),
        pltpu.VMEM((1, width), F32),
        pltpu.VMEM((1, hidden), F32),
        index,
        pltpu.VMEM((k_out, width), BF16),
        pltpu.VMEM((1, hidden), F32),
        index,
        pltpu.VMEM((k_out, width), BF16),
        pltpu.VMEM((1, width), F32),
        index,
        pltpu.VMEM((k_out, hidden), BF16),
        pltpu.VMEM((2 * slots, width), BF16),
        pltpu.VMEM((slots, width), BF16),
        pltpu.VMEM((128, width), BF16),
        pltpu.VMEM((tokens, tokens), BF16),
        pltpu.VMEM((slots, slots), F32),
        pltpu.VMEM((slots, slots), F32),
        pltpu.VMEM((128, slots), BF16),
        pltpu.VMEM((1, width), F32),
        pltpu.VMEM((2, n * feats, tokens), BF16),
        pltpu.VMEM((2, tokens, n * feats), BF16),
        pltpu.VMEM((2, chunks, n * feats, chunk), BF16),
        pltpu.VMEM((2, n, rows, strip), BF16),
        pltpu.VMEM((2, chunks, tokens, chunk), F32),
        pltpu.VMEM((2, chunks, tokens, chunk), BF16),
        pltpu.VMEM((2, chunks, n - 1, block, chunk), BF16),
        pltpu.VMEM((2, chunks, block, chunk), F32),
        pltpu.VMEM((2, n, chunks, tokens, chunk), BF16),
        pltpu.VMEM((tokens, 2 * slots), F32),
        pltpu.VMEM((tokens, 128), F32),
        pltpu.VMEM((2, tokens, slots), BF16),
        pltpu.VMEM((2, tokens, 128), BF16),
        pltpu.VMEM((2, 2, n - 1, block, width // 4), BF16),
        pltpu.VMEM((2, 2, n + 1, block, width // 4), BF16),
        pltpu.VMEM((2, n, rows, width // 2), BF16),
        pltpu.VMEM((2, n - 1, rows, width // 2), BF16),
        pltpu.VMEM((2, n, rows, strip), F32),
        pltpu.VMEM((2, rows, width // 2), F32),
        pltpu.VMEM((2, block, width // 2), F32),
        pltpu.VMEM((rows, width), BF16),
        dma((4 + 2 * chunks + 14,)),
    ]
    scratch += [dma((2,)), dma((2,)), dma((2, chunks)), dma((2, chunks))]
    scratch += [dma((2, chunks, cores)), dma((2, chunks, cores)), dma((2,)), dma((2,))]
    scratch += [dma((2, chunks)) for _ in range(4)]
    scratch += [dma((2, 2, reach, chunks)), dma((2, 2, reach, chunks))]
    scratch += [dma((2, 2, n - 1)), dma((2, 2, n - 1))]
    scratch += [dma((2,)) for _ in range(4)]
    return pl.pallas_call(
        functools.partial(kernel, n, cores),
        out_shape=jax.ShapeDtypeStruct((rows, width), BF16),
        in_specs=[hbm] * len(args),
        out_specs=hbm,
        scratch_shapes=scratch,
        compiler_params=pltpu.CompilerParams(
            collective_id=0, has_side_effects=True, vmem_limit_bytes=60 * 1024 * 1024
        ),
    )(
        heads_out.T,
        stream_in,
        proj_levels,
        proj_scale[None, :],
        norm_gain[None, :],
        gate_levels.T,
        gate_scale[None, :],
        gate_index,
        gate_extra.T,
        up_levels.T,
        up_scale[None, :],
        up_index,
        up_extra.T,
        down_levels,
        down_scale[None, :],
        down_index,
        down_extra.T,
    )


def solution(mesh):
    n = math.isqrt(mesh.shape["tensor"])
    torus = Mesh(
        mesh.devices.reshape(mesh.shape["groups"], n, n, mesh.shape["seq"]),
        ("groups", "tensor_0", "tensor_1", "seq"),
    )
    return jax.shard_map(
        functools.partial(local, n, mesh.shape["seq"]),
        mesh=torus,
        in_specs=(
            P(("groups", "seq"), TENSOR),
            P(GROUPS_SEQ_TENSOR, None),
            P(TENSOR, None),
            P(),
            P(),
            P(None, TENSOR),
            P(TENSOR),
            P(TENSOR, None),
            P(None, TENSOR),
            P(None, TENSOR),
            P(TENSOR),
            P(TENSOR, None),
            P(None, TENSOR),
            P(TENSOR, None),
            P(),
            P(TENSOR, None),
            P(TENSOR, None),
        ),
        out_specs=P(GROUPS_SEQ_TENSOR, None),
        check_vma=False,
    )
```

```python
import functools
import math

import jax
import jax.numpy as jnp
from jax import lax
from jax.experimental import pallas as pl
from jax.experimental.pallas import tpu as pltpu
from jax.sharding import Mesh
from jax.sharding import PartitionSpec as P

TENSOR = ("tensor_0", "tensor_1")
GROUPS_SEQ_TENSOR = ("groups", "seq", "tensor_0", "tensor_1")
MESH = pl.DeviceIdType.MESH
F32 = jnp.float32
BF16 = jnp.bfloat16
NT = (((1,), (1,)), ((), ()))


def dot(a, b):
    return jnp.dot(a, b, preferred_element_type=F32)


def dot_nt(a, b):
    return lax.dot_general(a, b, NT, preferred_element_type=F32)


def kernel(
    n,
    cores,
    heads_ref,
    stream_ref,
    projw_ref,
    pscale_in,
    gain_in,
    gatew_ref,
    gscale_in,
    gidx_in,
    gext_in,
    upw_ref,
    uscale_in,
    uidx_in,
    uext_in,
    downw_ref,
    dscale_in,
    didx_in,
    dext_in,
    out_ref,
    pscale_ref,
    gain_ref,
    gscale_ref,
    gidx_ref,
    gext_ref,
    uscale_ref,
    uidx_ref,
    uext_ref,
    dscale_ref,
    didx_ref,
    dext_ref,
    wcat,
    wd,
    onehot,
    perm,
    gpick,
    upick,
    dextp,
    invg,
    heads_all,
    ordered,
    w_all,
    strm,
    t_sum,
    t_half,
    r_one,
    mixed,
    y_all,
    acc,
    sumsq,
    hid,
    extra_parts,
    ring_s,
    ring_r,
    two_s,
    r_two,
    mix_s,
    mix_r,
    down_sum,
    out_v,
    load_sem,
    heads_ss,
    heads_rs,
    w_ss,
    w_rs,
    share_ss,
    share_rs,
    strm_ss,
    strm_rs,
    one_ss,
    one_rs,
    aga_ss,
    aga_rs,
    agb_ss,
    agb_rs,
    ring_ss,
    ring_rs,
    two_ss,
    two_rs,
    mix_ss,
    mix_rs,
):
    feats, tokens = heads_ref.shape
    width = projw_ref.shape[1]
    hidden = gatew_ref.shape[0]
    chunks = w_all.shape[1]
    chunk = w_all.shape[3]
    part = chunk // cores
    rows = stream_ref.shape[0]
    slots = gpick.shape[0]
    k_out = gext_ref.shape[0]
    half = width // 2
    strip = half // n
    block = tokens // n
    sub = tokens // 2
    wide = ring_s.shape[4]
    pieces = half // wide
    per = pieces // 2
    messages = per * (n - 1)
    reach = n // 2
    axes = (("tensor_0", "tensor_1"), ("tensor_1", "tensor_0"))
    pos = {name: lax.axis_index(name) for name in TENSOR}
    offsets = sorted(range(1, n), key=lambda r: -min(r, n - r))

    def at(name, shift):
        return lax.rem(pos[name] + (shift + n) % n, n)

    def cols(h, j):
        return pl.ds(pl.multiple_of(h * half + j * strip, strip), strip)

    def send(src, dst, ssem, rsem, name, target):
        return pltpu.make_async_remote_copy(
            src_ref=src,
            dst_ref=dst,
            send_sem=ssem,
            recv_sem=rsem,
            device_id={name: target},
            device_id_type=MESH,
        )

    def all_but_one(ref, ssem, rsem, name):
        return send(ref, ref, ssem, rsem, name, at(name, 1))

    core = lax.axis_index("seq")
    barrier = pltpu.get_barrier_semaphore()
    for name in TENSOR:
        for r in range(1, n):
            pl.semaphore_signal(
                barrier, inc=1, device_id={name: at(name, r)}, device_id_type=MESH
            )
    for q in range(1, cores):
        pl.semaphore_signal(
            barrier, inc=1, device_id={"seq": lax.rem(core + q, cores)}, device_id_type=MESH
        )

    def place(sender):
        return pl.ds(pl.multiple_of(sender * feats, feats), feats)

    mine = pl.ds(pl.multiple_of(core * part, part), part)

    def some_cols(h, j, c):
        return pl.ds(pl.multiple_of(h * half + j * strip + c * chunk, chunk), chunk)

    def own_part(h, j, c):
        start = h * half + j * strip + c * chunk + core * part
        return pl.ds(pl.multiple_of(start, part), part)

    first = []
    for h in (0, 1):
        me = pos[axes[h][0]]
        for src, dst in (
            (heads_ref, heads_all.at[h, place(me), :]),
            (stream_ref.at[:, cols(h, me)], strm.at[h, me]),
        ) + tuple(
            (projw_ref.at[:, own_part(h, me, c)], w_all.at[h, c, place(me), mine])
            for c in range(chunks)
        ):
            first.append(pltpu.make_async_copy(src, dst, load_sem.at[len(first)]))
            first[-1].start()
    pl.semaphore_wait(barrier, 2 * (n - 1) + cores - 1)

    def behind(h, d, k):
        shift = k if d else n - k
        return lax.rem(pos[axes[h][0]] + shift, n)

    def heads_copy(h, d, k):
        a = axes[h][0]
        few = feats // 2 if k == reach - 1 else feats
        start = behind(h, d, k) * feats + (d * few if k == reach - 1 else 0)
        there = heads_all.at[h, pl.ds(pl.multiple_of(start, few), few), :]
        return send(there, there, heads_ss.at[h, d, k], heads_rs.at[h, d, k], a, at(a, 1 - 2 * d))

    def heads_arrive(k):
        for h in (0, 1):
            for d in (0, 1):
                heads_copy(h, d, k).wait_recv()
                if k < reach - 1:
                    heads_copy(h, d, k + 1).start()

    def w_copy(h, c, r):
        a = axes[h][0]
        return send(
            projw_ref.at[:, own_part(h, at(a, r), c)],
            w_all.at[h, c, place(pos[a]), mine],
            w_ss.at[h, c],
            w_rs.at[h, c],
            a,
            at(a, r),
        )

    def share_copy(h, c, q):
        there = w_all.at[h, c, :, mine]
        to = lax.rem(core + q, cores)
        return send(there, there, share_ss.at[h, c, q], share_rs.at[h, c, q], "seq", to)

    def strm_copy(h, r):
        a = axes[h][0]
        return send(
            stream_ref.at[:, cols(h, at(a, r))],
            strm.at[h, pos[a]],
            strm_ss.at[h],
            strm_rs.at[h],
            a,
            at(a, r),
        )

    each = 2 + chunks
    for h in (0, 1):
        first[each * h].wait()
        for d in (0, 1):
            heads_copy(h, d, 0).start()
    for r in offsets:
        for h in (0, 1):
            w_copy(h, 0, r).start()
    small = []
    for src, dst in (
        (pscale_in, pscale_ref),
        (gain_in, gain_ref),
        (gscale_in, gscale_ref),
        (gidx_in, gidx_ref),
        (gext_in, gext_ref),
        (uscale_in, uscale_ref),
        (uidx_in, uidx_ref),
        (uext_in, uext_ref),
        (dscale_in, dscale_ref),
        (didx_in, didx_ref),
        (dext_in, dext_ref),
    ):
        small.append(pltpu.make_async_copy(src, dst, load_sem.at[len(first) + len(small)]))
        small[-1].start()
    base = len(first) + len(small)
    loads = [
        pltpu.make_async_copy(gatew_ref, wcat.at[pl.ds(0, hidden), :], load_sem.at[base]),
        pltpu.make_async_copy(upw_ref, wcat.at[pl.ds(slots, hidden), :], load_sem.at[base + 1]),
        pltpu.make_async_copy(downw_ref, wd.at[pl.ds(0, hidden), :], load_sem.at[base + 2]),
    ]
    for load in loads:
        load.start()

    heads_arrive(0)
    for c in range(1, chunks):
        for r in offsets:
            for h in (0, 1):
                w_copy(h, c, r).start()
    for r in offsets:
        for h in (0, 1):
            strm_copy(h, r).start()

    for copy in small:
        copy.wait()
    r_i = lax.broadcasted_iota(jnp.int32, (tokens, tokens), 0)
    c_i = lax.broadcasted_iota(jnp.int32, (tokens, tokens), 1)
    swapped = (
        lax.rem(lax.div(r_i, rows), n) * block + lax.div(r_i, block) * rows + lax.rem(r_i, rows)
    )
    perm[...] = jnp.where(c_i == swapped, 1.0, 0.0).astype(BF16)

    def index_column(idx_ref, count):
        row = lax.rem(lax.broadcasted_iota(jnp.int32, (count, 1), 0), k_out)
        column = jnp.zeros((count, 1), jnp.int32)
        for k in range(k_out):
            column = jnp.where(row == k, idx_ref[0, k], column)
        return column

    for pick, idx_ref in ((gpick, gidx_ref), (upick, uidx_ref)):
        pick[...] = jnp.zeros_like(pick)
        chosen = lax.broadcasted_iota(jnp.int32, (k_out, slots), 1) == index_column(idx_ref, k_out)
        pick[pl.ds(hidden, k_out), :] = jnp.where(chosen, 1.0, 0.0)

    one_rows = onehot.shape[0]
    didx = index_column(didx_ref, one_rows)
    live = lax.broadcasted_iota(jnp.int32, (one_rows, strip), 0) < 2 * k_out

    def prepare(j, carry):
        here = pl.ds(pl.multiple_of(j * strip, strip), strip)
        column = lax.broadcasted_iota(jnp.int32, (one_rows, strip), 1) + j * strip
        onehot[:, here] = jnp.where((column == didx) & live, 1.0, 0.0).astype(BF16)
        blank = jnp.zeros((slots - hidden - k_out, strip), F32)
        for base, ext in ((0, gext_ref), (slots, uext_ref)):
            filled = jnp.concatenate([ext[:, here].astype(F32), blank], axis=0)
            wcat[pl.ds(base + hidden, slots - hidden), here] = filled.astype(BF16)
        wd[pl.ds(hidden, slots - hidden), here] = jnp.zeros((slots - hidden, strip), BF16)
        invg[:, here] = 1.0 / gain_ref[:, here]
        return carry

    lax.fori_loop(0, width // strip, prepare, 0)
    dext = jnp.concatenate([dext_ref[...].astype(F32)] * 2, axis=0)
    dext = jnp.concatenate([dext, jnp.zeros((dextp.shape[0] - 2 * k_out, hidden), F32)], axis=0)
    dextp[...] = jnp.zeros_like(dextp)
    dextp[:, pl.ds(0, hidden)] = dext.astype(BF16)
    acc[...] = jnp.zeros_like(acc)
    sumsq[...] = jnp.zeros_like(sumsq)
    for h in (0, 1):
        for d in (0, 1):
            for m in range(pieces):
                ring_r[h, d, m] = jnp.zeros((block, wide), BF16)

    def one_copy(h, c, r):
        b = axes[h][1]
        away = pl.ds(pl.multiple_of(at(b, r) * block, block), block)
        return send(
            t_half.at[h, c, away, :],
            r_one.at[h, c, r - 1],
            one_ss.at[h, c],
            one_rs.at[h, c],
            b,
            at(b, r),
        )

    seen_w = pl.ds(0, (n - 1) * feats)
    seen_b = pl.ds(0, (n - 1) * block)
    for k in range(1, reach - 1):
        heads_arrive(k)
    for c in range(chunks):
        for h in (0, 1):
            a = axes[h][0]
            first[each * h + 2 + c].wait()
            all_but_one(
                w_all.at[h, c, seen_w, mine], w_ss.at[h, c], w_rs.at[h, c], a
            ).wait_recv()
            for q in range(1, cores):
                share_copy(h, c, q).start()
        for h in (0, 1):
            a = axes[h][0]
            if c == 0:
                for d in (0, 1):
                    heads_copy(h, d, reach - 1).wait_recv()
                if h == 0:
                    turn = perm[...]
                else:
                    turn = jnp.where(r_i == c_i, 1.0, 0.0).astype(BF16)
                ordered[h] = dot_nt(turn, heads_all[h]).astype(BF16)
            for q in range(1, cores):
                share_copy(h, c, q).wait_recv()
            t_sum[h, c] = dot(ordered[h], w_all[h, c])
            t_half[h, c] = t_sum[h, c].astype(BF16)
            for r in offsets:
                one_copy(h, c, r).start()

    def aga_copy(h, c, r):
        a, b = axes[h]
        own = pl.ds(pl.multiple_of(pos[b] * block, block), block)
        there = y_all.at[h, pos[a], c, own, :]
        return send(there, there, aga_ss.at[h, c], aga_rs.at[h, c], b, at(b, r))

    def mix_copy(h, r):
        a = axes[h][0]
        there = mix_r.at[h, :, pl.ds(pl.multiple_of(pos[a] * strip, strip), strip)]
        return send(mix_s.at[h, at(a, r)], there, mix_ss.at[h], mix_rs.at[h], a, at(a, r))

    for c in range(chunks):
        for h in (0, 1):
            a, b = axes[h]
            here = some_cols(h, pos[a], c)
            within = pl.ds(c * chunk, chunk)
            own = pl.ds(pl.multiple_of(pos[b] * block, block), block)
            total = t_sum[h, c, own, :]
            if c == 0:
                first[each * h + 1].wait()
                all_but_one(
                    strm.at[h, pl.ds(0, n - 1)], strm_ss.at[h], strm_rs.at[h], a
                ).wait_recv()
            all_but_one(r_one.at[h, c], one_ss.at[h, c], one_rs.at[h, c], b).wait_recv()
            for r in range(1, n):
                total += r_one[h, c, r - 1].astype(F32)
            mixed[h, c] = total * pscale_ref[:, here]
            for j in range(n):
                few = pl.ds(j * rows, rows)
                mixed[h, c, few, :] = mixed[h, c, few, :] + strm[h, j, :, within].astype(F32)
            y_all[h, pos[a], c, own, :] = (mixed[h, c] * gain_ref[:, here]).astype(BF16)
            for r in offsets:
                aga_copy(h, c, r).start()
            for j in range(n):
                mix_s[h, j, :, within] = mixed[h, c, pl.ds(j * rows, rows), :]
    for h in (0, 1):
        me = pos[axes[h][0]]
        for r in offsets:
            mix_copy(h, r).start()
        mix_r[h, :, pl.ds(pl.multiple_of(me * strip, strip), strip)] = mix_s[h, me]

    def agb_copy(h, d, k, c, strip_id, whole):
        a = axes[h][0]
        some = pl.ds(0, tokens) if whole else pl.ds(d * sub, sub)
        there = y_all.at[h, strip_id, c, some, :]
        return send(
            there, there, agb_ss.at[h, d, k, c], agb_rs.at[h, d, k, c], a, at(a, 1 - 2 * d)
        )

    def use(h, j):
        lanes = sumsq.shape[1]
        squares = sumsq[...]
        total = acc[...]
        for c in range(chunks):
            y = y_all[h, j, c]
            if h == 0:
                y = dot(perm[...], y).astype(BF16)
            here = some_cols(h, j, c)
            scaled = y.astype(F32) * invg[:, here]
            scaled = scaled * scaled
            for q in range(chunk // lanes):
                squares += scaled[:, q * lanes : (q + 1) * lanes]
            total += dot_nt(y, wcat[:, here])
        sumsq[...] = squares
        acc[...] = total

    for c in range(chunks):
        for h in (0, 1):
            a, b = axes[h]
            all_but_one(
                y_all.at[h, 0, c, seen_b, :], aga_ss.at[h, c], aga_rs.at[h, c], b
            ).wait_recv()
            for d in (0, 1):
                agb_copy(h, d, 0, c, pos[a], True).start()
    loads[0].wait()
    loads[1].wait()
    for h in (0, 1):
        use(h, pos[axes[h][0]])

    def gather_step(k, carry):
        for c in range(chunks):
            for h in (0, 1):
                for d in (0, 1):
                    j = behind(h, d, k)
                    agb_copy(h, d, k - 1, c, j, True).wait_recv()

                    @pl.when(k < reach - 1)
                    def _():
                        agb_copy(h, d, k, c, j, True).start()

                    @pl.when(k == reach - 1)
                    def _():
                        agb_copy(h, d, k, c, j, False).start()

        for h in (0, 1):
            for d in (0, 1):
                use(h, behind(h, d, k))
        return carry

    lax.fori_loop(1, reach, gather_step, 0)
    for h in (0, 1):
        j = behind(h, 0, reach)
        for d in (0, 1):
            for c in range(chunks):
                agb_copy(h, d, reach - 1, c, j, False).wait_recv()
        use(h, j)

    mean_sq = jnp.sum(sumsq[...], axis=1, keepdims=True) * (1.0 / width)
    factor = lax.rsqrt(mean_sq + 1e-05)

    def branch(base, scale_ref, pick):
        part = acc[:, pl.ds(base, slots)]
        scale = jnp.concatenate([scale_ref[...], jnp.zeros((1, slots - hidden), F32)], axis=1)
        added = jnp.dot(
            part, pick[...], precision=lax.Precision.HIGHEST, preferred_element_type=F32
        )
        return (part * scale + added) * factor

    gate = branch(0, gscale_ref, gpick)
    up = branch(slots, uscale_ref, upick)
    hid[0] = (gate / (1.0 + jnp.exp(-gate)) * up).astype(BF16)
    hid[1] = dot(perm[...], hid[0]).astype(BF16)
    for h in (0, 1):
        added = dot_nt(hid[h], dextp[...])
        high = added.astype(BF16)
        low = (added - high.astype(F32)).astype(BF16)
        lane = lax.broadcasted_iota(jnp.int32, added.shape, 1)
        extra_parts[h] = jnp.where(lane < k_out, high.astype(F32), low.astype(F32)).astype(BF16)
    loads[2].wait()

    def down(h, j, s):
        here = pl.ds(pl.multiple_of(h * half + s * wide, wide), wide)
        some = pl.ds(pl.multiple_of(j * block, block), block)
        base = dot(hid[h, some, :], wd[:, here]) * dscale_ref[:, here]
        return base + dot(extra_parts[h, some, :], onehot[:, here])

    def ring_copy(h, d, m):
        a = axes[h][0]
        return send(
            ring_s.at[h, d, m],
            ring_r.at[h, d, m + pieces],
            ring_ss.at[h, d, m],
            ring_rs.at[h, d, m],
            a,
            at(a, 1 - 2 * d),
        )

    def ring_step(m, carry):
        group = lax.div(m, per)
        within = lax.rem(m, per)
        away = lax.div(n - group, 2)
        odd = lax.rem(group, 2)
        for h in (0, 1):
            for d in (0, 1):
                s = (odd if d == 0 else 1 - odd) * per + within
                shift = n - away if d else away
                j = lax.rem(pos[axes[h][0]] + shift, n)
                value = down(h, j, s)

                @pl.when(m >= pieces)
                def _():
                    ring_copy(h, d, m - pieces).wait_recv()

                ring_s[h, d, m] = (value + ring_r[h, d, m].astype(F32)).astype(BF16)
                ring_copy(h, d, m).start()
        return carry

    lax.fori_loop(0, messages, ring_step, 0)

    def two_copy(h, r):
        b = axes[h][1]
        return send(
            two_s.at[h, at(b, r)], r_two.at[h, r - 1], two_ss.at[h], two_rs.at[h], b, at(b, r)
        )

    for h in (0, 1):
        for s in range(pieces):
            down_sum[h, :, pl.ds(s * wide, wide)] = down(h, pos[axes[h][0]], s)
    for h in (0, 1):
        for d in (0, 1):
            for m in range(messages - pieces, messages):
                ring_copy(h, d, m).wait_recv()
        for s in range(pieces):
            some = pl.ds(s * wide, wide)
            late = messages + per + s % per
            plus = ring_r[h, 0, late - s // per * per].astype(F32)
            minus = ring_r[h, 1, late - per + s // per * per].astype(F32)
            down_sum[h, :, some] = down_sum[h, :, some] + plus + minus
        for j in range(n):
            two_s[h, j] = down_sum[h, pl.ds(j * rows, rows), :].astype(BF16)
        for r in offsets:
            two_copy(h, r).start()

    last = []
    for h in (0, 1):
        a, b = axes[h]
        all_but_one(mix_s.at[h, pl.ds(0, n - 1)], mix_ss.at[h], mix_rs.at[h], a).wait_recv()
        total = mix_r[h] + two_s[h, pos[b]].astype(F32)
        all_but_one(r_two.at[h], two_ss.at[h], two_rs.at[h], b).wait_recv()
        for r in range(1, n):
            total += r_two[h, r - 1].astype(F32)
        here = pl.ds(h * half, half)
        out_v[:, here] = total.astype(BF16)
        last.append(
            pltpu.make_async_copy(out_v.at[:, here], out_ref.at[:, here], load_sem.at[3 * h])
        )
        last[h].start()

    for h in (0, 1):
        a, b = axes[h]
        for d in (0, 1):
            for k in range(reach):
                heads_copy(h, d, k).wait_send()
        all_but_one(strm.at[h, pl.ds(0, n - 1)], strm_ss.at[h], strm_rs.at[h], a).wait_send()
        for c in range(chunks):
            all_but_one(
                w_all.at[h, c, seen_w, mine], w_ss.at[h, c], w_rs.at[h, c], a
            ).wait_send()
            for q in range(1, cores):
                share_copy(h, c, q).wait_send()
            all_but_one(
                y_all.at[h, 0, c, seen_b, :], aga_ss.at[h, c], aga_rs.at[h, c], b
            ).wait_send()
            all_but_one(r_one.at[h, c], one_ss.at[h, c], one_rs.at[h, c], b).wait_send()
        all_but_one(mix_s.at[h, pl.ds(0, n - 1)], mix_ss.at[h], mix_rs.at[h], a).wait_send()
        all_but_one(r_two.at[h], two_ss.at[h], two_rs.at[h], b).wait_send()
        for d in (0, 1):
            for k in range(reach):
                for c in range(chunks):
                    agb_copy(h, d, k, c, behind(h, d, k), k < reach - 1).wait_send()
            for m in range(messages):
                ring_copy(h, d, m).wait_send()
    for copy in last:
        copy.wait()


def local(n, cores, *args):
    (
        heads_out,
        stream_in,
        proj_levels,
        proj_scale,
        norm_gain,
        gate_levels,
        gate_scale,
        gate_index,
        gate_extra,
        up_levels,
        up_scale,
        up_index,
        up_extra,
        down_levels,
        down_scale,
        down_index,
        down_extra,
    ) = args
    tokens, feats = heads_out.shape
    rows, width = stream_in.shape
    hidden = gate_levels.shape[1]
    k_out = gate_extra.shape[1]
    slots = -(-(hidden + k_out) // 128) * 128
    strip = width // 2 // n
    chunks = 2
    pieces = 4
    messages = pieces // 2 * (n - 1)
    chunk = strip // chunks
    block = tokens // n
    reach = n // 2
    index = pltpu.SMEM(gate_index.shape, jnp.int32)
    hbm = pl.BlockSpec(memory_space=pl.ANY)
    dma = pltpu.SemaphoreType.DMA
    scratch = [
        pltpu.VMEM((1, width), F32),
        pltpu.VMEM((1, width), F32),
        pltpu.VMEM((1, hidden), F32),
        index,
        pltpu.VMEM((k_out, width), BF16),
        pltpu.VMEM((1, hidden), F32),
        index,
        pltpu.VMEM((k_out, width), BF16),
        pltpu.VMEM((1, width), F32),
        index,
        pltpu.VMEM((k_out, hidden), BF16),
        pltpu.VMEM((2 * slots, width), BF16),
        pltpu.VMEM((slots, width), BF16),
        pltpu.VMEM((128, width), BF16),
        pltpu.VMEM((tokens, tokens), BF16),
        pltpu.VMEM((slots, slots), F32),
        pltpu.VMEM((slots, slots), F32),
        pltpu.VMEM((128, slots), BF16),
        pltpu.VMEM((1, width), F32),
        pltpu.VMEM((2, n * feats, tokens), BF16),
        pltpu.VMEM((2, tokens, n * feats), BF16),
        pltpu.VMEM((2, chunks, n * feats, chunk), BF16),
        pltpu.VMEM((2, n, rows, strip), BF16),
        pltpu.VMEM((2, chunks, tokens, chunk), F32),
        pltpu.VMEM((2, chunks, tokens, chunk), BF16),
        pltpu.VMEM((2, chunks, n - 1, block, chunk), BF16),
        pltpu.VMEM((2, chunks, block, chunk), F32),
        pltpu.VMEM((2, n, chunks, tokens, chunk), BF16),
        pltpu.VMEM((tokens, 2 * slots), F32),
        pltpu.VMEM((tokens, 128), F32),
        pltpu.VMEM((2, tokens, slots), BF16),
        pltpu.VMEM((2, tokens, 128), BF16),
        pltpu.VMEM((2, 2, messages, block, width // 2 // pieces), BF16),
        pltpu.VMEM((2, 2, messages + pieces, block, width // 2 // pieces), BF16),
        pltpu.VMEM((2, n, rows, width // 2), BF16),
        pltpu.VMEM((2, n - 1, rows, width // 2), BF16),
        pltpu.VMEM((2, n, rows, strip), F32),
        pltpu.VMEM((2, rows, width // 2), F32),
        pltpu.VMEM((2, block, width // 2), F32),
        pltpu.VMEM((rows, width), BF16),
        dma((4 + 2 * chunks + 14,)),
    ]
    scratch += [dma((2, 2, reach)), dma((2, 2, reach)), dma((2, chunks)), dma((2, chunks))]
    scratch += [dma((2, chunks, cores)), dma((2, chunks, cores)), dma((2,)), dma((2,))]
    scratch += [dma((2, chunks)) for _ in range(4)]
    scratch += [dma((2, 2, reach, chunks)), dma((2, 2, reach, chunks))]
    scratch += [dma((2, 2, messages)), dma((2, 2, messages))]
    scratch += [dma((2,)) for _ in range(4)]
    return pl.pallas_call(
        functools.partial(kernel, n, cores),
        out_shape=jax.ShapeDtypeStruct((rows, width), BF16),
        in_specs=[hbm] * len(args),
        out_specs=hbm,
        scratch_shapes=scratch,
        compiler_params=pltpu.CompilerParams(
            collective_id=0, has_side_effects=True, vmem_limit_bytes=60 * 1024 * 1024
        ),
    )(
        heads_out.T,
        stream_in,
        proj_levels,
        proj_scale[None, :],
        norm_gain[None, :],
        gate_levels.T,
        gate_scale[None, :],
        gate_index,
        gate_extra.T,
        up_levels.T,
        up_scale[None, :],
        up_index,
        up_extra.T,
        down_levels,
        down_scale[None, :],
        down_index,
        down_extra.T,
    )


def solution(mesh):
    n = math.isqrt(mesh.shape["tensor"])
    torus = Mesh(
        mesh.devices.reshape(mesh.shape["groups"], n, n, mesh.shape["seq"]),
        ("groups", "tensor_0", "tensor_1", "seq"),
    )
    return jax.shard_map(
        functools.partial(local, n, mesh.shape["seq"]),
        mesh=torus,
        in_specs=(
            P(("groups", "seq"), TENSOR),
            P(GROUPS_SEQ_TENSOR, None),
            P(TENSOR, None),
            P(),
            P(),
            P(None, TENSOR),
            P(TENSOR),
            P(TENSOR, None),
            P(None, TENSOR),
            P(None, TENSOR),
            P(TENSOR),
            P(TENSOR, None),
            P(None, TENSOR),
            P(TENSOR, None),
            P(),
            P(TENSOR, None),
            P(TENSOR, None),
        ),
        out_specs=P(GROUPS_SEQ_TENSOR, None),
        check_vma=False,
    )
```

```python
import functools
import math

import jax
import jax.numpy as jnp
from jax import lax
from jax.experimental import pallas as pl
from jax.experimental.pallas import tpu as pltpu
from jax.sharding import Mesh
from jax.sharding import PartitionSpec as P

TENSOR = ("tensor_0", "tensor_1")
GROUPS_SEQ_TENSOR = ("groups", "seq", "tensor_0", "tensor_1")
MESH = pl.DeviceIdType.MESH
F32 = jnp.float32
BF16 = jnp.bfloat16
NT = (((1,), (1,)), ((), ()))


def dot(a, b):
    return jnp.dot(a, b, preferred_element_type=F32)


def dot_nt(a, b):
    return lax.dot_general(a, b, NT, preferred_element_type=F32)


def kernel(
    n,
    cores,
    heads_ref,
    stream_ref,
    projw_ref,
    pscale_in,
    gain_in,
    gatew_ref,
    gscale_in,
    gidx_in,
    gext_in,
    upw_ref,
    uscale_in,
    uidx_in,
    uext_in,
    downw_ref,
    dscale_in,
    didx_in,
    dext_in,
    out_ref,
    pscale_ref,
    gain_ref,
    gscale_ref,
    gidx_ref,
    gext_ref,
    uscale_ref,
    uidx_ref,
    uext_ref,
    dscale_ref,
    didx_ref,
    dext_ref,
    wcat,
    wd,
    onehot,
    perm,
    gpick,
    upick,
    dextp,
    invg,
    heads_all,
    ordered,
    w_all,
    strm,
    t_sum,
    t_half,
    r_one,
    mixed,
    y_all,
    acc,
    sumsq,
    hid,
    extra_parts,
    ring_s,
    ring_r,
    two_s,
    r_two,
    mix_s,
    mix_r,
    down_sum,
    out_v,
    load_sem,
    heads_ss,
    heads_rs,
    w_ss,
    w_rs,
    share_ss,
    share_rs,
    strm_ss,
    strm_rs,
    one_ss,
    one_rs,
    aga_ss,
    aga_rs,
    agb_ss,
    agb_rs,
    ring_ss,
    ring_rs,
    two_ss,
    two_rs,
    mix_ss,
    mix_rs,
):
    feats, tokens = heads_ref.shape
    width = projw_ref.shape[1]
    hidden = gatew_ref.shape[0]
    chunks = w_all.shape[1]
    chunk = w_all.shape[3]
    part = chunk // cores
    rows = stream_ref.shape[0]
    slots = gpick.shape[0]
    k_out = gext_ref.shape[0]
    half = width // 2
    strip = half // n
    block = tokens // n
    sub = tokens // 2
    wide = ring_s.shape[4]
    pieces = half // wide
    per = pieces // 2
    messages = per * (n - 1)
    reach = n // 2
    axes = (("tensor_0", "tensor_1"), ("tensor_1", "tensor_0"))
    pos = {name: lax.axis_index(name) for name in TENSOR}
    offsets = sorted(range(1, n), key=lambda r: -min(r, n - r))

    def at(name, shift):
        return lax.rem(pos[name] + (shift + n) % n, n)

    def cols(h, j):
        return pl.ds(pl.multiple_of(h * half + j * strip, strip), strip)

    def send(src, dst, ssem, rsem, name, target):
        return pltpu.make_async_remote_copy(
            src_ref=src,
            dst_ref=dst,
            send_sem=ssem,
            recv_sem=rsem,
            device_id={name: target},
            device_id_type=MESH,
        )

    def all_but_one(ref, ssem, rsem, name):
        return send(ref, ref, ssem, rsem, name, at(name, 1))

    core = lax.axis_index("seq")
    barrier = pltpu.get_barrier_semaphore()
    for name in TENSOR:
        for r in range(1, n):
            pl.semaphore_signal(
                barrier, inc=1, device_id={name: at(name, r)}, device_id_type=MESH
            )
    for q in range(1, cores):
        pl.semaphore_signal(
            barrier, inc=1, device_id={"seq": lax.rem(core + q, cores)}, device_id_type=MESH
        )

    def place(sender):
        return pl.ds(pl.multiple_of(sender * feats, feats), feats)

    mine = pl.ds(pl.multiple_of(core * part, part), part)

    def some_cols(h, j, c):
        return pl.ds(pl.multiple_of(h * half + j * strip + c * chunk, chunk), chunk)

    def own_part(h, j, c):
        start = h * half + j * strip + c * chunk + core * part
        return pl.ds(pl.multiple_of(start, part), part)

    first = []
    for h in (0, 1):
        me = pos[axes[h][0]]
        for src, dst in (
            (heads_ref, heads_all.at[h, place(me), :]),
            (stream_ref.at[:, cols(h, me)], strm.at[h, me]),
        ) + tuple(
            (projw_ref.at[:, own_part(h, me, c)], w_all.at[h, c, place(me), mine])
            for c in range(chunks)
        ):
            first.append(pltpu.make_async_copy(src, dst, load_sem.at[len(first)]))
            first[-1].start()
    pl.semaphore_wait(barrier, 2 * (n - 1) + cores - 1)

    def heads_copy(h, r):
        a = axes[h][0]
        there = heads_all.at[h, place(pos[a]), :]
        return send(there, there, heads_ss.at[0], heads_rs.at[h], a, at(a, r))

    def w_copy(h, c, r):
        a = axes[h][0]
        return send(
            projw_ref.at[:, own_part(h, at(a, r), c)],
            w_all.at[h, c, place(pos[a]), mine],
            w_ss.at[0],
            w_rs.at[h, c],
            a,
            at(a, r),
        )

    def share_copy(h, c, q):
        there = w_all.at[h, c, :, mine]
        to = lax.rem(core + q, cores)
        return send(there, there, share_ss.at[q - 1], share_rs.at[h, c, q - 1], "seq", to)

    def strm_copy(h, r):
        a = axes[h][0]
        return send(
            stream_ref.at[:, cols(h, at(a, r))],
            strm.at[h, pos[a]],
            strm_ss.at[0],
            strm_rs.at[h],
            a,
            at(a, r),
        )

    each = 2 + chunks
    for c in range(chunks):
        for r in offsets:
            for h in (0, 1):
                w_copy(h, c, r).start()
        if c == 0:
            for h in (0, 1):
                first[each * h].wait()
            for r in offsets:
                for h in (0, 1):
                    heads_copy(h, r).start()
    for r in offsets:
        for h in (0, 1):
            strm_copy(h, r).start()
    small = []
    for src, dst in (
        (pscale_in, pscale_ref),
        (gain_in, gain_ref),
        (gscale_in, gscale_ref),
        (gidx_in, gidx_ref),
        (gext_in, gext_ref),
        (uscale_in, uscale_ref),
        (uidx_in, uidx_ref),
        (uext_in, uext_ref),
        (dscale_in, dscale_ref),
        (didx_in, didx_ref),
        (dext_in, dext_ref),
    ):
        small.append(pltpu.make_async_copy(src, dst, load_sem.at[len(first) + len(small)]))
        small[-1].start()
    base = len(first) + len(small)
    loads = [
        pltpu.make_async_copy(gatew_ref, wcat.at[pl.ds(0, hidden), :], load_sem.at[base]),
        pltpu.make_async_copy(upw_ref, wcat.at[pl.ds(slots, hidden), :], load_sem.at[base + 1]),
        pltpu.make_async_copy(downw_ref, wd.at[pl.ds(0, hidden), :], load_sem.at[base + 2]),
    ]
    for load in loads:
        load.start()

    for copy in small:
        copy.wait()
    r_i = lax.broadcasted_iota(jnp.int32, (tokens, tokens), 0)
    c_i = lax.broadcasted_iota(jnp.int32, (tokens, tokens), 1)
    swapped = (
        lax.rem(lax.div(r_i, rows), n) * block + lax.div(r_i, block) * rows + lax.rem(r_i, rows)
    )
    perm[...] = jnp.where(c_i == swapped, 1.0, 0.0).astype(BF16)

    def index_column(idx_ref, count):
        row = lax.rem(lax.broadcasted_iota(jnp.int32, (count, 1), 0), k_out)
        column = jnp.zeros((count, 1), jnp.int32)
        for k in range(k_out):
            column = jnp.where(row == k, idx_ref[0, k], column)
        return column

    for pick, idx_ref in ((gpick, gidx_ref), (upick, uidx_ref)):
        pick[...] = jnp.zeros_like(pick)
        chosen = lax.broadcasted_iota(jnp.int32, (k_out, slots), 1) == index_column(idx_ref, k_out)
        pick[pl.ds(hidden, k_out), :] = jnp.where(chosen, 1.0, 0.0)

    one_rows = onehot.shape[0]
    didx = index_column(didx_ref, one_rows)
    live = lax.broadcasted_iota(jnp.int32, (one_rows, strip), 0) < 2 * k_out

    def prepare(j, carry):
        here = pl.ds(pl.multiple_of(j * strip, strip), strip)
        column = lax.broadcasted_iota(jnp.int32, (one_rows, strip), 1) + j * strip
        onehot[:, here] = jnp.where((column == didx) & live, 1.0, 0.0).astype(BF16)
        blank = jnp.zeros((slots - hidden - k_out, strip), F32)
        for base, ext in ((0, gext_ref), (slots, uext_ref)):
            filled = jnp.concatenate([ext[:, here].astype(F32), blank], axis=0)
            wcat[pl.ds(base + hidden, slots - hidden), here] = filled.astype(BF16)
        wd[pl.ds(hidden, slots - hidden), here] = jnp.zeros((slots - hidden, strip), BF16)
        invg[:, here] = 1.0 / gain_ref[:, here]
        return carry

    lax.fori_loop(0, width // strip, prepare, 0)
    dext = jnp.concatenate([dext_ref[...].astype(F32)] * 2, axis=0)
    dext = jnp.concatenate([dext, jnp.zeros((dextp.shape[0] - 2 * k_out, hidden), F32)], axis=0)
    dextp[...] = jnp.zeros_like(dextp)
    dextp[:, pl.ds(0, hidden)] = dext.astype(BF16)
    acc[...] = jnp.zeros_like(acc)
    sumsq[...] = jnp.zeros_like(sumsq)
    for h in (0, 1):
        for d in (0, 1):
            for m in range(pieces):
                ring_r[h, d, m] = jnp.zeros((block, wide), BF16)

    def one_copy(h, c, r):
        b = axes[h][1]
        away = pl.ds(pl.multiple_of(at(b, r) * block, block), block)
        return send(
            t_half.at[h, c, away, :],
            r_one.at[h, c, r - 1],
            one_ss.at[0],
            one_rs.at[h, c],
            b,
            at(b, r),
        )

    seen_w = pl.ds(0, (n - 1) * feats)
    seen_b = pl.ds(0, (n - 1) * block)
    for c in range(chunks):
        for h in (0, 1):
            a = axes[h][0]
            first[each * h + 2 + c].wait()
            all_but_one(
                w_all.at[h, c, seen_w, mine], w_ss.at[0], w_rs.at[h, c], a
            ).wait_recv()
            for q in range(1, cores):
                share_copy(h, c, q).start()
        for h in (0, 1):
            a = axes[h][0]
            if c == 0:
                all_but_one(
                    heads_all.at[h, seen_w, :], heads_ss.at[0], heads_rs.at[h], a
                ).wait_recv()
                if h == 0:
                    turn = perm[...]
                else:
                    turn = jnp.where(r_i == c_i, 1.0, 0.0).astype(BF16)
                ordered[h] = dot_nt(turn, heads_all[h]).astype(BF16)
            for q in range(1, cores):
                share_copy(h, c, q).wait_recv()
            t_sum[h, c] = dot(ordered[h], w_all[h, c])
            t_half[h, c] = t_sum[h, c].astype(BF16)
            for r in offsets:
                one_copy(h, c, r).start()

    def aga_copy(h, c, r):
        a, b = axes[h]
        own = pl.ds(pl.multiple_of(pos[b] * block, block), block)
        there = y_all.at[h, pos[a], c, own, :]
        return send(there, there, aga_ss.at[0], aga_rs.at[h, c], b, at(b, r))

    def mix_copy(h, r):
        a = axes[h][0]
        there = mix_r.at[h, :, pl.ds(pl.multiple_of(pos[a] * strip, strip), strip)]
        return send(mix_s.at[h, at(a, r)], there, mix_ss.at[0], mix_rs.at[h], a, at(a, r))

    for c in range(chunks):
        for h in (0, 1):
            a, b = axes[h]
            here = some_cols(h, pos[a], c)
            within = pl.ds(c * chunk, chunk)
            own = pl.ds(pl.multiple_of(pos[b] * block, block), block)
            total = t_sum[h, c, own, :]
            if c == 0:
                first[each * h + 1].wait()
                all_but_one(
                    strm.at[h, pl.ds(0, n - 1)], strm_ss.at[0], strm_rs.at[h], a
                ).wait_recv()
            all_but_one(r_one.at[h, c], one_ss.at[0], one_rs.at[h, c], b).wait_recv()
            for r in range(1, n):
                total += r_one[h, c, r - 1].astype(F32)
            mixed[h, c] = total * pscale_ref[:, here]
            for j in range(n):
                few = pl.ds(j * rows, rows)
                mixed[h, c, few, :] = mixed[h, c, few, :] + strm[h, j, :, within].astype(F32)
            y_all[h, pos[a], c, own, :] = (mixed[h, c] * gain_ref[:, here]).astype(BF16)
            for r in offsets:
                aga_copy(h, c, r).start()
            for j in range(n):
                mix_s[h, j, :, within] = mixed[h, c, pl.ds(j * rows, rows), :]
    def agb_copy(h, d, k, c, strip_id, whole):
        a = axes[h][0]
        some = pl.ds(0, tokens) if whole else pl.ds(d * sub, sub)
        there = y_all.at[h, strip_id, c, some, :]
        return send(
            there, there, agb_ss.at[0], agb_rs.at[h, d, k, c], a, at(a, 1 - 2 * d)
        )

    def behind(h, d, k):
        shift = k if d else n - k
        return lax.rem(pos[axes[h][0]] + shift, n)

    def use(h, j):
        lanes = sumsq.shape[1]
        squares = sumsq[...]
        total = acc[...]
        for c in range(chunks):
            y = y_all[h, j, c]
            if h == 0:
                y = dot(perm[...], y).astype(BF16)
            here = some_cols(h, j, c)
            scaled = y.astype(F32) * invg[:, here]
            scaled = scaled * scaled
            for q in range(chunk // lanes):
                squares += scaled[:, q * lanes : (q + 1) * lanes]
            total += dot_nt(y, wcat[:, here])
        sumsq[...] = squares
        acc[...] = total

    for c in range(chunks):
        for h in (0, 1):
            a, b = axes[h]
            all_but_one(
                y_all.at[h, 0, c, seen_b, :], aga_ss.at[0], aga_rs.at[h, c], b
            ).wait_recv()
            for d in (0, 1):
                agb_copy(h, d, 0, c, pos[a], True).start()
    loads[0].wait()
    loads[1].wait()
    for h in (0, 1):
        use(h, pos[axes[h][0]])

    def gather_step(k, carry):
        for c in range(chunks):
            for h in (0, 1):
                for d in (0, 1):
                    j = behind(h, d, k)
                    agb_copy(h, d, k - 1, c, j, True).wait_recv()

                    @pl.when(k < reach - 1)
                    def _():
                        agb_copy(h, d, k, c, j, True).start()

                    @pl.when(k == reach - 1)
                    def _():
                        agb_copy(h, d, k, c, j, False).start()

        for h in (0, 1):
            for d in (0, 1):
                use(h, behind(h, d, k))
        return carry

    lax.fori_loop(1, reach, gather_step, 0)
    for h in (0, 1):
        me = pos[axes[h][0]]
        for r in offsets:
            mix_copy(h, r).start()
        mix_r[h, :, pl.ds(pl.multiple_of(me * strip, strip), strip)] = mix_s[h, me]
    for h in (0, 1):
        j = behind(h, 0, reach)
        for d in (0, 1):
            for c in range(chunks):
                agb_copy(h, d, reach - 1, c, j, False).wait_recv()
        use(h, j)

    mean_sq = jnp.sum(sumsq[...], axis=1, keepdims=True) * (1.0 / width)
    factor = lax.rsqrt(mean_sq + 1e-05)

    def branch(base, scale_ref, pick):
        part = acc[:, pl.ds(base, slots)]
        scale = jnp.concatenate([scale_ref[...], jnp.zeros((1, slots - hidden), F32)], axis=1)
        added = jnp.dot(
            part, pick[...], precision=lax.Precision.HIGHEST, preferred_element_type=F32
        )
        return (part * scale + added) * factor

    gate = branch(0, gscale_ref, gpick)
    up = branch(slots, uscale_ref, upick)
    hid[0] = (gate / (1.0 + jnp.exp(-gate)) * up).astype(BF16)
    hid[1] = dot(perm[...], hid[0]).astype(BF16)
    for h in (0, 1):
        added = dot_nt(hid[h], dextp[...])
        high = added.astype(BF16)
        low = (added - high.astype(F32)).astype(BF16)
        lane = lax.broadcasted_iota(jnp.int32, added.shape, 1)
        extra_parts[h] = jnp.where(lane < k_out, high.astype(F32), low.astype(F32)).astype(BF16)
    loads[2].wait()

    def down(h, j, s):
        here = pl.ds(pl.multiple_of(h * half + s * wide, wide), wide)
        some = pl.ds(pl.multiple_of(j * block, block), block)
        base = dot(hid[h, some, :], wd[:, here]) * dscale_ref[:, here]
        return base + dot(extra_parts[h, some, :], onehot[:, here])

    def ring_copy(h, d, m):
        a = axes[h][0]
        return send(
            ring_s.at[h, d, m],
            ring_r.at[h, d, m + pieces],
            ring_ss.at[0],
            ring_rs.at[h, d, m],
            a,
            at(a, 1 - 2 * d),
        )

    def ring_step(m, carry):
        group = lax.div(m, per)
        within = lax.rem(m, per)
        away = lax.div(n - group, 2)
        odd = lax.rem(group, 2)
        for h in (0, 1):
            for d in (0, 1):
                s = (odd if d == 0 else 1 - odd) * per + within
                shift = n - away if d else away
                j = lax.rem(pos[axes[h][0]] + shift, n)
                value = down(h, j, s)

                @pl.when(m >= pieces)
                def _():
                    ring_copy(h, d, m - pieces).wait_recv()

                ring_s[h, d, m] = (value + ring_r[h, d, m].astype(F32)).astype(BF16)
                ring_copy(h, d, m).start()
        return carry

    lax.fori_loop(0, messages, ring_step, 0)

    def two_copy(h, p, r):
        b = axes[h][1]
        return send(
            two_s.at[h, p, at(b, r)],
            r_two.at[h, p, r - 1],
            two_ss.at[0],
            two_rs.at[h, p],
            b,
            at(b, r),
        )

    for h in (0, 1):
        for s in range(pieces):
            down_sum[h, s] = down(h, pos[axes[h][0]], s)
    for p in range(per):
        for h in (0, 1):
            for d in (0, 1):
                for m in (messages - pieces + p, messages - per + p):
                    ring_copy(h, d, m).wait_recv()
            for q in (0, 1):
                s = q * per + p
                plus = ring_r[h, 0, messages + (1 - q) * per + p].astype(F32)
                minus = ring_r[h, 1, messages + q * per + p].astype(F32)
                down_sum[h, s] = down_sum[h, s] + plus + minus
                for j in range(n):
                    few = down_sum[h, s, pl.ds(j * rows, rows), :]
                    two_s[h, p, j, :, pl.ds(q * wide, wide)] = few.astype(BF16)
            for r in offsets:
                two_copy(h, p, r).start()

    last = []
    for h in (0, 1):
        a = axes[h][0]
        all_but_one(mix_s.at[h, pl.ds(0, n - 1)], mix_ss.at[0], mix_rs.at[h], a).wait_recv()
    for p in range(per):
        for h in (0, 1):
            b = axes[h][1]
            total = two_s[h, p, pos[b]].astype(F32)
            all_but_one(r_two.at[h, p], two_ss.at[0], two_rs.at[h, p], b).wait_recv()
            for r in range(1, n):
                total += r_two[h, p, r - 1].astype(F32)
            for q in (0, 1):
                here = (q * per + p) * wide
                value = total[:, q * wide : (q + 1) * wide] + mix_r[h, :, pl.ds(here, wide)]
                out_v[:, pl.ds(h * half + here, wide)] = value.astype(BF16)
    for h in (0, 1):
        here = pl.ds(h * half, half)
        last.append(
            pltpu.make_async_copy(out_v.at[:, here], out_ref.at[:, here], load_sem.at[3 * h])
        )
        last[h].start()

    def all_sent(ref, ssem, rsem):
        send(ref, ref, ssem, rsem, TENSOR[0], at(TENSOR[0], 1)).wait_send()

    most = pl.ds(0, n - 1)
    all_sent(heads_all.at[:, seen_w, :], heads_ss.at[0], heads_rs.at[0])
    all_sent(w_all.at[:, :, seen_w, mine], w_ss.at[0], w_rs.at[0, 0])
    for q in range(1, cores):
        all_sent(w_all.at[:, :, :, mine], share_ss.at[q - 1], share_rs.at[0, 0, q - 1])
    all_sent(strm.at[:, most], strm_ss.at[0], strm_rs.at[0])
    all_sent(r_one, one_ss.at[0], one_rs.at[0, 0])
    all_sent(y_all.at[:, 0, :, seen_b, :], aga_ss.at[0], aga_rs.at[0, 0])
    all_sent(y_all.at[:, most], agb_ss.at[0], agb_rs.at[0, 0, 0, 0])
    all_sent(mix_s.at[:, most], mix_ss.at[0], mix_rs.at[0])
    all_sent(ring_s, ring_ss.at[0], ring_rs.at[0, 0, 0])
    all_sent(r_two, two_ss.at[0], two_rs.at[0, 0])
    for copy in last:
        copy.wait()


def local(n, cores, *args):
    (
        heads_out,
        stream_in,
        proj_levels,
        proj_scale,
        norm_gain,
        gate_levels,
        gate_scale,
        gate_index,
        gate_extra,
        up_levels,
        up_scale,
        up_index,
        up_extra,
        down_levels,
        down_scale,
        down_index,
        down_extra,
    ) = args
    tokens, feats = heads_out.shape
    rows, width = stream_in.shape
    hidden = gate_levels.shape[1]
    k_out = gate_extra.shape[1]
    slots = -(-(hidden + k_out) // 128) * 128
    strip = width // 2 // n
    chunks = 2
    pieces = 4
    messages = pieces // 2 * (n - 1)
    chunk = strip // chunks
    block = tokens // n
    reach = n // 2
    index = pltpu.SMEM(gate_index.shape, jnp.int32)
    hbm = pl.BlockSpec(memory_space=pl.ANY)
    dma = pltpu.SemaphoreType.DMA
    scratch = [
        pltpu.VMEM((1, width), F32),
        pltpu.VMEM((1, width), F32),
        pltpu.VMEM((1, hidden), F32),
        index,
        pltpu.VMEM((k_out, width), BF16),
        pltpu.VMEM((1, hidden), F32),
        index,
        pltpu.VMEM((k_out, width), BF16),
        pltpu.VMEM((1, width), F32),
        index,
        pltpu.VMEM((k_out, hidden), BF16),
        pltpu.VMEM((2 * slots, width), BF16),
        pltpu.VMEM((slots, width), BF16),
        pltpu.VMEM((128, width), BF16),
        pltpu.VMEM((tokens, tokens), BF16),
        pltpu.VMEM((slots, slots), F32),
        pltpu.VMEM((slots, slots), F32),
        pltpu.VMEM((128, slots), BF16),
        pltpu.VMEM((1, width), F32),
        pltpu.VMEM((2, n * feats, tokens), BF16),
        pltpu.VMEM((2, tokens, n * feats), BF16),
        pltpu.VMEM((2, chunks, n * feats, chunk), BF16),
        pltpu.VMEM((2, n, rows, strip), BF16),
        pltpu.VMEM((2, chunks, tokens, chunk), F32),
        pltpu.VMEM((2, chunks, tokens, chunk), BF16),
        pltpu.VMEM((2, chunks, n - 1, block, chunk), BF16),
        pltpu.VMEM((2, chunks, block, chunk), F32),
        pltpu.VMEM((2, n, chunks, tokens, chunk), BF16),
        pltpu.VMEM((tokens, 2 * slots), F32),
        pltpu.VMEM((tokens, 128), F32),
        pltpu.VMEM((2, tokens, slots), BF16),
        pltpu.VMEM((2, tokens, 128), BF16),
        pltpu.VMEM((2, 2, messages, block, width // 2 // pieces), BF16),
        pltpu.VMEM((2, 2, messages + pieces, block, width // 2 // pieces), BF16),
        pltpu.VMEM((2, pieces // 2, n, rows, width // pieces), BF16),
        pltpu.VMEM((2, pieces // 2, n - 1, rows, width // pieces), BF16),
        pltpu.VMEM((2, n, rows, strip), F32),
        pltpu.VMEM((2, rows, width // 2), F32),
        pltpu.VMEM((2, pieces, block, width // 2 // pieces), F32),
        pltpu.VMEM((rows, width), BF16),
        dma((4 + 2 * chunks + 14,)),
    ]
    for sends, receives in (
        (1, (2,)),
        (1, (2, chunks)),
        (cores, (2, chunks, cores)),
        (1, (2,)),
        (1, (2, chunks)),
        (1, (2, chunks)),
        (1, (2, 2, reach, chunks)),
        (1, (2, 2, messages)),
        (1, (2, pieces // 2)),
        (1, (2,)),
    ):
        scratch += [dma((sends,)), dma(receives)]
    return pl.pallas_call(
        functools.partial(kernel, n, cores),
        out_shape=jax.ShapeDtypeStruct((rows, width), BF16),
        in_specs=[hbm] * len(args),
        out_specs=hbm,
        scratch_shapes=scratch,
        compiler_params=pltpu.CompilerParams(
            collective_id=0, has_side_effects=True, vmem_limit_bytes=60 * 1024 * 1024
        ),
    )(
        heads_out.T,
        stream_in,
        proj_levels,
        proj_scale[None, :],
        norm_gain[None, :],
        gate_levels.T,
        gate_scale[None, :],
        gate_index,
        gate_extra.T,
        up_levels.T,
        up_scale[None, :],
        up_index,
        up_extra.T,
        down_levels,
        down_scale[None, :],
        down_index,
        down_extra.T,
    )


def solution(mesh):
    n = math.isqrt(mesh.shape["tensor"])
    torus = Mesh(
        mesh.devices.reshape(mesh.shape["groups"], n, n, mesh.shape["seq"]),
        ("groups", "tensor_0", "tensor_1", "seq"),
    )
    return jax.shard_map(
        functools.partial(local, n, mesh.shape["seq"]),
        mesh=torus,
        in_specs=(
            P(("groups", "seq"), TENSOR),
            P(GROUPS_SEQ_TENSOR, None),
            P(TENSOR, None),
            P(),
            P(),
            P(None, TENSOR),
            P(TENSOR),
            P(TENSOR, None),
            P(None, TENSOR),
            P(None, TENSOR),
            P(TENSOR),
            P(TENSOR, None),
            P(None, TENSOR),
            P(TENSOR, None),
            P(),
            P(TENSOR, None),
            P(TENSOR, None),
        ),
        out_specs=P(GROUPS_SEQ_TENSOR, None),
        check_vma=False,
    )
```

```python
import functools
import math

import jax
import jax.numpy as jnp
from jax import lax
from jax.experimental import pallas as pl
from jax.experimental.pallas import tpu as pltpu
from jax.sharding import Mesh
from jax.sharding import PartitionSpec as P

TENSOR = ("tensor_0", "tensor_1")
GROUPS_SEQ_TENSOR = ("groups", "seq", "tensor_0", "tensor_1")
MESH = pl.DeviceIdType.MESH
F32 = jnp.float32
BF16 = jnp.bfloat16
NT = (((1,), (1,)), ((), ()))


def dot(a, b):
    return jnp.dot(a, b, preferred_element_type=F32)


def dot_nt(a, b):
    return lax.dot_general(a, b, NT, preferred_element_type=F32)


def kernel(
    n,
    cores,
    heads_ref,
    stream_ref,
    projw_ref,
    pscale_in,
    gain_in,
    gatew_ref,
    gscale_in,
    gidx_in,
    gext_in,
    upw_ref,
    uscale_in,
    uidx_in,
    uext_in,
    downw_ref,
    dscale_in,
    didx_in,
    dext_in,
    out_ref,
    pscale_ref,
    gain_ref,
    gscale_ref,
    gidx_ref,
    gext_ref,
    uscale_ref,
    uidx_ref,
    uext_ref,
    dscale_ref,
    didx_ref,
    dext_ref,
    wcat,
    wd,
    onehot,
    perm,
    gpick,
    upick,
    dextp,
    invg,
    heads_all,
    ordered,
    w_all,
    strm,
    t_sum,
    t_half,
    r_one,
    mixed,
    y_all,
    acc,
    sumsq,
    hid,
    extra_parts,
    ring_s,
    ring_r,
    two_s,
    r_two,
    mix_s,
    mix_r,
    down_sum,
    load_sem,
    heads_ss,
    heads_rs,
    w_ss,
    w_rs,
    share_ss,
    share_rs,
    strm_ss,
    strm_rs,
    one_ss,
    one_rs,
    aga_ss,
    aga_rs,
    agb_ss,
    agb_rs,
    ring_ss,
    ring_rs,
    two_ss,
    two_rs,
    mix_ss,
    mix_rs,
):
    feats, tokens = heads_ref.shape
    width = projw_ref.shape[1]
    hidden = gatew_ref.shape[0]
    chunks = w_all.shape[1]
    chunk = w_all.shape[3]
    part = chunk // cores
    rows = stream_ref.shape[0]
    slots = gpick.shape[0]
    k_out = gext_ref.shape[0]
    half = width // 2
    strip = half // n
    block = tokens // n
    sub = tokens // 2
    wide = ring_s.shape[4]
    pieces = half // wide
    per = pieces // 2
    messages = per * (n - 1)
    reach = n // 2
    axes = (("tensor_0", "tensor_1"), ("tensor_1", "tensor_0"))
    pos = {name: lax.axis_index(name) for name in TENSOR}
    offsets = sorted(range(1, n), key=lambda r: -min(r, n - r))

    def at(name, shift):
        return lax.rem(pos[name] + (shift + n) % n, n)

    def cols(h, j):
        return pl.ds(pl.multiple_of(h * half + j * strip, strip), strip)

    def send(src, dst, ssem, rsem, name, target):
        return pltpu.make_async_remote_copy(
            src_ref=src,
            dst_ref=dst,
            send_sem=ssem,
            recv_sem=rsem,
            device_id={name: target},
            device_id_type=MESH,
        )

    def all_but_one(ref, ssem, rsem, name):
        return send(ref, ref, ssem, rsem, name, at(name, 1))

    core = lax.axis_index("seq")
    barrier = pltpu.get_barrier_semaphore()
    for name in TENSOR:
        for r in range(1, n):
            pl.semaphore_signal(
                barrier, inc=1, device_id={name: at(name, r)}, device_id_type=MESH
            )
    for q in range(1, cores):
        pl.semaphore_signal(
            barrier, inc=1, device_id={"seq": lax.rem(core + q, cores)}, device_id_type=MESH
        )

    def place(sender):
        return pl.ds(pl.multiple_of(sender * feats, feats), feats)

    mine = pl.ds(pl.multiple_of(core * part, part), part)

    def some_cols(h, j, c):
        return pl.ds(pl.multiple_of(h * half + j * strip + c * chunk, chunk), chunk)

    def own_part(h, j, c):
        start = h * half + j * strip + c * chunk + core * part
        return pl.ds(pl.multiple_of(start, part), part)

    first = []
    for h in (0, 1):
        me = pos[axes[h][0]]
        for src, dst in (
            (heads_ref, heads_all.at[h, place(me), :]),
            (stream_ref.at[:, cols(h, me)], strm.at[h, me]),
        ) + tuple(
            (projw_ref.at[:, own_part(h, me, c)], w_all.at[h, c, place(me), mine])
            for c in range(chunks)
        ):
            first.append(pltpu.make_async_copy(src, dst, load_sem.at[len(first)]))
            first[-1].start()
    pl.semaphore_wait(barrier, 2 * (n - 1) + cores - 1)

    def heads_copy(h, r):
        a = axes[h][0]
        there = heads_all.at[h, place(pos[a]), :]
        return send(there, there, heads_ss.at[0], heads_rs.at[h], a, at(a, r))

    def w_copy(h, c, r):
        a = axes[h][0]
        return send(
            projw_ref.at[:, own_part(h, at(a, r), c)],
            w_all.at[h, c, place(pos[a]), mine],
            w_ss.at[0],
            w_rs.at[h, c],
            a,
            at(a, r),
        )

    def share_copy(h, c, q):
        there = w_all.at[h, c, :, mine]
        to = lax.rem(core + q, cores)
        return send(there, there, share_ss.at[q - 1], share_rs.at[h, c, q - 1], "seq", to)

    def strm_copy(h, r):
        a = axes[h][0]
        return send(
            stream_ref.at[:, cols(h, at(a, r))],
            strm.at[h, pos[a]],
            strm_ss.at[0],
            strm_rs.at[h],
            a,
            at(a, r),
        )

    each = 2 + chunks
    for c in range(chunks):
        for r in offsets:
            for h in (0, 1):
                w_copy(h, c, r).start()
        if c == 0:
            for h in (0, 1):
                first[each * h].wait()
            for r in offsets:
                for h in (0, 1):
                    heads_copy(h, r).start()
    for r in offsets:
        for h in (0, 1):
            strm_copy(h, r).start()
    small = []
    for src, dst in (
        (pscale_in, pscale_ref),
        (gain_in, gain_ref),
        (gscale_in, gscale_ref),
        (gidx_in, gidx_ref),
        (gext_in, gext_ref),
        (uscale_in, uscale_ref),
        (uidx_in, uidx_ref),
        (uext_in, uext_ref),
        (dscale_in, dscale_ref),
        (didx_in, didx_ref),
        (dext_in, dext_ref),
    ):
        small.append(pltpu.make_async_copy(src, dst, load_sem.at[len(first) + len(small)]))
        small[-1].start()
    base = len(first) + len(small)
    loads = [
        pltpu.make_async_copy(gatew_ref, wcat.at[pl.ds(0, hidden), :], load_sem.at[base]),
        pltpu.make_async_copy(upw_ref, wcat.at[pl.ds(slots, hidden), :], load_sem.at[base + 1]),
        pltpu.make_async_copy(downw_ref, wd.at[pl.ds(0, hidden), :], load_sem.at[base + 2]),
    ]
    for load in loads:
        load.start()

    for copy in small:
        copy.wait()
    r_i = lax.broadcasted_iota(jnp.int32, (tokens, tokens), 0)
    c_i = lax.broadcasted_iota(jnp.int32, (tokens, tokens), 1)
    swapped = (
        lax.rem(lax.div(r_i, rows), n) * block + lax.div(r_i, block) * rows + lax.rem(r_i, rows)
    )
    perm[...] = jnp.where(c_i == swapped, 1.0, 0.0).astype(BF16)

    def index_column(idx_ref, count):
        row = lax.rem(lax.broadcasted_iota(jnp.int32, (count, 1), 0), k_out)
        column = jnp.zeros((count, 1), jnp.int32)
        for k in range(k_out):
            column = jnp.where(row == k, idx_ref[0, k], column)
        return column

    for pick, idx_ref in ((gpick, gidx_ref), (upick, uidx_ref)):
        pick[...] = jnp.zeros_like(pick)
        chosen = lax.broadcasted_iota(jnp.int32, (k_out, slots), 1) == index_column(idx_ref, k_out)
        pick[pl.ds(hidden, k_out), :] = jnp.where(chosen, 1.0, 0.0)

    one_rows = onehot.shape[0]
    didx = index_column(didx_ref, one_rows)
    live = lax.broadcasted_iota(jnp.int32, (one_rows, strip), 0) < 2 * k_out

    def prepare(j, carry):
        here = pl.ds(pl.multiple_of(j * strip, strip), strip)
        column = lax.broadcasted_iota(jnp.int32, (one_rows, strip), 1) + j * strip
        onehot[:, here] = jnp.where((column == didx) & live, 1.0, 0.0).astype(BF16)
        blank = jnp.zeros((slots - hidden - k_out, strip), F32)
        for base, ext in ((0, gext_ref), (slots, uext_ref)):
            filled = jnp.concatenate([ext[:, here].astype(F32), blank], axis=0)
            wcat[pl.ds(base + hidden, slots - hidden), here] = filled.astype(BF16)
        wd[pl.ds(hidden, slots - hidden), here] = jnp.zeros((slots - hidden, strip), BF16)
        invg[:, here] = 1.0 / gain_ref[:, here]
        return carry

    lax.fori_loop(0, width // strip, prepare, 0)
    dext = jnp.concatenate([dext_ref[...].astype(F32)] * 2, axis=0)
    dext = jnp.concatenate([dext, jnp.zeros((dextp.shape[0] - 2 * k_out, hidden), F32)], axis=0)
    dextp[...] = jnp.zeros_like(dextp)
    dextp[:, pl.ds(0, hidden)] = dext.astype(BF16)
    acc[...] = jnp.zeros_like(acc)
    sumsq[...] = jnp.zeros_like(sumsq)
    for h in (0, 1):
        for d in (0, 1):
            for m in range(pieces):
                ring_r[h, d, m] = jnp.zeros((block, wide), BF16)

    def one_copy(h, c, r):
        b = axes[h][1]
        away = pl.ds(pl.multiple_of(at(b, r) * block, block), block)
        return send(
            t_half.at[h, c, away, :],
            r_one.at[h, c, r - 1],
            one_ss.at[0],
            one_rs.at[h, c],
            b,
            at(b, r),
        )

    seen_w = pl.ds(0, (n - 1) * feats)
    seen_b = pl.ds(0, (n - 1) * block)
    for c in range(chunks):
        for h in (0, 1):
            a = axes[h][0]
            first[each * h + 2 + c].wait()
            all_but_one(
                w_all.at[h, c, seen_w, mine], w_ss.at[0], w_rs.at[h, c], a
            ).wait_recv()
            for q in range(1, cores):
                share_copy(h, c, q).start()
        for h in (0, 1):
            a = axes[h][0]
            if c == 0:
                all_but_one(
                    heads_all.at[h, seen_w, :], heads_ss.at[0], heads_rs.at[h], a
                ).wait_recv()
                if h == 0:
                    turn = perm[...]
                else:
                    turn = jnp.where(r_i == c_i, 1.0, 0.0).astype(BF16)
                ordered[h] = dot_nt(turn, heads_all[h]).astype(BF16)
            for q in range(1, cores):
                share_copy(h, c, q).wait_recv()
            t_sum[h, c] = dot(ordered[h], w_all[h, c])
            t_half[h, c] = t_sum[h, c].astype(BF16)
            for r in offsets:
                one_copy(h, c, r).start()

    def aga_copy(h, c, r):
        a, b = axes[h]
        own = pl.ds(pl.multiple_of(pos[b] * block, block), block)
        there = y_all.at[h, pos[a], c, own, :]
        return send(there, there, aga_ss.at[0], aga_rs.at[h, c], b, at(b, r))

    def mix_copy(h, r):
        a = axes[h][0]
        there = mix_r.at[h, :, pl.ds(pl.multiple_of(pos[a] * strip, strip), strip)]
        return send(mix_s.at[h, at(a, r)], there, mix_ss.at[0], mix_rs.at[h], a, at(a, r))

    for c in range(chunks):
        for h in (0, 1):
            a, b = axes[h]
            here = some_cols(h, pos[a], c)
            within = pl.ds(c * chunk, chunk)
            own = pl.ds(pl.multiple_of(pos[b] * block, block), block)
            total = t_sum[h, c, own, :]
            if c == 0:
                first[each * h + 1].wait()
                all_but_one(
                    strm.at[h, pl.ds(0, n - 1)], strm_ss.at[0], strm_rs.at[h], a
                ).wait_recv()
            all_but_one(r_one.at[h, c], one_ss.at[0], one_rs.at[h, c], b).wait_recv()
            for r in range(1, n):
                total += r_one[h, c, r - 1].astype(F32)
            mixed[h, c] = total * pscale_ref[:, here]
            for j in range(n):
                few = pl.ds(j * rows, rows)
                mixed[h, c, few, :] = mixed[h, c, few, :] + strm[h, j, :, within].astype(F32)
            y_all[h, pos[a], c, own, :] = (mixed[h, c] * gain_ref[:, here]).astype(BF16)
            for r in offsets:
                aga_copy(h, c, r).start()
            for j in range(n):
                mix_s[h, j, :, within] = mixed[h, c, pl.ds(j * rows, rows), :]
    def agb_copy(h, d, k, c, strip_id, whole):
        a = axes[h][0]
        some = pl.ds(0, tokens) if whole else pl.ds(d * sub, sub)
        there = y_all.at[h, strip_id, c, some, :]
        return send(
            there, there, agb_ss.at[0], agb_rs.at[h, d, k, c], a, at(a, 1 - 2 * d)
        )

    def behind(h, d, k):
        shift = k if d else n - k
        return lax.rem(pos[axes[h][0]] + shift, n)

    def use(h, j):
        lanes = sumsq.shape[1]
        squares = sumsq[...]
        total = acc[...]
        for c in range(chunks):
            y = y_all[h, j, c]
            if h == 0:
                y = dot(perm[...], y).astype(BF16)
            here = some_cols(h, j, c)
            scaled = y.astype(F32) * invg[:, here]
            scaled = scaled * scaled
            for q in range(chunk // lanes):
                squares += scaled[:, q * lanes : (q + 1) * lanes]
            total += dot_nt(y, wcat[:, here])
        sumsq[...] = squares
        acc[...] = total

    for c in range(chunks):
        for h in (0, 1):
            a, b = axes[h]
            all_but_one(
                y_all.at[h, 0, c, seen_b, :], aga_ss.at[0], aga_rs.at[h, c], b
            ).wait_recv()
            for d in (0, 1):
                agb_copy(h, d, 0, c, pos[a], True).start()
    loads[0].wait()
    loads[1].wait()
    for h in (0, 1):
        use(h, pos[axes[h][0]])

    def gather_step(k, carry):
        for c in range(chunks):
            for h in (0, 1):
                for d in (0, 1):
                    j = behind(h, d, k)
                    agb_copy(h, d, k - 1, c, j, True).wait_recv()

                    @pl.when(k < reach - 1)
                    def _():
                        agb_copy(h, d, k, c, j, True).start()

                    @pl.when(k == reach - 1)
                    def _():
                        agb_copy(h, d, k, c, j, False).start()

        for h in (0, 1):
            for d in (0, 1):
                use(h, behind(h, d, k))
        return carry

    lax.fori_loop(1, reach, gather_step, 0)
    for h in (0, 1):
        me = pos[axes[h][0]]
        for r in offsets:
            mix_copy(h, r).start()
        mix_r[h, :, pl.ds(pl.multiple_of(me * strip, strip), strip)] = mix_s[h, me]
    for h in (0, 1):
        j = behind(h, 0, reach)
        for d in (0, 1):
            for c in range(chunks):
                agb_copy(h, d, reach - 1, c, j, False).wait_recv()
        use(h, j)

    mean_sq = jnp.sum(sumsq[...], axis=1, keepdims=True) * (1.0 / width)
    factor = lax.rsqrt(mean_sq + 1e-05)

    def branch(base, scale_ref, pick):
        part = acc[:, pl.ds(base, slots)]
        scale = jnp.concatenate([scale_ref[...], jnp.zeros((1, slots - hidden), F32)], axis=1)
        added = jnp.dot(
            part, pick[...], precision=lax.Precision.HIGHEST, preferred_element_type=F32
        )
        return (part * scale + added) * factor

    gate = branch(0, gscale_ref, gpick)
    up = branch(slots, uscale_ref, upick)
    hid[0] = (gate / (1.0 + jnp.exp(-gate)) * up).astype(BF16)
    hid[1] = dot(perm[...], hid[0]).astype(BF16)
    for h in (0, 1):
        added = dot_nt(hid[h], dextp[...])
        high = added.astype(BF16)
        low = (added - high.astype(F32)).astype(BF16)
        lane = lax.broadcasted_iota(jnp.int32, added.shape, 1)
        extra_parts[h] = jnp.where(lane < k_out, high.astype(F32), low.astype(F32)).astype(BF16)
    loads[2].wait()

    def down(h, j, s):
        here = pl.ds(pl.multiple_of(h * half + s * wide, wide), wide)
        some = pl.ds(pl.multiple_of(j * block, block), block)
        base = dot(hid[h, some, :], wd[:, here]) * dscale_ref[:, here]
        return base + dot(extra_parts[h, some, :], onehot[:, here])

    def ring_copy(h, d, m):
        a = axes[h][0]
        return send(
            ring_s.at[h, d, m],
            ring_r.at[h, d, m + pieces],
            ring_ss.at[0],
            ring_rs.at[h, d, m],
            a,
            at(a, 1 - 2 * d),
        )

    def ring_step(m, carry):
        group = lax.div(m, per)
        within = lax.rem(m, per)
        away = lax.div(n - group, 2)
        odd = lax.rem(group, 2)
        for h in (0, 1):
            for d in (0, 1):
                s = (odd if d == 0 else 1 - odd) * per + within
                shift = n - away if d else away
                j = lax.rem(pos[axes[h][0]] + shift, n)
                value = down(h, j, s)

                @pl.when(m >= pieces)
                def _():
                    ring_copy(h, d, m - pieces).wait_recv()

                ring_s[h, d, m] = (value + ring_r[h, d, m].astype(F32)).astype(BF16)
                ring_copy(h, d, m).start()
        return carry

    lax.fori_loop(0, messages, ring_step, 0)

    def two_copy(h, p, r):
        b = axes[h][1]
        return send(
            two_s.at[h, p, at(b, r)],
            r_two.at[h, p, r - 1],
            two_ss.at[0],
            two_rs.at[h, p],
            b,
            at(b, r),
        )

    for h in (0, 1):
        for s in range(pieces):
            down_sum[h, s] = down(h, pos[axes[h][0]], s)
    for p in range(per):
        for h in (0, 1):
            for d in (0, 1):
                for m in (messages - pieces + p, messages - per + p):
                    ring_copy(h, d, m).wait_recv()
            for q in (0, 1):
                s = q * per + p
                plus = ring_r[h, 0, messages + (1 - q) * per + p].astype(F32)
                minus = ring_r[h, 1, messages + q * per + p].astype(F32)
                down_sum[h, s] = down_sum[h, s] + plus + minus
                for j in range(n):
                    few = down_sum[h, s, pl.ds(j * rows, rows), :]
                    two_s[h, p, j, :, pl.ds(q * wide, wide)] = few.astype(BF16)
            for r in offsets:
                two_copy(h, p, r).start()

    for h in (0, 1):
        a = axes[h][0]
        all_but_one(mix_s.at[h, pl.ds(0, n - 1)], mix_ss.at[0], mix_rs.at[h], a).wait_recv()
    for p in range(per):
        for h in (0, 1):
            b = axes[h][1]
            total = two_s[h, p, pos[b]].astype(F32)
            all_but_one(r_two.at[h, p], two_ss.at[0], two_rs.at[h, p], b).wait_recv()
            for r in range(1, n):
                total += r_two[h, p, r - 1].astype(F32)
            for q in (0, 1):
                here = (q * per + p) * wide
                value = total[:, q * wide : (q + 1) * wide] + mix_r[h, :, pl.ds(here, wide)]
                out_ref[:, pl.ds(h * half + here, wide)] = value.astype(BF16)
    def all_sent(ref, ssem, rsem):
        send(ref, ref, ssem, rsem, TENSOR[0], at(TENSOR[0], 1)).wait_send()

    most = pl.ds(0, n - 1)
    all_sent(heads_all.at[:, seen_w, :], heads_ss.at[0], heads_rs.at[0])
    all_sent(w_all.at[:, :, seen_w, mine], w_ss.at[0], w_rs.at[0, 0])
    for q in range(1, cores):
        all_sent(w_all.at[:, :, :, mine], share_ss.at[q - 1], share_rs.at[0, 0, q - 1])
    all_sent(strm.at[:, most], strm_ss.at[0], strm_rs.at[0])
    all_sent(r_one, one_ss.at[0], one_rs.at[0, 0])
    all_sent(y_all.at[:, 0, :, seen_b, :], aga_ss.at[0], aga_rs.at[0, 0])
    all_sent(y_all.at[:, most], agb_ss.at[0], agb_rs.at[0, 0, 0, 0])
    all_sent(mix_s.at[:, most], mix_ss.at[0], mix_rs.at[0])
    all_sent(ring_s, ring_ss.at[0], ring_rs.at[0, 0, 0])
    all_sent(r_two, two_ss.at[0], two_rs.at[0, 0])

def local(n, cores, *args):
    (
        heads_out,
        stream_in,
        proj_levels,
        proj_scale,
        norm_gain,
        gate_levels,
        gate_scale,
        gate_index,
        gate_extra,
        up_levels,
        up_scale,
        up_index,
        up_extra,
        down_levels,
        down_scale,
        down_index,
        down_extra,
    ) = args
    tokens, feats = heads_out.shape
    rows, width = stream_in.shape
    hidden = gate_levels.shape[1]
    k_out = gate_extra.shape[1]
    slots = -(-(hidden + k_out) // 128) * 128
    strip = width // 2 // n
    chunks = 2
    pieces = 4
    messages = pieces // 2 * (n - 1)
    chunk = strip // chunks
    block = tokens // n
    reach = n // 2
    index = pltpu.SMEM(gate_index.shape, jnp.int32)
    hbm = pl.BlockSpec(memory_space=pltpu.HBM)
    dma = pltpu.SemaphoreType.DMA
    scratch = [
        pltpu.VMEM((1, width), F32),
        pltpu.VMEM((1, width), F32),
        pltpu.VMEM((1, hidden), F32),
        index,
        pltpu.VMEM((k_out, width), BF16),
        pltpu.VMEM((1, hidden), F32),
        index,
        pltpu.VMEM((k_out, width), BF16),
        pltpu.VMEM((1, width), F32),
        index,
        pltpu.VMEM((k_out, hidden), BF16),
        pltpu.VMEM((2 * slots, width), BF16),
        pltpu.VMEM((slots, width), BF16),
        pltpu.VMEM((128, width), BF16),
        pltpu.VMEM((tokens, tokens), BF16),
        pltpu.VMEM((slots, slots), F32),
        pltpu.VMEM((slots, slots), F32),
        pltpu.VMEM((128, slots), BF16),
        pltpu.VMEM((1, width), F32),
        pltpu.VMEM((2, n * feats, tokens), BF16),
        pltpu.VMEM((2, tokens, n * feats), BF16),
        pltpu.VMEM((2, chunks, n * feats, chunk), BF16),
        pltpu.VMEM((2, n, rows, strip), BF16),
        pltpu.VMEM((2, chunks, tokens, chunk), F32),
        pltpu.VMEM((2, chunks, tokens, chunk), BF16),
        pltpu.VMEM((2, chunks, n - 1, block, chunk), BF16),
        pltpu.VMEM((2, chunks, block, chunk), F32),
        pltpu.VMEM((2, n, chunks, tokens, chunk), BF16),
        pltpu.VMEM((tokens, 2 * slots), F32),
        pltpu.VMEM((tokens, 128), F32),
        pltpu.VMEM((2, tokens, slots), BF16),
        pltpu.VMEM((2, tokens, 128), BF16),
        pltpu.VMEM((2, 2, messages, block, width // 2 // pieces), BF16),
        pltpu.VMEM((2, 2, messages + pieces, block, width // 2 // pieces), BF16),
        pltpu.VMEM((2, pieces // 2, n, rows, width // pieces), BF16),
        pltpu.VMEM((2, pieces // 2, n - 1, rows, width // pieces), BF16),
        pltpu.VMEM((2, n, rows, strip), F32),
        pltpu.VMEM((2, rows, width // 2), F32),
        pltpu.VMEM((2, pieces, block, width // 2 // pieces), F32),
        dma((4 + 2 * chunks + 14,)),
    ]
    for sends, receives in (
        (1, (2,)),
        (1, (2, chunks)),
        (cores, (2, chunks, max(cores - 1, 1))),
        (1, (2,)),
        (1, (2, chunks)),
        (1, (2, chunks)),
        (1, (2, 2, reach, chunks)),
        (1, (2, 2, messages)),
        (1, (2, pieces // 2)),
        (1, (2,)),
    ):
        scratch += [dma((sends,)), dma(receives)]
    return pl.pallas_call(
        functools.partial(kernel, n, cores),
        out_shape=jax.ShapeDtypeStruct((rows, width), BF16),
        in_specs=[hbm] * len(args),
        out_specs=pl.BlockSpec(memory_space=pltpu.VMEM),
        scratch_shapes=scratch,
        compiler_params=pltpu.CompilerParams(
            collective_id=0, has_side_effects=True, vmem_limit_bytes=48 * 1024 * 1024
        ),
    )(
        *(
            pltpu.with_memory_space_constraint(arg, pltpu.HBM)
            for arg in (
                heads_out.T,
                stream_in,
                proj_levels,
                proj_scale[None, :],
                norm_gain[None, :],
                gate_levels.T,
                gate_scale[None, :],
                gate_index,
                gate_extra.T,
                up_levels.T,
                up_scale[None, :],
                up_index,
                up_extra.T,
                down_levels,
                down_scale[None, :],
                down_index,
                down_extra.T,
            )
        )
    )


def solution(mesh):
    n = math.isqrt(mesh.shape["tensor"])
    torus = Mesh(
        mesh.devices.reshape(mesh.shape["groups"], n, n, mesh.shape["seq"]),
        ("groups", "tensor_0", "tensor_1", "seq"),
    )
    return jax.shard_map(
        functools.partial(local, n, mesh.shape["seq"]),
        mesh=torus,
        in_specs=(
            P(("groups", "seq"), TENSOR),
            P(GROUPS_SEQ_TENSOR, None),
            P(TENSOR, None),
            P(),
            P(),
            P(None, TENSOR),
            P(TENSOR),
            P(TENSOR, None),
            P(None, TENSOR),
            P(None, TENSOR),
            P(TENSOR),
            P(TENSOR, None),
            P(None, TENSOR),
            P(TENSOR, None),
            P(),
            P(TENSOR, None),
            P(TENSOR, None),
        ),
        out_specs=P(GROUPS_SEQ_TENSOR, None),
        check_vma=False,
    )
```

```python
import functools
import math

import jax
import jax.numpy as jnp
from jax import lax
from jax.experimental import pallas as pl
from jax.experimental.pallas import tpu as pltpu
from jax.sharding import Mesh
from jax.sharding import PartitionSpec as P

TENSOR = ("tensor_0", "tensor_1")
GROUPS_SEQ_TENSOR = ("groups", "seq", "tensor_0", "tensor_1")
MESH = pl.DeviceIdType.MESH
F32 = jnp.float32
BF16 = jnp.bfloat16
NT = (((1,), (1,)), ((), ()))


def dot(a, b):
    return jnp.dot(a, b, preferred_element_type=F32)


def dot_nt(a, b):
    return lax.dot_general(a, b, NT, preferred_element_type=F32)


def kernel(
    n,
    cores,
    heads_ref,
    stream_ref,
    projw_ref,
    pscale_in,
    gain_in,
    gatew_ref,
    gscale_in,
    gidx_in,
    gext_in,
    upw_ref,
    uscale_in,
    uidx_in,
    uext_in,
    downw_ref,
    dscale_in,
    didx_in,
    dext_in,
    out_ref,
    pscale_ref,
    gain_ref,
    gscale_ref,
    gidx_ref,
    gext_ref,
    uscale_ref,
    uidx_ref,
    uext_ref,
    dscale_ref,
    didx_ref,
    dext_ref,
    wcat,
    wd,
    onehot,
    perm,
    gpick,
    upick,
    dextp,
    invg,
    heads_all,
    ordered,
    w_all,
    strm,
    t_sum,
    t_half,
    r_one,
    mixed,
    y_all,
    acc,
    sumsq,
    hid,
    extra_parts,
    ring_s,
    ring_r,
    two_s,
    r_two,
    mix_s,
    mix_r,
    down_sum,
    load_sem,
    heads_ss,
    heads_rs,
    w_ss,
    w_rs,
    share_ss,
    share_rs,
    strm_ss,
    strm_rs,
    one_ss,
    one_rs,
    aga_ss,
    aga_rs,
    agb_ss,
    agb_rs,
    ring_ss,
    ring_rs,
    two_ss,
    two_rs,
    mix_ss,
    mix_rs,
):
    feats, tokens = heads_ref.shape
    width = projw_ref.shape[1]
    hidden = gatew_ref.shape[0]
    chunks = w_all.shape[1]
    chunk = w_all.shape[3]
    part = chunk // cores
    rows = stream_ref.shape[0]
    slots = gpick.shape[0]
    k_out = gext_ref.shape[0]
    half = width // 2
    strip = half // n
    block = tokens // n
    sub = tokens // 2
    wide = ring_s.shape[4]
    pieces = half // wide
    per = pieces // 2
    messages = per * (n - 1)
    reach = n // 2
    axes = (("tensor_0", "tensor_1"), ("tensor_1", "tensor_0"))
    pos = {name: lax.axis_index(name) for name in TENSOR}
    offsets = sorted(range(1, n), key=lambda r: -min(r, n - r))

    def at(name, shift):
        return lax.rem(pos[name] + (shift + n) % n, n)

    def cols(h, j):
        return pl.ds(pl.multiple_of(h * half + j * strip, strip), strip)

    def send(src, dst, ssem, rsem, name, target):
        return pltpu.make_async_remote_copy(
            src_ref=src,
            dst_ref=dst,
            send_sem=ssem,
            recv_sem=rsem,
            device_id={name: target},
            device_id_type=MESH,
        )

    def all_but_one(ref, ssem, rsem, name):
        return send(ref, ref, ssem, rsem, name, at(name, 1))

    core = lax.axis_index("seq")
    barrier = pltpu.get_barrier_semaphore()
    for name in TENSOR:
        for r in range(1, n):
            pl.semaphore_signal(
                barrier, inc=1, device_id={name: at(name, r)}, device_id_type=MESH
            )
    for q in range(1, cores):
        pl.semaphore_signal(
            barrier, inc=1, device_id={"seq": lax.rem(core + q, cores)}, device_id_type=MESH
        )

    def place(sender):
        return pl.ds(pl.multiple_of(sender * feats, feats), feats)

    mine = pl.ds(pl.multiple_of(core * part, part), part)

    def some_cols(h, j, c):
        return pl.ds(pl.multiple_of(h * half + j * strip + c * chunk, chunk), chunk)

    def own_part(h, j, c):
        start = h * half + j * strip + c * chunk + core * part
        return pl.ds(pl.multiple_of(start, part), part)

    first = []
    for h in (0, 1):
        me = pos[axes[h][0]]
        for src, dst in (
            (heads_ref, heads_all.at[h, place(me), :]),
            (stream_ref.at[:, cols(h, me)], strm.at[h, me]),
        ) + tuple(
            (projw_ref.at[:, own_part(h, me, c)], w_all.at[h, c, place(me), mine])
            for c in range(chunks)
        ):
            first.append(pltpu.make_async_copy(src, dst, load_sem.at[len(first)]))
            first[-1].start()
    pl.semaphore_wait(barrier, 2 * (n - 1) + cores - 1)

    def heads_copy(h, r):
        a = axes[h][0]
        there = heads_all.at[h, place(pos[a]), :]
        return send(there, there, heads_ss.at[0], heads_rs.at[h], a, at(a, r))

    def w_copy(h, c, r):
        a = axes[h][0]
        return send(
            projw_ref.at[:, own_part(h, at(a, r), c)],
            w_all.at[h, c, place(pos[a]), mine],
            w_ss.at[0],
            w_rs.at[h, c],
            a,
            at(a, r),
        )

    def share_copy(h, c, q):
        there = w_all.at[h, c, :, mine]
        to = lax.rem(core + q, cores)
        return send(there, there, share_ss.at[q - 1], share_rs.at[h, c, q - 1], "seq", to)

    def strm_copy(h, r):
        a = axes[h][0]
        return send(
            stream_ref.at[:, cols(h, at(a, r))],
            strm.at[h, pos[a]],
            strm_ss.at[0],
            strm_rs.at[h],
            a,
            at(a, r),
        )

    each = 2 + chunks
    for c in range(chunks):
        for r in offsets:
            for h in (0, 1):
                w_copy(h, c, r).start()
        if c == 0:
            for h in (0, 1):
                first[each * h].wait()
            for r in offsets:
                for h in (0, 1):
                    heads_copy(h, r).start()
    for r in offsets:
        for h in (0, 1):
            strm_copy(h, r).start()
    small = []
    for src, dst in (
        (pscale_in, pscale_ref),
        (gain_in, gain_ref),
        (gscale_in, gscale_ref),
        (gidx_in, gidx_ref),
        (gext_in, gext_ref),
        (uscale_in, uscale_ref),
        (uidx_in, uidx_ref),
        (uext_in, uext_ref),
        (dscale_in, dscale_ref),
        (didx_in, didx_ref),
        (dext_in, dext_ref),
    ):
        small.append(pltpu.make_async_copy(src, dst, load_sem.at[len(first) + len(small)]))
        small[-1].start()
    base = len(first) + len(small)
    loads = [
        pltpu.make_async_copy(gatew_ref, wcat.at[pl.ds(0, hidden), :], load_sem.at[base]),
        pltpu.make_async_copy(upw_ref, wcat.at[pl.ds(slots, hidden), :], load_sem.at[base + 1]),
        pltpu.make_async_copy(downw_ref, wd.at[pl.ds(0, hidden), :], load_sem.at[base + 2]),
    ]
    for load in loads:
        load.start()

    for copy in small:
        copy.wait()
    r_i = lax.broadcasted_iota(jnp.int32, (tokens, tokens), 0)
    c_i = lax.broadcasted_iota(jnp.int32, (tokens, tokens), 1)
    swapped = (
        lax.rem(lax.div(r_i, rows), n) * block + lax.div(r_i, block) * rows + lax.rem(r_i, rows)
    )
    perm[...] = jnp.where(c_i == swapped, 1.0, 0.0).astype(BF16)

    def index_column(idx_ref, count):
        row = lax.rem(lax.broadcasted_iota(jnp.int32, (count, 1), 0), k_out)
        column = jnp.zeros((count, 1), jnp.int32)
        for k in range(k_out):
            column = jnp.where(row == k, idx_ref[0, k], column)
        return column

    for pick, idx_ref in ((gpick, gidx_ref), (upick, uidx_ref)):
        pick[...] = jnp.zeros_like(pick)
        chosen = lax.broadcasted_iota(jnp.int32, (k_out, slots), 1) == index_column(idx_ref, k_out)
        pick[pl.ds(hidden, k_out), :] = jnp.where(chosen, 1.0, 0.0)

    one_rows = onehot.shape[0]
    didx = index_column(didx_ref, one_rows)
    live = lax.broadcasted_iota(jnp.int32, (one_rows, strip), 0) < 2 * k_out

    def prepare(j, carry):
        here = pl.ds(pl.multiple_of(j * strip, strip), strip)
        column = lax.broadcasted_iota(jnp.int32, (one_rows, strip), 1) + j * strip
        onehot[:, here] = jnp.where((column == didx) & live, 1.0, 0.0).astype(BF16)
        blank = jnp.zeros((slots - hidden - k_out, strip), F32)
        for base, ext in ((0, gext_ref), (slots, uext_ref)):
            filled = jnp.concatenate([ext[:, here].astype(F32), blank], axis=0)
            wcat[pl.ds(base + hidden, slots - hidden), here] = filled.astype(BF16)
        wd[pl.ds(hidden, slots - hidden), here] = jnp.zeros((slots - hidden, strip), BF16)
        invg[:, here] = 1.0 / gain_ref[:, here]
        return carry

    lax.fori_loop(0, width // strip, prepare, 0)
    dext = jnp.concatenate([dext_ref[...].astype(F32)] * 2, axis=0)
    dext = jnp.concatenate([dext, jnp.zeros((dextp.shape[0] - 2 * k_out, hidden), F32)], axis=0)
    dextp[...] = jnp.zeros_like(dextp)
    dextp[:, pl.ds(0, hidden)] = dext.astype(BF16)
    acc[...] = jnp.zeros_like(acc)
    sumsq[...] = jnp.zeros_like(sumsq)
    for h in (0, 1):
        for d in (0, 1):
            for m in range(pieces):
                ring_r[h, d, m] = jnp.zeros((block, wide), BF16)

    def one_copy(h, c, r):
        b = axes[h][1]
        away = pl.ds(pl.multiple_of(at(b, r) * block, block), block)
        return send(
            t_half.at[h, c, away, :],
            r_one.at[h, c, r - 1],
            one_ss.at[0],
            one_rs.at[h, c],
            b,
            at(b, r),
        )

    seen_w = pl.ds(0, (n - 1) * feats)
    seen_b = pl.ds(0, (n - 1) * block)
    for c in range(chunks):
        for h in (0, 1):
            a = axes[h][0]
            first[each * h + 2 + c].wait()
            all_but_one(
                w_all.at[h, c, seen_w, mine], w_ss.at[0], w_rs.at[h, c], a
            ).wait_recv()
            for q in range(1, cores):
                share_copy(h, c, q).start()
        for h in (0, 1):
            a = axes[h][0]
            if c == 0:
                all_but_one(
                    heads_all.at[h, seen_w, :], heads_ss.at[0], heads_rs.at[h], a
                ).wait_recv()
                if h == 0:
                    turn = perm[...]
                else:
                    turn = jnp.where(r_i == c_i, 1.0, 0.0).astype(BF16)
                ordered[h] = dot_nt(turn, heads_all[h]).astype(BF16)
            for q in range(1, cores):
                share_copy(h, c, q).wait_recv()
            t_sum[h, c] = dot(ordered[h], w_all[h, c])
            t_half[h, c] = t_sum[h, c].astype(BF16)
            for r in offsets:
                one_copy(h, c, r).start()

    def aga_copy(h, c, r):
        a, b = axes[h]
        own = pl.ds(pl.multiple_of(pos[b] * block, block), block)
        there = y_all.at[h, pos[a], c, own, :]
        return send(there, there, aga_ss.at[0], aga_rs.at[h, c], b, at(b, r))

    def mix_copy(h, r):
        a = axes[h][0]
        there = mix_r.at[h, :, pl.ds(pl.multiple_of(pos[a] * strip, strip), strip)]
        return send(mix_s.at[h, at(a, r)], there, mix_ss.at[0], mix_rs.at[h], a, at(a, r))

    for c in range(chunks):
        for h in (0, 1):
            a, b = axes[h]
            here = some_cols(h, pos[a], c)
            within = pl.ds(c * chunk, chunk)
            own = pl.ds(pl.multiple_of(pos[b] * block, block), block)
            total = t_sum[h, c, own, :]
            if c == 0:
                first[each * h + 1].wait()
                all_but_one(
                    strm.at[h, pl.ds(0, n - 1)], strm_ss.at[0], strm_rs.at[h], a
                ).wait_recv()
            all_but_one(r_one.at[h, c], one_ss.at[0], one_rs.at[h, c], b).wait_recv()
            for r in range(1, n):
                total += r_one[h, c, r - 1].astype(F32)
            mixed[h, c] = total * pscale_ref[:, here]
            for j in range(n):
                few = pl.ds(j * rows, rows)
                mixed[h, c, few, :] = mixed[h, c, few, :] + strm[h, j, :, within].astype(F32)
            y_all[h, pos[a], c, own, :] = (mixed[h, c] * gain_ref[:, here]).astype(BF16)
            for r in offsets:
                aga_copy(h, c, r).start()
            for j in range(n):
                mix_s[h, j, :, within] = mixed[h, c, pl.ds(j * rows, rows), :]
    def agb_copy(h, d, k, c, strip_id, whole):
        a = axes[h][0]
        some = pl.ds(0, tokens) if whole else pl.ds(d * sub, sub)
        there = y_all.at[h, strip_id, c, some, :]
        return send(
            there, there, agb_ss.at[0], agb_rs.at[h, d, k, c], a, at(a, 1 - 2 * d)
        )

    def behind(h, d, k):
        shift = k if d else n - k
        return lax.rem(pos[axes[h][0]] + shift, n)

    def use(h, j):
        lanes = sumsq.shape[1]
        squares = sumsq[...]
        total = acc[...]
        for c in range(chunks):
            y = y_all[h, j, c]
            if h == 0:
                y = dot(perm[...], y).astype(BF16)
            here = some_cols(h, j, c)
            scaled = y.astype(F32) * invg[:, here]
            scaled = scaled * scaled
            for q in range(chunk // lanes):
                squares += scaled[:, q * lanes : (q + 1) * lanes]
            total += dot_nt(y, wcat[:, here])
        sumsq[...] = squares
        acc[...] = total

    for c in range(chunks):
        for h in (0, 1):
            a, b = axes[h]
            all_but_one(
                y_all.at[h, 0, c, seen_b, :], aga_ss.at[0], aga_rs.at[h, c], b
            ).wait_recv()
            for d in (0, 1):
                agb_copy(h, d, 0, c, pos[a], True).start()
    loads[0].wait()
    loads[1].wait()
    for h in (0, 1):
        use(h, pos[axes[h][0]])

    def gather_step(k, carry):
        for c in range(chunks):
            for h in (0, 1):
                for d in (0, 1):
                    j = behind(h, d, k)
                    agb_copy(h, d, k - 1, c, j, True).wait_recv()

                    @pl.when(k < reach - 1)
                    def _():
                        agb_copy(h, d, k, c, j, True).start()

                    @pl.when(k == reach - 1)
                    def _():
                        agb_copy(h, d, k, c, j, False).start()

        for h in (0, 1):
            for d in (0, 1):
                use(h, behind(h, d, k))
        return carry

    lax.fori_loop(1, reach, gather_step, 0)
    for h in (0, 1):
        me = pos[axes[h][0]]
        for r in offsets:
            mix_copy(h, r).start()
        mix_r[h, :, pl.ds(pl.multiple_of(me * strip, strip), strip)] = mix_s[h, me]
    for h in (0, 1):
        j = behind(h, 0, reach)
        for d in (0, 1):
            for c in range(chunks):
                agb_copy(h, d, reach - 1, c, j, False).wait_recv()
        use(h, j)

    mean_sq = jnp.sum(sumsq[...], axis=1, keepdims=True) * (1.0 / width)
    factor = lax.rsqrt(mean_sq + 1e-05)

    upper = hidden // 128 * 128

    def branch(base, scale_ref, pick):
        part = acc[:, pl.ds(base, slots)]
        scale = jnp.concatenate([scale_ref[...], jnp.zeros((1, slots - hidden), F32)], axis=1)
        added = jnp.dot(
            part[:, upper:],
            pick[pl.ds(upper, slots - upper), :],
            precision=lax.Precision.HIGHEST,
            preferred_element_type=F32,
        )
        return (part * scale + added) * factor

    gate = branch(0, gscale_ref, gpick)
    up = branch(slots, uscale_ref, upick)
    hid[0] = (gate / (1.0 + jnp.exp(-gate)) * up).astype(BF16)
    hid[1] = dot(perm[...], hid[0]).astype(BF16)
    for h in (0, 1):
        added = dot_nt(hid[h], dextp[...])
        high = added.astype(BF16)
        low = (added - high.astype(F32)).astype(BF16)
        lane = lax.broadcasted_iota(jnp.int32, added.shape, 1)
        extra_parts[h] = jnp.where(lane < k_out, high.astype(F32), low.astype(F32)).astype(BF16)
    loads[2].wait()

    def down(h, j, s):
        here = pl.ds(pl.multiple_of(h * half + s * wide, wide), wide)
        some = pl.ds(pl.multiple_of(j * block, block), block)
        base = dot(hid[h, some, :], wd[:, here]) * dscale_ref[:, here]
        return base + dot(extra_parts[h, some, :], onehot[:, here])

    def ring_copy(h, d, m):
        a = axes[h][0]
        return send(
            ring_s.at[h, d, m],
            ring_r.at[h, d, m + pieces],
            ring_ss.at[0],
            ring_rs.at[h, d, m],
            a,
            at(a, 1 - 2 * d),
        )

    def ring_step(m, carry):
        group = lax.div(m, per)
        within = lax.rem(m, per)
        away = lax.div(n - group, 2)
        odd = lax.rem(group, 2)
        for h in (0, 1):
            for d in (0, 1):
                s = (odd if d == 0 else 1 - odd) * per + within
                shift = n - away if d else away
                j = lax.rem(pos[axes[h][0]] + shift, n)
                value = down(h, j, s)

                @pl.when(m >= pieces)
                def _():
                    ring_copy(h, d, m - pieces).wait_recv()

                ring_s[h, d, m] = (value + ring_r[h, d, m].astype(F32)).astype(BF16)
                ring_copy(h, d, m).start()
        return carry

    lax.fori_loop(0, messages, ring_step, 0)

    def two_copy(h, p, r):
        b = axes[h][1]
        return send(
            two_s.at[h, p, at(b, r)],
            r_two.at[h, p, r - 1],
            two_ss.at[0],
            two_rs.at[h, p],
            b,
            at(b, r),
        )

    for h in (0, 1):
        for s in range(pieces):
            down_sum[h, s] = down(h, pos[axes[h][0]], s)
    for p in range(per):
        for h in (0, 1):
            for d in (0, 1):
                for m in (messages - pieces + p, messages - per + p):
                    ring_copy(h, d, m).wait_recv()
            for q in (0, 1):
                s = q * per + p
                plus = ring_r[h, 0, messages + (1 - q) * per + p].astype(F32)
                minus = ring_r[h, 1, messages + q * per + p].astype(F32)
                down_sum[h, s] = down_sum[h, s] + plus + minus
                for j in range(n):
                    few = down_sum[h, s, pl.ds(j * rows, rows), :]
                    two_s[h, p, j, :, pl.ds(q * wide, wide)] = few.astype(BF16)
            for r in offsets:
                two_copy(h, p, r).start()

    for h in (0, 1):
        a = axes[h][0]
        all_but_one(mix_s.at[h, pl.ds(0, n - 1)], mix_ss.at[0], mix_rs.at[h], a).wait_recv()
    for p in range(per):
        for h in (0, 1):
            b = axes[h][1]
            total = two_s[h, p, pos[b]].astype(F32)
            all_but_one(r_two.at[h, p], two_ss.at[0], two_rs.at[h, p], b).wait_recv()
            for r in range(1, n):
                total += r_two[h, p, r - 1].astype(F32)
            for q in (0, 1):
                here = (q * per + p) * wide
                value = total[:, q * wide : (q + 1) * wide] + mix_r[h, :, pl.ds(here, wide)]
                out_ref[:, pl.ds(h * half + here, wide)] = value.astype(BF16)
    def all_sent(ref, ssem, rsem):
        send(ref, ref, ssem, rsem, TENSOR[0], at(TENSOR[0], 1)).wait_send()

    most = pl.ds(0, n - 1)
    all_sent(heads_all.at[:, seen_w, :], heads_ss.at[0], heads_rs.at[0])
    all_sent(w_all.at[:, :, seen_w, mine], w_ss.at[0], w_rs.at[0, 0])
    for q in range(1, cores):
        all_sent(w_all.at[:, :, :, mine], share_ss.at[q - 1], share_rs.at[0, 0, q - 1])
    all_sent(strm.at[:, most], strm_ss.at[0], strm_rs.at[0])
    all_sent(r_one, one_ss.at[0], one_rs.at[0, 0])
    all_sent(y_all.at[:, 0, :, seen_b, :], aga_ss.at[0], aga_rs.at[0, 0])
    all_sent(y_all.at[:, most], agb_ss.at[0], agb_rs.at[0, 0, 0, 0])
    all_sent(mix_s.at[:, most], mix_ss.at[0], mix_rs.at[0])
    all_sent(ring_s, ring_ss.at[0], ring_rs.at[0, 0, 0])
    all_sent(r_two, two_ss.at[0], two_rs.at[0, 0])

def local(n, cores, *args):
    (
        heads_out,
        stream_in,
        proj_levels,
        proj_scale,
        norm_gain,
        gate_levels,
        gate_scale,
        gate_index,
        gate_extra,
        up_levels,
        up_scale,
        up_index,
        up_extra,
        down_levels,
        down_scale,
        down_index,
        down_extra,
    ) = args
    tokens, feats = heads_out.shape
    rows, width = stream_in.shape
    hidden = gate_levels.shape[1]
    k_out = gate_extra.shape[1]
    slots = -(-(hidden + k_out) // 128) * 128
    strip = width // 2 // n
    chunks = 2
    pieces = 4
    messages = pieces // 2 * (n - 1)
    chunk = strip // chunks
    block = tokens // n
    reach = n // 2
    index = pltpu.SMEM(gate_index.shape, jnp.int32)
    hbm = pl.BlockSpec(memory_space=pltpu.HBM)
    dma = pltpu.SemaphoreType.DMA
    scratch = [
        pltpu.VMEM((1, width), F32),
        pltpu.VMEM((1, width), F32),
        pltpu.VMEM((1, hidden), F32),
        index,
        pltpu.VMEM((k_out, width), BF16),
        pltpu.VMEM((1, hidden), F32),
        index,
        pltpu.VMEM((k_out, width), BF16),
        pltpu.VMEM((1, width), F32),
        index,
        pltpu.VMEM((k_out, hidden), BF16),
        pltpu.VMEM((2 * slots, width), BF16),
        pltpu.VMEM((slots, width), BF16),
        pltpu.VMEM((128, width), BF16),
        pltpu.VMEM((tokens, tokens), BF16),
        pltpu.VMEM((slots, slots), F32),
        pltpu.VMEM((slots, slots), F32),
        pltpu.VMEM((128, slots), BF16),
        pltpu.VMEM((1, width), F32),
        pltpu.VMEM((2, n * feats, tokens), BF16),
        pltpu.VMEM((2, tokens, n * feats), BF16),
        pltpu.VMEM((2, chunks, n * feats, chunk), BF16),
        pltpu.VMEM((2, n, rows, strip), BF16),
        pltpu.VMEM((2, chunks, tokens, chunk), F32),
        pltpu.VMEM((2, chunks, tokens, chunk), BF16),
        pltpu.VMEM((2, chunks, n - 1, block, chunk), BF16),
        pltpu.VMEM((2, chunks, block, chunk), F32),
        pltpu.VMEM((2, n, chunks, tokens, chunk), BF16),
        pltpu.VMEM((tokens, 2 * slots), F32),
        pltpu.VMEM((tokens, 128), F32),
        pltpu.VMEM((2, tokens, slots), BF16),
        pltpu.VMEM((2, tokens, 128), BF16),
        pltpu.VMEM((2, 2, messages, block, width // 2 // pieces), BF16),
        pltpu.VMEM((2, 2, messages + pieces, block, width // 2 // pieces), BF16),
        pltpu.VMEM((2, pieces // 2, n, rows, width // pieces), BF16),
        pltpu.VMEM((2, pieces // 2, n - 1, rows, width // pieces), BF16),
        pltpu.VMEM((2, n, rows, strip), F32),
        pltpu.VMEM((2, rows, width // 2), F32),
        pltpu.VMEM((2, pieces, block, width // 2 // pieces), F32),
        dma((4 + 2 * chunks + 14,)),
    ]
    for sends, receives in (
        (1, (2,)),
        (1, (2, chunks)),
        (cores, (2, chunks, max(cores - 1, 1))),
        (1, (2,)),
        (1, (2, chunks)),
        (1, (2, chunks)),
        (1, (2, 2, reach, chunks)),
        (1, (2, 2, messages)),
        (1, (2, pieces // 2)),
        (1, (2,)),
    ):
        scratch += [dma((sends,)), dma(receives)]
    return pl.pallas_call(
        functools.partial(kernel, n, cores),
        out_shape=jax.ShapeDtypeStruct((rows, width), BF16),
        in_specs=[hbm] * len(args),
        out_specs=pl.BlockSpec(memory_space=pltpu.VMEM),
        scratch_shapes=scratch,
        compiler_params=pltpu.CompilerParams(
            collective_id=0, has_side_effects=True, vmem_limit_bytes=48 * 1024 * 1024
        ),
    )(
        *(
            pltpu.with_memory_space_constraint(arg, pltpu.HBM)
            for arg in (
                heads_out.T,
                stream_in,
                proj_levels,
                proj_scale[None, :],
                norm_gain[None, :],
                gate_levels.T,
                gate_scale[None, :],
                gate_index,
                gate_extra.T,
                up_levels.T,
                up_scale[None, :],
                up_index,
                up_extra.T,
                down_levels,
                down_scale[None, :],
                down_index,
                down_extra.T,
            )
        )
    )


def solution(mesh):
    n = math.isqrt(mesh.shape["tensor"])
    torus = Mesh(
        mesh.devices.reshape(mesh.shape["groups"], n, n, mesh.shape["seq"]),
        ("groups", "tensor_0", "tensor_1", "seq"),
    )
    return jax.shard_map(
        functools.partial(local, n, mesh.shape["seq"]),
        mesh=torus,
        in_specs=(
            P(("groups", "seq"), TENSOR),
            P(GROUPS_SEQ_TENSOR, None),
            P(TENSOR, None),
            P(),
            P(),
            P(None, TENSOR),
            P(TENSOR),
            P(TENSOR, None),
            P(None, TENSOR),
            P(None, TENSOR),
            P(TENSOR),
            P(TENSOR, None),
            P(None, TENSOR),
            P(TENSOR, None),
            P(),
            P(TENSOR, None),
            P(TENSOR, None),
        ),
        out_specs=P(GROUPS_SEQ_TENSOR, None),
        check_vma=False,
    )
```
